16 devices in a mesh: dp: 2 (over z), cp: 8 (over y, x, core).
Axes of the slice: x: 2, y: 2, z: 2, core: 2. Of those that a mesh axis runs over, the one named last changes fastest.
Arguments:
- x: bfloat16 [32, 7168], P('dp'), parts along dimension 0
- w_dq: bfloat16 [7168, 1536], replicated
- g_q: float32 [1536], replicated
- w_uq: bfloat16 [1536, 24576], replicated
- w_dkv: bfloat16 [7168, 576], replicated
- g_kv: float32 [512], replicated
- w_uk: bfloat16 [512, 128, 128], replicated
- w_uv: bfloat16 [512, 128, 128], replicated
- w_o: bfloat16 [16384, 7168], replicated
- cache_c: bfloat16 [32, 32768, 512], P('dp', 'cp'), parts along dimension 0
- cache_kr: bfloat16 [32, 32768, 64], P('dp', 'cp'), parts along dimension 0
- ctx_len: int32 [32], P('dp'), parts along dimension 0
Outputs:
- output 1: bfloat16 [32, 7168], P('dp'), parts along dimension 0
- output 2: bfloat16 [32, 512], P('dp'), parts along dimension 0
- output 3: bfloat16 [32, 64], P('dp'), parts along dimension 0
There are 2 independent parts. The reference program is written for one: setup_inputs(seed, part) draws one part's arguments, and reference() takes and returns one part's arrays. A program takes and returns all parts, laid end to end along the dimension named above; an argument that names none is the same for every part.
All inputs are finite; a program needn't handle non-finite values.
Results may differ from the reference program's by a relative error of at most 0.0063435.
Values sent between devices are 32-bit elements.
A program may use at most 1.75 GiB of HBM per device.

```python
import jax
import jax.numpy as jnp
from jax import lax

BATCH = 16
T_DEV = 4096
GROUP_SIZE = 8
D_MODEL = 7168
HEADS = 128
Q_LORA = 1536
LATENT = 512
NOPE_DIM = 128
ROPE_DIM = 64
V_DIM = 128

SEQ = T_DEV * GROUP_SIZE
QK_DIM = NOPE_DIM + ROPE_DIM
NORM_EPS = 1e-6
ROPE_THETA = 10000.0


def rms_norm(values, gain_vec):
    mean_sq = jnp.mean(jnp.square(values), axis=-1, keepdims=True)
    return values * lax.rsqrt(mean_sq + NORM_EPS) * gain_vec


def rope_tables(positions):
    half_dim = ROPE_DIM // 2
    inv_freq = ROPE_THETA ** (-2.0 * jnp.arange(half_dim, dtype=jnp.float32) / ROPE_DIM)
    angles = positions.astype(jnp.float32)[..., None] * inv_freq
    return jnp.cos(angles), jnp.sin(angles)


def rope_rotate(values, cos_tab, sin_tab):
    half_dim = values.shape[-1] // 2
    lo_half = values[..., :half_dim]
    hi_half = values[..., half_dim:]
    return jnp.concatenate([lo_half * cos_tab - hi_half * sin_tab, hi_half * cos_tab + lo_half * sin_tab], axis=-1)


def setup_inputs(seed: int = 0, part: int = 0) -> dict:
    shared_keys = jax.random.split(jax.random.key(seed), 8)
    part_keys = jax.random.split(jax.random.fold_in(jax.random.key(seed + 1), part), 8)

    def draw_normal(key, shape, std):
        return jax.random.normal(key, shape, jnp.float32) * std

    x = draw_normal(part_keys[0], (BATCH, D_MODEL), 1.0).astype(jnp.bfloat16)
    w_dq = draw_normal(shared_keys[0], (D_MODEL, Q_LORA), D_MODEL ** -0.5).astype(jnp.bfloat16)
    g_q = jax.random.uniform(shared_keys[1], (Q_LORA,), jnp.float32, 0.5, 1.5)
    w_uq = draw_normal(shared_keys[2], (Q_LORA, HEADS * QK_DIM), Q_LORA ** -0.5).astype(jnp.bfloat16)
    w_dkv = draw_normal(shared_keys[3], (D_MODEL, LATENT + ROPE_DIM), D_MODEL ** -0.5).astype(jnp.bfloat16)
    g_kv = jax.random.uniform(shared_keys[4], (LATENT,), jnp.float32, 0.5, 1.5)
    w_uk = draw_normal(shared_keys[5], (LATENT, HEADS, NOPE_DIM), LATENT ** -0.5).astype(jnp.bfloat16)
    w_uv = draw_normal(shared_keys[6], (LATENT, HEADS, V_DIM), LATENT ** -0.5).astype(jnp.bfloat16)
    w_o = draw_normal(shared_keys[7], (HEADS * V_DIM, D_MODEL), (HEADS * V_DIM) ** -0.5).astype(jnp.bfloat16)
    pos_ramp = 2.0 * jnp.arange(SEQ, dtype=jnp.float32) / SEQ - 1.0
    drift_dir = draw_normal(part_keys[1], (BATCH, 1, LATENT), 1.0)
    cache_c = (draw_normal(part_keys[2], (BATCH, SEQ, LATENT), 1.0) + drift_dir * pos_ramp[None, :, None]).astype(jnp.bfloat16)
    key_base = jnp.broadcast_to(draw_normal(part_keys[3], (BATCH, 1, ROPE_DIM), 1.0), (BATCH, SEQ, ROPE_DIM))
    cos_tab, sin_tab = rope_tables(jnp.arange(SEQ))
    cache_kr = (rope_rotate(key_base, cos_tab[None], sin_tab[None]) + draw_normal(part_keys[4], (BATCH, SEQ, ROPE_DIM), 0.5)).astype(jnp.bfloat16)
    ctx_len = jax.random.randint(part_keys[5], (BATCH,), SEQ // 2, SEQ, dtype=jnp.int32).at[0].set(SEQ - 1)
    return {'x': x, 'w_dq': w_dq, 'g_q': g_q, 'w_uq': w_uq, 'w_dkv': w_dkv, 'g_kv': g_kv, 'w_uk': w_uk, 'w_uv': w_uv, 'w_o': w_o, 'cache_c': cache_c, 'cache_kr': cache_kr, 'ctx_len': ctx_len}


def reference(x, w_dq, g_q, w_uq, w_dkv, g_kv, w_uk, w_uv, w_o, cache_c, cache_kr, ctx_len):
    cq_low = jnp.dot(x, w_dq, preferred_element_type=jnp.float32).astype(jnp.bfloat16)
    cq_norm = rms_norm(cq_low.astype(jnp.float32), g_q).astype(jnp.bfloat16)
    q_full = jnp.dot(cq_norm, w_uq, preferred_element_type=jnp.float32).astype(jnp.bfloat16).reshape(BATCH, HEADS, QK_DIM)
    cos_tab, sin_tab = rope_tables(ctx_len)
    q_rope = rope_rotate(q_full[:, :, NOPE_DIM:].astype(jnp.float32), cos_tab[:, None, :], sin_tab[:, None, :]).astype(jnp.bfloat16)
    q_lat = jnp.einsum('bhn,khn->bhk', q_full[:, :, :NOPE_DIM].astype(jnp.float32), w_uk.astype(jnp.float32)).astype(jnp.bfloat16)
    kv_full = jnp.dot(x, w_dkv, preferred_element_type=jnp.float32)
    c_new = rms_norm(kv_full[:, :LATENT], g_kv).astype(jnp.bfloat16)
    kr_new = rope_rotate(kv_full[:, LATENT:], cos_tab, sin_tab).astype(jnp.bfloat16)
    score_scale = QK_DIM ** -0.5
    positions = jnp.arange(SEQ)

    def attend_one(item_args):
        q_lat_r, q_rope_r, c_rows, kr_rows, c_new_r, kr_new_r, req_len = item_args
        scores = (jnp.dot(q_lat_r, c_rows.T, preferred_element_type=jnp.float32) + jnp.dot(q_rope_r, kr_rows.T, preferred_element_type=jnp.float32)) * score_scale
        scores = jnp.where(positions[None, :] < req_len, scores, -jnp.inf)
        new_score = (jnp.dot(q_lat_r, c_new_r, preferred_element_type=jnp.float32) + jnp.dot(q_rope_r, kr_new_r, preferred_element_type=jnp.float32)) * score_scale
        row_max = jnp.maximum(jnp.max(scores, axis=1), new_score)
        weights = jnp.exp(scores - row_max[:, None])
        new_weight = jnp.exp(new_score - row_max)
        row_sum = jnp.sum(weights, axis=1) + new_weight
        lat_acc = jnp.dot(weights.astype(jnp.bfloat16), c_rows, preferred_element_type=jnp.float32)
        lat_acc = lat_acc + new_weight.astype(jnp.bfloat16).astype(jnp.float32)[:, None] * c_new_r.astype(jnp.float32)[None, :]
        return lat_acc / row_sum[:, None]

    o_lat = lax.map(attend_one, (q_lat, q_rope, cache_c, cache_kr, c_new, kr_new, ctx_len)).astype(jnp.bfloat16)
    o_heads = jnp.einsum('bhk,khv->bhv', o_lat.astype(jnp.float32), w_uv.astype(jnp.float32)).astype(jnp.bfloat16)
    attn_out = jnp.dot(o_heads.reshape(BATCH, HEADS * V_DIM), w_o, preferred_element_type=jnp.float32)
    x_out = (x.astype(jnp.float32) + attn_out).astype(jnp.bfloat16)
    return x_out, c_new, kr_new
```

```python
import functools

import jax
import jax.numpy as jnp
from jax import lax
from jax.experimental import pallas as pl
from jax.experimental.pallas import tpu as pltpu
from jax.sharding import PartitionSpec as P

NORM_EPS = 1e-6
ROPE_THETA = 10000.0
MASKED = -1e30
FLOOR = -1e29
LOG2E = 1.4426950408889634


def rms_norm(values, gain_vec):
    mean_sq = jnp.mean(jnp.square(values), axis=-1, keepdims=True)
    return values * lax.rsqrt(mean_sq + NORM_EPS) * gain_vec


def rope_tables(positions, rope_dim):
    half_dim = rope_dim // 2
    inv_freq = ROPE_THETA ** (-2.0 * jnp.arange(half_dim, dtype=jnp.float32) / rope_dim)
    angles = positions.astype(jnp.float32)[..., None] * inv_freq
    return jnp.cos(angles), jnp.sin(angles)


def rope_rotate(values, cos_tab, sin_tab):
    half_dim = values.shape[-1] // 2
    lo_half = values[..., :half_dim]
    hi_half = values[..., half_dim:]
    return jnp.concatenate([lo_half * cos_tab - hi_half * sin_tab, hi_half * cos_tab + lo_half * sin_tab], axis=-1)


def project_step(x, w_dq, g_q, w_uq, w_dkv, g_kv, w_uk, ctx_len):
    n_req = x.shape[0]
    latent, n_heads, nope_dim = w_uk.shape
    rope_dim = w_dkv.shape[1] - latent
    cq_low = jnp.dot(x, w_dq, preferred_element_type=jnp.float32).astype(jnp.bfloat16)
    cq_norm = rms_norm(cq_low.astype(jnp.float32), g_q).astype(jnp.bfloat16)
    q_full = jnp.dot(cq_norm, w_uq, preferred_element_type=jnp.float32).astype(jnp.bfloat16)
    q_full = q_full.reshape(n_req, n_heads, nope_dim + rope_dim)
    cos_tab, sin_tab = rope_tables(ctx_len, rope_dim)
    q_rope = rope_rotate(q_full[:, :, nope_dim:].astype(jnp.float32), cos_tab[:, None, :], sin_tab[:, None, :]).astype(jnp.bfloat16)
    q_lat = jnp.einsum('bhn,khn->bhk', q_full[:, :, :nope_dim], w_uk, preferred_element_type=jnp.float32).astype(jnp.bfloat16)
    kv_full = jnp.dot(x, w_dkv, preferred_element_type=jnp.float32)
    c_new = rms_norm(kv_full[:, :latent], g_kv).astype(jnp.bfloat16)
    kr_new = rope_rotate(kv_full[:, latent:], cos_tab, sin_tab).astype(jnp.bfloat16)
    return q_lat, q_rope, c_new, kr_new


def attend_body(scale, t_chunk, ctx_ref, q_ref, qr_ref, c_ref, kr_ref, acc_ref, ml_ref, s_ref):
    b = pl.program_id(0)
    t_dev = c_ref.shape[1]
    base = lax.axis_index('cp') * t_dev
    limit = ctx_ref[b] - base
    q = q_ref[0]
    qr = qr_ref[0]
    n_chunks = t_dev // t_chunk
    lane_max = None
    nt = (((1,), (1,)), ((), ()))
    for i in range(n_chunks):
        sl = pl.ds(i * t_chunk, t_chunk)
        s = lax.dot_general(q, c_ref[0, sl, :], nt, preferred_element_type=jnp.float32)
        s = s + jnp.dot(qr, kr_ref[0, :, sl], preferred_element_type=jnp.float32)
        pos = lax.broadcasted_iota(jnp.int32, (1, t_chunk), 1) + i * t_chunk
        s = jnp.where(pos < limit, s, MASKED)
        s_ref[:, sl] = s
        cm = jnp.max(s, axis=1, keepdims=True)
        lane_max = cm if lane_max is None else jnp.maximum(lane_max, cm)
    m = jnp.maximum(lane_max, FLOOR)
    k2 = scale * LOG2E
    acc = None
    l = None
    for i in range(n_chunks):
        sl = pl.ds(i * t_chunk, t_chunk)
        p = jnp.exp2((s_ref[:, sl] - m) * k2)
        ls = jnp.sum(p, axis=1, keepdims=True)
        l = ls if l is None else l + ls
        o = jnp.dot(p.astype(jnp.bfloat16), c_ref[0, sl, :], preferred_element_type=jnp.float32)
        acc = o if acc is None else acc + o
    acc_ref[0] = acc
    lane = lax.broadcasted_iota(jnp.int32, (acc.shape[0], 128), 1)
    ml_ref[0] = jnp.where(lane == 0, m * scale, l)


def attend(q_lat, q_rope, cache_c, cache_kr_t, ctx_len, scale):
    n_req, heads, latent = q_lat.shape
    t_dev = cache_c.shape[1]
    rope = q_rope.shape[2]
    grid_spec = pltpu.PrefetchScalarGridSpec(
        num_scalar_prefetch=1,
        grid=(n_req,),
        in_specs=[
            pl.BlockSpec((1, heads, latent), lambda b, c: (b, 0, 0)),
            pl.BlockSpec((1, heads, rope), lambda b, c: (b, 0, 0)),
            pl.BlockSpec((1, t_dev, latent), lambda b, c: (b, 0, 0)),
            pl.BlockSpec((1, rope, t_dev), lambda b, c: (b, 0, 0)),
        ],
        out_specs=[
            pl.BlockSpec((1, heads, latent), lambda b, c: (b, 0, 0)),
            pl.BlockSpec((1, heads, 128), lambda b, c: (b, 0, 0)),
        ],
        scratch_shapes=[pltpu.VMEM((heads, t_dev), jnp.float32)],
    )
    return pl.pallas_call(
        functools.partial(attend_body, scale, min(512, t_dev)),
        grid_spec=grid_spec,
        out_shape=[
            jax.ShapeDtypeStruct((n_req, heads, latent), jnp.float32),
            jax.ShapeDtypeStruct((n_req, heads, 128), jnp.float32),
        ],
        compiler_params=pltpu.CompilerParams(vmem_limit_bytes=60 * 1024 * 1024),
        name='attend',
    )(ctx_len, q_lat, q_rope, cache_c, cache_kr_t)


def solution(mesh):
    n_cp = mesh.shape['cp']

    def decode_step(x, w_dq, g_q, w_uq, w_dkv, g_kv, w_uk, w_uv, w_o, cache_c, cache_kr, ctx_len):
        scale = (w_uk.shape[2] + cache_kr.shape[2]) ** -0.5
        me = lax.axis_index('cp')
        n_heads = w_uk.shape[1]
        hs = n_heads // n_cp
        q_lat, q_rope, c_new, kr_new = project_step(x, w_dq, g_q, w_uq, w_dkv, g_kv, w_uk, ctx_len)
        acc, ml = attend(q_lat, q_rope, cache_c, jnp.swapaxes(cache_kr, 1, 2), ctx_len, scale)
        m, l = ml[:, :, 0], ml[:, :, 1]
        new_s = (jnp.einsum('bhk,bk->bh', q_lat, c_new, preferred_element_type=jnp.float32)
                 + jnp.einsum('bhr,br->bh', q_rope, kr_new, preferred_element_type=jnp.float32)) * scale
        ml_all = lax.all_gather(ml[:, :, :2], 'cp')
        top = jnp.maximum(jnp.max(ml_all[..., 0], axis=0), new_s)
        w_new = jnp.exp(new_s - top)
        total = jnp.sum(jnp.exp(ml_all[..., 0] - top[None]) * ml_all[..., 1], axis=0) + w_new
        part = acc * jnp.exp(m - top)[:, :, None]
        mine = lax.psum_scatter(part, 'cp', scatter_dimension=1, tiled=True)
        w_new = lax.dynamic_slice_in_dim(w_new, me * hs, hs, 1)
        total = lax.dynamic_slice_in_dim(total, me * hs, hs, 1)
        mine = mine + w_new[:, :, None] * c_new.astype(jnp.float32)[:, None, :]
        o_lat = (mine / total[:, :, None]).astype(jnp.bfloat16)
        uv = lax.dynamic_slice_in_dim(w_uv, me * hs, hs, 1)
        o_heads = jnp.einsum('bhk,khv->bhv', o_lat, uv, preferred_element_type=jnp.float32).astype(jnp.bfloat16)
        rows = hs * w_uv.shape[2]
        wo = lax.dynamic_slice_in_dim(w_o, me * rows, rows, 0)
        part_out = jnp.dot(o_heads.reshape(x.shape[0], -1), wo, preferred_element_type=jnp.float32)
        attn_out = lax.psum(part_out, 'cp')
        return (x.astype(jnp.float32) + attn_out).astype(jnp.bfloat16), c_new, kr_new

    spec_rows = P('dp', None)
    spec_cache = P('dp', 'cp', None)
    in_specs = (spec_rows, P(), P(), P(), P(), P(), P(), P(), P(), spec_cache, spec_cache, P('dp'))
    out_specs = (spec_rows, spec_rows, spec_rows)
    return jax.shard_map(decode_step, mesh=mesh, in_specs=in_specs, out_specs=out_specs, check_vma=False)
```

```python
import functools

import jax
import jax.numpy as jnp
from jax import lax
from jax.experimental import pallas as pl
from jax.experimental.pallas import tpu as pltpu
from jax.sharding import PartitionSpec as P

NORM_EPS = 1e-6
ROPE_THETA = 10000.0
MASKED = -1e30
FLOOR = -1e29
LOG2E = 1.4426950408889634


def rms_norm(values, gain_vec):
    mean_sq = jnp.mean(jnp.square(values), axis=-1, keepdims=True)
    return values * lax.rsqrt(mean_sq + NORM_EPS) * gain_vec


def rope_tables(positions, rope_dim):
    half_dim = rope_dim // 2
    inv_freq = ROPE_THETA ** (-2.0 * jnp.arange(half_dim, dtype=jnp.float32) / rope_dim)
    angles = positions.astype(jnp.float32)[..., None] * inv_freq
    return jnp.cos(angles), jnp.sin(angles)


def rope_rotate(values, cos_tab, sin_tab):
    half_dim = values.shape[-1] // 2
    lo_half = values[..., :half_dim]
    hi_half = values[..., half_dim:]
    return jnp.concatenate([lo_half * cos_tab - hi_half * sin_tab, hi_half * cos_tab + lo_half * sin_tab], axis=-1)


def project_step(x, w_dq, g_q, w_uq, w_dkv, g_kv, w_uk, ctx_len):
    n_req = x.shape[0]
    latent, n_heads, nope_dim = w_uk.shape
    rope_dim = w_dkv.shape[1] - latent
    cq_low = jnp.dot(x, w_dq, preferred_element_type=jnp.float32).astype(jnp.bfloat16)
    cq_norm = rms_norm(cq_low.astype(jnp.float32), g_q).astype(jnp.bfloat16)
    q_full = jnp.dot(cq_norm, w_uq, preferred_element_type=jnp.float32).astype(jnp.bfloat16)
    q_full = q_full.reshape(n_req, n_heads, nope_dim + rope_dim)
    cos_tab, sin_tab = rope_tables(ctx_len, rope_dim)
    q_rope = rope_rotate(q_full[:, :, nope_dim:].astype(jnp.float32), cos_tab[:, None, :], sin_tab[:, None, :]).astype(jnp.bfloat16)
    q_lat = jnp.einsum('bhn,khn->bhk', q_full[:, :, :nope_dim], w_uk, preferred_element_type=jnp.float32).astype(jnp.bfloat16)
    kv_full = jnp.dot(x, w_dkv, preferred_element_type=jnp.float32)
    c_new = rms_norm(kv_full[:, :latent], g_kv).astype(jnp.bfloat16)
    kr_new = rope_rotate(kv_full[:, latent:], cos_tab, sin_tab).astype(jnp.bfloat16)
    return q_lat, q_rope, c_new, kr_new


def exchange(src, dst, send_sem, recv_sem, peer):
    return pltpu.make_async_remote_copy(
        src_ref=src, dst_ref=dst, send_sem=send_sem, recv_sem=recv_sem,
        device_id={'cp': peer}, device_id_type=pl.DeviceIdType.MESH)


def merge(parts, latent):
    tops = [p[:, latent:latent + 1] for p in parts]
    top = functools.reduce(jnp.maximum, tops)
    acc, mass = None, None
    for p, t in zip(parts, tops):
        f = jnp.exp(t - top)
        a, w = p[:, :latent] * f, p[:, latent + 64:latent + 65] * f
        acc = a if acc is None else acc + a
        mass = w if mass is None else mass + w
    return acc, top, mass


def stats(top, mass):
    lane = lax.broadcasted_iota(jnp.int32, (top.shape[0], 128), 1)
    return jnp.where(lane < 64, top, mass)


def attend_out_body(
        dims, ctx_ref, q_ref, qr_ref, cn_ref, kn_ref, x_ref, c_hbm, kr_hbm, uv_hbm, wo_hbm, out_ref,
        c_buf, kr_buf, s_ref, wo_buf, uv_raw, uv_ref, acc_buf, recv_a, comb, recv_b, own_b, olat_ref, o_ref,
        po_ref, half_ref, quart_ref, fin_ref, xo_ref,
        c_sem, uv_sem, wo_sem, sa_sem, ra_sem, sb_sem, rb_sem, h_sem, q_sem, f_sem, g_sem):
    n_req, heads, latent, t_dev, t_chunk, n_slots, n_split, scale, v_dim, d_model, wo_cols = dims
    me = lax.axis_index('cp')
    core = lax.rem(me, 2)
    chip = me // 2
    partner = chip * 2 + (1 - core)
    hp = heads // 2
    hs = heads // 8
    my_head = core * hp + chip * hs
    half_cols = d_model // 2
    qcols = d_model // 8
    n_wo = d_model // wo_cols

    def peer_chip(d):
        return lax.rem(chip + d, 4)

    def peer(d):
        return peer_chip(d) * 2 + core

    def c_copies(b):
        slot = lax.rem(b, n_slots)
        step = t_dev // n_split
        out = []
        for i in range(n_split):
            sl = pl.ds(i * step, step)
            out.append(pltpu.make_async_copy(c_hbm.at[b, sl], c_buf.at[slot, sl], c_sem.at[slot, i]))
        out.append(pltpu.make_async_copy(kr_hbm.at[b], kr_buf.at[slot], c_sem.at[slot, n_split]))
        return out

    def wo_copy(i):
        cols = pl.ds(pl.multiple_of(i * wo_cols, wo_cols), wo_cols)
        rows = pl.ds(pl.multiple_of(my_head * v_dim, hs * v_dim), hs * v_dim)
        return pltpu.make_async_copy(wo_hbm.at[rows, cols], wo_buf.at[:, cols], wo_sem.at[i])

    uv_copy = pltpu.make_async_copy(uv_hbm.at[:, pl.ds(pl.multiple_of(my_head, hs), hs), :], uv_raw, uv_sem)
    uv_copy.start()
    for b in range(n_slots - 1):
        for cp in c_copies(b):
            cp.start()

    barrier = pltpu.get_barrier_semaphore()
    pl.semaphore_signal(barrier, inc=1, device_id={'cp': partner}, device_id_type=pl.DeviceIdType.MESH)
    for d in (1, 2, 3):
        pl.semaphore_signal(barrier, inc=1, device_id={'cp': peer(d)}, device_id_type=pl.DeviceIdType.MESH)
    pl.semaphore_wait(barrier, 4)

    uv_copy.wait()
    grp = s_ref.shape[0] // latent
    for g in range(hs // grp):
        s_ref[...] = uv_raw[:, g * grp:(g + 1) * grp, :].astype(jnp.float32).reshape(latent * grp, v_dim)
        for h in range(grp):
            uv_ref[g * grp + h] = s_ref[pl.ds(h, latent, stride=grp), :].astype(jnp.bfloat16)

    def send_a(b):
        slot = lax.rem(b, 2)
        return exchange(acc_buf.at[slot, pl.ds(pl.multiple_of((1 - core) * hp, hp), hp)], recv_a.at[b], sa_sem.at[b], ra_sem.at[b], partner)

    def send_b(b, d):
        slot = lax.rem(b, 2)
        return exchange(comb.at[slot, pl.ds(pl.multiple_of(peer_chip(d) * hs, hs), hs)], recv_b.at[b, d - 1], sb_sem.at[b, d - 1],
                        rb_sem.at[b, d - 1], peer(d))

    def pair_merge(b):
        slot = lax.rem(b, 2)
        send_a(b).wait_recv()
        mine = acc_buf[slot, pl.ds(pl.multiple_of(core * hp, hp), hp), :]
        acc, top, mass = merge([mine, recv_a[b]], latent)
        comb[slot, :, :latent] = acc
        comb[slot, :, latent:] = stats(top, mass)
        own_b[b] = comb[slot, pl.ds(pl.multiple_of(chip * hs, hs), hs), :]

    base = me * t_dev
    nt = (((1,), (1,)), ((), ()))
    n_chunks = t_dev // t_chunk
    lanes = t_chunk // 128
    k2 = scale * LOG2E

    def step(b, carry):
        slot = lax.rem(b, n_slots)

        @pl.when(b + n_slots - 1 < n_req)
        def _():
            for cp in c_copies(b + n_slots - 1):
                cp.start()

        @pl.when(b < n_wo)
        def _():
            wo_copy(b).start()

        for cp in c_copies(b):
            cp.wait()

        @pl.when(b >= 1)
        def _():
            send_a(b - 1).start()

        @pl.when(b >= 2)
        def _():
            for d in (1, 2, 3):
                send_b(b - 2, d).start()

        limit = ctx_ref[b] - base
        q = q_ref[b]
        qr = qr_ref[b]
        top = None
        for i in range(n_chunks):
            sl = pl.ds(i * t_chunk, t_chunk)
            s = lax.dot_general(q, c_buf[slot, sl, :], nt, preferred_element_type=jnp.float32)
            s = s + jnp.dot(qr, kr_buf[slot, :, sl], preferred_element_type=jnp.float32)
            pos = lax.broadcasted_iota(jnp.int32, (1, t_chunk), 1) + i * t_chunk
            s = jnp.where(pos < limit, s, MASKED)
            for j in range(lanes):
                s_ref[pl.ds((i * lanes + j) * heads, heads), :] = s[:, j * 128:(j + 1) * 128]
            cm = jnp.max(s, axis=1, keepdims=True)
            top = cm if top is None else jnp.maximum(top, cm)
        top = jnp.maximum(top, FLOOR)
        acc, mass = None, None
        for i in range(n_chunks):
            sl = pl.ds(i * t_chunk, t_chunk)
            s = jnp.concatenate([s_ref[pl.ds((i * lanes + j) * heads, heads), :] for j in range(lanes)], axis=1)
            p = jnp.exp2((s - top) * k2)
            ls = jnp.sum(p, axis=1, keepdims=True)
            mass = ls if mass is None else mass + ls
            o = jnp.dot(p.astype(jnp.bfloat16), c_buf[slot, sl, :], preferred_element_type=jnp.float32)
            acc = o if acc is None else acc + o

        @pl.when(b >= 2)
        def _():
            send_a(b - 2).wait_send()

        @pl.when(b >= 3)
        def _():
            for d in (1, 2, 3):
                send_b(b - 3, d).wait_send()

        a_slot = lax.rem(b, 2)
        acc_buf[a_slot, :, :latent] = acc
        acc_buf[a_slot, :, latent:] = stats(top * scale, mass)

        @pl.when(b >= 1)
        def _():
            pair_merge(b - 1)

        return carry

    lax.fori_loop(0, n_req, step, 0)
    last = n_req - 1
    send_a(last).start()
    for d in (1, 2, 3):
        send_b(last - 1, d).start()
    send_a(last - 1).wait_send()
    for d in (1, 2, 3):
        send_b(last - 2, d).wait_send()
    pair_merge(last)
    for d in (1, 2, 3):
        send_b(last, d).start()

    def final(b, carry):
        for d in (1, 2, 3):
            send_b(b, d).wait_recv()
        q = q_ref[b, pl.ds(pl.multiple_of(my_head, hs), hs), :].astype(jnp.float32)
        qr = qr_ref[b, pl.ds(pl.multiple_of(my_head, hs), hs), :].astype(jnp.float32)
        cn = cn_ref[pl.ds(b, 1), :]
        kn = kn_ref[pl.ds(b, 1), :]
        s_new = (jnp.sum(q * cn, axis=1, keepdims=True) + jnp.sum(qr * kn, axis=1, keepdims=True)) * scale
        parts = [own_b[b]] + [recv_b[b, d] for d in range(3)]
        tops = [p[:, latent:latent + 1] for p in parts] + [s_new]
        top = functools.reduce(jnp.maximum, tops)
        w_new = jnp.exp(s_new - top)
        mass = w_new
        acc = w_new.astype(jnp.bfloat16).astype(jnp.float32) * cn
        for p, t in zip(parts, tops):
            f = jnp.exp(t - top)
            acc = acc + p[:, :latent] * f
            mass = mass + p[:, latent + 64:latent + 65] * f
        o_lat = (acc / mass).astype(jnp.bfloat16).astype(jnp.float32)
        for j in range(latent // 128):
            olat_ref[j, pl.ds(pl.multiple_of(b * hs, hs), hs), :] = o_lat[:, j * 128:(j + 1) * 128]
        return carry

    lax.fori_loop(0, n_req, final, 0)
    send_a(last).wait_send()
    for b in (last - 1, last):
        for d in (1, 2, 3):
            send_b(b, d).wait_send()

    for h in range(hs):
        lhs = jnp.concatenate([olat_ref[j, pl.ds(h, n_req, stride=hs), :] for j in range(latent // 128)], axis=1)
        o = jnp.dot(lhs.astype(jnp.bfloat16), uv_ref[h], preferred_element_type=jnp.float32)
        o_ref[:, h * v_dim:(h + 1) * v_dim] = o.astype(jnp.bfloat16)

    def project(i, carry):
        wo_copy(i).wait()
        cols = pl.ds(pl.multiple_of(i * wo_cols, wo_cols), wo_cols)
        po_ref[:, cols] = jnp.dot(o_ref[...], wo_buf[:, cols], preferred_element_type=jnp.float32)
        return carry

    lax.fori_loop(0, n_wo, project, 0)

    to_pair = exchange(po_ref.at[:, pl.ds(pl.multiple_of((1 - core) * half_cols, half_cols), half_cols)], half_ref, h_sem.at[0], h_sem.at[1], partner)
    to_pair.start()
    to_pair.wait()
    my_half = pl.ds(pl.multiple_of(core * half_cols, half_cols), half_cols)
    half_ref[...] = half_ref[...] + po_ref[:, my_half]

    def to_quart(d):
        return exchange(half_ref.at[:, pl.ds(pl.multiple_of(peer_chip(d) * qcols, qcols), qcols)], quart_ref.at[d - 1], q_sem.at[0, d - 1],
                        q_sem.at[1, d - 1], peer(d))

    for d in (1, 2, 3):
        to_quart(d).start()
    for d in (1, 2, 3):
        to_quart(d).wait()
    mine = pl.ds(pl.multiple_of(chip * qcols, qcols), qcols)
    my_cols = pl.ds(pl.multiple_of(core * half_cols + chip * qcols, qcols), qcols)
    total = half_ref[:, mine] + quart_ref[0] + quart_ref[1] + quart_ref[2]
    fin_ref[...] = (x_ref[:, my_cols].astype(jnp.float32) + total).astype(jnp.bfloat16).astype(jnp.float32)

    def to_all(d):
        return exchange(fin_ref, xo_ref.at[:, my_cols], f_sem.at[0, d - 1], f_sem.at[1, d - 1], peer(d))

    def from_all(d):
        cols = pl.ds(pl.multiple_of(core * half_cols + lax.rem(chip + 4 - d, 4) * qcols, qcols), qcols)
        return exchange(fin_ref, xo_ref.at[:, cols], f_sem.at[0, d - 1], f_sem.at[1, d - 1], peer(d)), cols

    for d in (1, 2, 3):
        to_all(d).start()
    g0 = exchange(fin_ref, xo_ref.at[:, my_cols], g_sem.at[0, 0], g_sem.at[1, 0], partner)
    g0.start()
    fwd = [g0]
    for d in (1, 2, 3):
        got, cols = from_all(d)
        got.wait_recv()
        f = exchange(xo_ref.at[:, cols], xo_ref.at[:, cols], g_sem.at[0, d], g_sem.at[1, d], partner)
        f.start()
        fwd.append(f)
    for d in (1, 2, 3):
        to_all(d).wait_send()
    for f in fwd:
        f.wait()
    for j in range(8):
        sl = pl.ds(j * qcols, qcols)
        out_ref[:, sl] = xo_ref[:, sl].astype(jnp.bfloat16)
    out_ref[:, my_cols] = fin_ref[...].astype(jnp.bfloat16)


def attend_out(x, q_lat, q_rope, c_new, kr_new, cache_c, cache_kr_t, w_uv, w_o, ctx_len, scale):
    n_req, heads, latent = q_lat.shape
    t_dev = cache_c.shape[1]
    rope = q_rope.shape[2]
    v_dim = w_uv.shape[2]
    d_model = x.shape[1]
    n_slots, n_split, wo_cols = 3, 4, 512
    hs = heads // 8
    wide = latent + 128
    f32, bf16 = jnp.float32, jnp.bfloat16
    dims = (n_req, heads, latent, t_dev, 512, n_slots, n_split, scale, v_dim, d_model, wo_cols)
    vmem = pl.BlockSpec(memory_space=pltpu.VMEM)
    hbm = pl.BlockSpec(memory_space=pl.ANY)
    dma = pltpu.SemaphoreType.DMA
    return pl.pallas_call(
        functools.partial(attend_out_body, dims),
        out_shape=jax.ShapeDtypeStruct(x.shape, bf16),
        in_specs=[pl.BlockSpec(memory_space=pltpu.SMEM)] + [vmem] * 5 + [hbm] * 4,
        out_specs=vmem,
        scratch_shapes=[
            pltpu.VMEM((n_slots, t_dev, latent), bf16),
            pltpu.VMEM((n_slots, rope, t_dev), bf16),
            pltpu.VMEM((t_dev * heads // 128, 128), f32),
            pltpu.VMEM((hs * v_dim, d_model), bf16),
            pltpu.VMEM((latent, hs, v_dim), bf16),
            pltpu.VMEM((hs, latent, v_dim), bf16),
            pltpu.VMEM((2, heads, wide), f32),
            pltpu.VMEM((n_req, heads // 2, wide), f32),
            pltpu.VMEM((2, heads // 2, wide), f32),
            pltpu.VMEM((n_req, 3, hs, wide), f32),
            pltpu.VMEM((n_req, hs, wide), f32),
            pltpu.VMEM((latent // 128, n_req * hs, 128), f32),
            pltpu.VMEM((n_req, hs * v_dim), bf16),
            pltpu.VMEM((n_req, d_model), f32),
            pltpu.VMEM((n_req, d_model // 2), f32),
            pltpu.VMEM((3, n_req, d_model // 8), f32),
            pltpu.VMEM((n_req, d_model // 8), f32),
            pltpu.VMEM((n_req, d_model), f32),
            dma((n_slots, n_split + 1)), dma, dma((d_model // wo_cols,)),
            dma((n_req,)), dma((n_req,)), dma((n_req, 3)), dma((n_req, 3)),
            dma((2,)), dma((2, 3)), dma((2, 3)), dma((2, 4)),
        ],
        compiler_params=pltpu.CompilerParams(
            vmem_limit_bytes=67043328, collective_id=0, has_side_effects=True),
        name='attend_out',
    )(ctx_len, q_lat, q_rope, c_new.astype(f32), kr_new.astype(f32), x, cache_c, cache_kr_t, w_uv, w_o)


def solution(mesh):
    def decode_step(x, w_dq, g_q, w_uq, w_dkv, g_kv, w_uk, w_uv, w_o, cache_c, cache_kr, ctx_len):
        scale = (w_uk.shape[2] + cache_kr.shape[2]) ** -0.5
        q_lat, q_rope, c_new, kr_new = project_step(x, w_dq, g_q, w_uq, w_dkv, g_kv, w_uk, ctx_len)
        x_out = attend_out(x, q_lat, q_rope, c_new, kr_new, cache_c, jnp.swapaxes(cache_kr, 1, 2), w_uv, w_o, ctx_len, scale)
        return x_out, c_new, kr_new

    spec_rows = P('dp', None)
    spec_cache = P('dp', 'cp', None)
    in_specs = (spec_rows, P(), P(), P(), P(), P(), P(), P(), P(), spec_cache, spec_cache, P('dp'))
    out_specs = (spec_rows, spec_rows, spec_rows)
    return jax.shard_map(decode_step, mesh=mesh, in_specs=in_specs, out_specs=out_specs, check_vma=False)
```

```python
import functools

import jax
import jax.numpy as jnp
from jax import lax
from jax.experimental import pallas as pl
from jax.experimental.pallas import tpu as pltpu
from jax.sharding import PartitionSpec as P

NORM_EPS = 1e-6
ROPE_THETA = 10000.0
MASKED = -1e30
FLOOR = -1e29
LOG2E = 1.4426950408889634


def rope_tables(positions, rope_dim):
    half_dim = rope_dim // 2
    inv_freq = ROPE_THETA ** (-2.0 * jnp.arange(half_dim, dtype=jnp.float32) / rope_dim)
    angles = positions.astype(jnp.float32)[..., None] * inv_freq
    return jnp.cos(angles), jnp.sin(angles)


def exchange(src, dst, send_sem, recv_sem, peer):
    return pltpu.make_async_remote_copy(
        src_ref=src, dst_ref=dst, send_sem=send_sem, recv_sem=recv_sem,
        device_id={'cp': peer}, device_id_type=pl.DeviceIdType.MESH)


def merge(parts, latent):
    tops = [p[:, latent:latent + 1] for p in parts]
    top = functools.reduce(jnp.maximum, tops)
    acc, mass = None, None
    for p, t in zip(parts, tops):
        f = jnp.exp(t - top)
        a, w = p[:, :latent] * f, p[:, latent + 64:latent + 65] * f
        acc = a if acc is None else acc + a
        mass = w if mass is None else mass + w
    return acc, top, mass


def stats(top, mass):
    lane = lax.broadcasted_iota(jnp.int32, (top.shape[0], 128), 1)
    return jnp.where(lane < 64, top, mass)


def project_body(
        dims, x_ref, gq_ref, gkv_ref, cos_ref, sin_ref, dq_hbm, uq_hbm, dkv_hbm, uk_hbm,
        ql_ref, qr_ref, cn_ref, kr_ref,
        dq_buf, dkv_buf, uq_buf, uk_buf, w_ref, cq_ref, kv_ref, norm_ref, q_ref,
        dq_sem, dkv_sem, uq_sem, uk_sem, cs_sem, cr_sem, ks_sem, kr_sem, qs_sem, qv_sem):
    n_req, heads, latent, nope, rope, low, d_model, n_dq, n_slots, grp = dims
    me = lax.axis_index('cp')
    core = lax.rem(me, 2)
    chip = me // 2
    partner = chip * 2 + (1 - core)
    hp = heads // 2
    qcols = low // 4
    kcols = latent // 4
    n_grp = hp // grp
    wide = grp * (nope + rope)
    drows = d_model // n_dq
    f32, bf16 = jnp.float32, jnp.bfloat16
    nt = (((1,), (1,)), ((), ()))

    def peer(d):
        return lax.rem(chip + d, 4) * 2 + core

    def dq_copy(i):
        rows = pl.ds(i * drows, drows)
        return pltpu.make_async_copy(dq_hbm.at[rows, pl.ds(pl.multiple_of(chip * qcols, qcols), qcols)], dq_buf.at[rows], dq_sem.at[i])

    def dkv_copies():
        return [pltpu.make_async_copy(dkv_hbm.at[pl.ds(pl.multiple_of(chip * kcols, kcols), kcols)], dkv_buf.at[pl.ds(0, kcols)], dkv_sem.at[0]),
                pltpu.make_async_copy(dkv_hbm.at[pl.ds(latent, rope)], dkv_buf.at[pl.ds(kcols, rope)], dkv_sem.at[1])]

    def grp_copies(g):
        slot = lax.rem(g, n_slots)
        head = core * hp + g * grp
        cols = pl.ds(pl.multiple_of(head * (nope + rope), wide), wide)
        half = low // 2
        return [pltpu.make_async_copy(uq_hbm.at[pl.ds(i * half, half), cols], uq_buf.at[slot, pl.ds(i * half, half)], uq_sem.at[slot, i]) for i in (0, 1)] + [
            pltpu.make_async_copy(uk_hbm.at[:, pl.ds(pl.multiple_of(head, grp), grp), :], uk_buf.at[slot], uk_sem.at[slot])]

    for i in range(n_dq):
        dq_copy(i).start()
    for cp in dkv_copies():
        cp.start()
    for g in range(n_slots - 1):
        for cp in grp_copies(g):
            cp.start()

    barrier = pltpu.get_barrier_semaphore()
    pl.semaphore_signal(barrier, inc=1, device_id={'cp': partner}, device_id_type=pl.DeviceIdType.MESH)
    for d in (1, 2, 3):
        pl.semaphore_signal(barrier, inc=1, device_id={'cp': peer(d)}, device_id_type=pl.DeviceIdType.MESH)

    cq = None
    for i in range(n_dq):
        dq_copy(i).wait()
        part = jnp.dot(x_ref[:, i * drows:(i + 1) * drows], dq_buf[i * drows:(i + 1) * drows, :], preferred_element_type=f32)
        cq = part if cq is None else cq + part
    cq_ref[chip] = cq.astype(bf16).astype(f32)
    pl.semaphore_wait(barrier, 4)

    def send_cq(d):
        return exchange(cq_ref.at[chip], cq_ref.at[chip], cs_sem.at[d - 1], cr_sem.at[d - 1], peer(d))

    def recv_cq(d):
        frm = lax.rem(chip + 4 - d, 4)
        return exchange(cq_ref.at[frm], cq_ref.at[frm], cs_sem.at[d - 1], cr_sem.at[d - 1], peer(d))

    def send_kv(d):
        return exchange(kv_ref.at[chip], kv_ref.at[chip], ks_sem.at[d - 1], kr_sem.at[d - 1], peer(d))

    def recv_kv(d):
        frm = lax.rem(chip + 4 - d, 4)
        return exchange(kv_ref.at[frm], kv_ref.at[frm], ks_sem.at[d - 1], kr_sem.at[d - 1], peer(d))

    for d in (1, 2, 3):
        send_cq(d).start()

    for cp in dkv_copies():
        cp.wait()
    kv = lax.dot_general(x_ref[...], dkv_buf[...], nt, preferred_element_type=f32)
    kv_ref[chip] = kv[:, :kcols]
    cos, sin = cos_ref[...], sin_ref[...]

    def rotate(v):
        lo, hi = v[:, :rope // 2], v[:, rope // 2:]
        return jnp.concatenate([lo * cos - hi * sin, hi * cos + lo * sin], axis=1)

    kr_ref[...] = rotate(kv[:, kcols:kcols + rope]).astype(bf16)

    for d in (1, 2, 3):
        recv_cq(d).wait_recv()
    for d in (1, 2, 3):
        send_kv(d).start()
    total = None
    for i in range(4):
        sq = jnp.sum(cq_ref[i] * cq_ref[i], axis=1, keepdims=True)
        total = sq if total is None else total + sq
    inv = lax.rsqrt(total * (1.0 / low) + NORM_EPS)
    for i in range(4):
        norm_ref[:, i * qcols:(i + 1) * qcols] = (cq_ref[i] * inv * gq_ref[:, i * qcols:(i + 1) * qcols]).astype(bf16)

    n_lat = latent // 128

    def send_q(g):
        rows = pl.ds(pl.multiple_of((core * hp + g * grp) * n_req, grp * n_req), grp * n_req)
        return exchange(q_ref.at[:, rows], q_ref.at[:, rows], qs_sem.at[g], qv_sem.at[g], partner)

    def recv_q(g):
        rows = pl.ds(pl.multiple_of(((1 - core) * hp + g * grp) * n_req, grp * n_req), grp * n_req)
        return exchange(q_ref.at[:, rows], q_ref.at[:, rows], qs_sem.at[g], qv_sem.at[g], partner)

    def group(g, carry):
        slot = lax.rem(g, n_slots)

        @pl.when(g + n_slots - 1 < n_grp)
        def _():
            for cp in grp_copies(g + n_slots - 1):
                cp.start()

        for cp in grp_copies(g):
            cp.wait()

        @pl.when(g >= 1)
        def _():
            send_q(g - 1).start()

        q = jnp.dot(norm_ref[...], uq_buf[slot], preferred_element_type=f32).astype(bf16).astype(f32)
        w_ref[...] = uk_buf[slot].astype(f32).reshape(latent * grp, nope)
        for h in range(grp):
            at = h * (nope + rope)
            w = w_ref[pl.ds(h, latent, stride=grp), :].astype(bf16)
            lat = lax.dot_general(q[:, at:at + nope].astype(bf16), w, nt, preferred_element_type=f32)
            rows = pl.ds(pl.multiple_of((core * hp + g * grp + h) * n_req, n_req), n_req)
            for j in range(n_lat):
                q_ref[j, rows, :] = lat[:, j * 128:(j + 1) * 128]
            rot = rotate(q[:, at + nope:at + nope + rope])
            q_ref[n_lat, rows, :] = jnp.concatenate([rot, jnp.zeros((n_req, 128 - rope), f32)], axis=1)
        return carry

    lax.fori_loop(0, n_grp, group, 0)
    send_q(n_grp - 1).start()

    for d in (1, 2, 3):
        recv_kv(d).wait_recv()
    total = None
    for i in range(4):
        sq = jnp.sum(kv_ref[i] * kv_ref[i], axis=1, keepdims=True)
        total = sq if total is None else total + sq
    inv = lax.rsqrt(total * (1.0 / latent) + NORM_EPS)
    for i in range(4):
        cn_ref[:, i * kcols:(i + 1) * kcols] = (kv_ref[i] * inv * gkv_ref[:, i * kcols:(i + 1) * kcols]).astype(bf16)
    for d in (1, 2, 3):
        send_cq(d).wait_send()
        send_kv(d).wait_send()

    def settle(g, carry):
        send_q(g).wait_send()
        recv_q(g).wait_recv()
        return carry

    lax.fori_loop(0, n_grp, settle, 0)

    def emit(b, carry):
        for j in range(n_lat):
            ql_ref[b, :, j * 128:(j + 1) * 128] = q_ref[j, pl.ds(b, heads, stride=n_req), :].astype(bf16)
        qr_ref[b] = q_ref[n_lat, pl.ds(b, heads, stride=n_req), :][:, :rope].astype(bf16)
        return carry

    lax.fori_loop(0, n_req, emit, 0)


def project(x, w_dq, g_q, w_uq, w_dkv, g_kv, w_uk, ctx_len):
    n_req, d_model = x.shape
    latent, heads, nope = w_uk.shape
    rope = w_dkv.shape[1] - latent
    low = w_dq.shape[1]
    n_dq, n_slots, grp = 4, 4, 8
    f32, bf16 = jnp.float32, jnp.bfloat16
    dims = (n_req, heads, latent, nope, rope, low, d_model, n_dq, n_slots, grp)
    cos_tab, sin_tab = rope_tables(ctx_len, rope)
    vmem = pl.BlockSpec(memory_space=pltpu.VMEM)
    hbm = pl.BlockSpec(memory_space=pl.ANY)
    dma = pltpu.SemaphoreType.DMA
    wide = grp * (nope + rope)
    n_grp = heads // 2 // grp
    return pl.pallas_call(
        functools.partial(project_body, dims),
        out_shape=[
            jax.ShapeDtypeStruct((n_req, heads, latent), bf16),
            jax.ShapeDtypeStruct((n_req, heads, rope), bf16),
            jax.ShapeDtypeStruct((n_req, latent), bf16),
            jax.ShapeDtypeStruct((n_req, rope), bf16),
        ],
        in_specs=[vmem] * 5 + [hbm] * 4,
        out_specs=[vmem] * 4,
        scratch_shapes=[
            pltpu.VMEM((d_model, low // 4), bf16),
            pltpu.VMEM((latent // 4 + rope, d_model), bf16),
            pltpu.VMEM((n_slots, low, wide), bf16),
            pltpu.VMEM((n_slots, latent, grp, nope), bf16),
            pltpu.VMEM((latent * grp, nope), f32),
            pltpu.VMEM((4, n_req, low // 4), f32),
            pltpu.VMEM((4, n_req, latent // 4), f32),
            pltpu.VMEM((n_req, low), bf16),
            pltpu.VMEM((latent // 128 + 1, heads * n_req, 128), f32),
            dma((n_dq,)), dma((2,)), dma((n_slots, 2)), dma((n_slots,)),
            dma((3,)), dma((3,)), dma((3,)), dma((3,)), dma((n_grp,)), dma((n_grp,)),
        ],
        compiler_params=pltpu.CompilerParams(vmem_limit_bytes=60 * 1024 * 1024, collective_id=1, has_side_effects=True),
        name='project',
    )(x, g_q.reshape(1, low), g_kv.reshape(1, latent), cos_tab, sin_tab, w_dq, w_uq, jnp.swapaxes(w_dkv, 0, 1), w_uk)


def attend_out_body(
        dims, ctx_ref, q_ref, qr_ref, cn_ref, kn_ref, x_ref, c_hbm, kr_hbm, uv_hbm, wo_hbm, out_ref,
        c_buf, kr_buf, s_ref, wo_buf, uv_raw, uv_ref, acc_buf, recv_a, comb, recv_b, own_b, olat_ref, o_ref,
        po_ref, half_ref, quart_ref, fin_ref, xo_ref,
        c_sem, uv_sem, wo_sem, sa_sem, ra_sem, sb_sem, rb_sem, h_sem, q_sem, f_sem, g_sem):
    n_req, heads, latent, t_dev, t_chunk, n_slots, n_split, scale, v_dim, d_model, wo_cols = dims
    me = lax.axis_index('cp')
    core = lax.rem(me, 2)
    chip = me // 2
    partner = chip * 2 + (1 - core)
    hp = heads // 2
    hs = heads // 8
    my_head = core * hp + chip * hs
    half_cols = d_model // 2
    qcols = d_model // 8
    n_wo = d_model // wo_cols

    def peer_chip(d):
        return lax.rem(chip + d, 4)

    def peer(d):
        return peer_chip(d) * 2 + core

    def c_copies(b):
        slot = lax.rem(b, n_slots)
        step = t_dev // n_split
        out = []
        for i in range(n_split):
            sl = pl.ds(i * step, step)
            out.append(pltpu.make_async_copy(c_hbm.at[b, sl], c_buf.at[slot, sl], c_sem.at[slot, i]))
        out.append(pltpu.make_async_copy(kr_hbm.at[b], kr_buf.at[slot], c_sem.at[slot, n_split]))
        return out

    def wo_copy(i):
        cols = pl.ds(pl.multiple_of(i * wo_cols, wo_cols), wo_cols)
        rows = pl.ds(pl.multiple_of(my_head * v_dim, hs * v_dim), hs * v_dim)
        return pltpu.make_async_copy(wo_hbm.at[rows, cols], wo_buf.at[:, cols], wo_sem.at[i])

    uv_copy = pltpu.make_async_copy(uv_hbm.at[:, pl.ds(pl.multiple_of(my_head, hs), hs), :], uv_raw, uv_sem)
    uv_copy.start()
    for b in range(n_slots - 1):
        for cp in c_copies(b):
            cp.start()

    barrier = pltpu.get_barrier_semaphore()
    pl.semaphore_signal(barrier, inc=1, device_id={'cp': partner}, device_id_type=pl.DeviceIdType.MESH)
    for d in (1, 2, 3):
        pl.semaphore_signal(barrier, inc=1, device_id={'cp': peer(d)}, device_id_type=pl.DeviceIdType.MESH)
    pl.semaphore_wait(barrier, 4)

    uv_copy.wait()
    grp = s_ref.shape[0] // latent
    for g in range(hs // grp):
        s_ref[...] = uv_raw[:, g * grp:(g + 1) * grp, :].astype(jnp.float32).reshape(latent * grp, v_dim)
        for h in range(grp):
            uv_ref[g * grp + h] = s_ref[pl.ds(h, latent, stride=grp), :].astype(jnp.bfloat16)

    def send_a(b):
        slot = lax.rem(b, 2)
        return exchange(acc_buf.at[slot, pl.ds(pl.multiple_of((1 - core) * hp, hp), hp)], recv_a.at[b], sa_sem.at[b], ra_sem.at[b], partner)

    def send_b(b, d):
        slot = lax.rem(b, 2)
        return exchange(comb.at[slot, pl.ds(pl.multiple_of(peer_chip(d) * hs, hs), hs)], recv_b.at[b, d - 1], sb_sem.at[b, d - 1],
                        rb_sem.at[b, d - 1], peer(d))

    def pair_merge(b):
        slot = lax.rem(b, 2)
        send_a(b).wait_recv()
        mine = acc_buf[slot, pl.ds(pl.multiple_of(core * hp, hp), hp), :]
        acc, top, mass = merge([mine, recv_a[b]], latent)
        comb[slot, :, :latent] = acc
        comb[slot, :, latent:] = stats(top, mass)
        own_b[b] = comb[slot, pl.ds(pl.multiple_of(chip * hs, hs), hs), :]

    base = me * t_dev
    nt = (((1,), (1,)), ((), ()))
    n_chunks = t_dev // t_chunk
    lanes = t_chunk // 128
    k2 = scale * LOG2E

    def step(b, carry):
        slot = lax.rem(b, n_slots)

        @pl.when(b + n_slots - 1 < n_req)
        def _():
            for cp in c_copies(b + n_slots - 1):
                cp.start()

        @pl.when(b < n_wo)
        def _():
            wo_copy(b).start()

        for cp in c_copies(b):
            cp.wait()

        @pl.when(b >= 1)
        def _():
            send_a(b - 1).start()

        @pl.when(b >= 2)
        def _():
            for d in (1, 2, 3):
                send_b(b - 2, d).start()

        limit = ctx_ref[b] - base
        q = q_ref[b]
        qr = qr_ref[b]
        top = None
        for i in range(n_chunks):
            sl = pl.ds(i * t_chunk, t_chunk)
            s = lax.dot_general(q, c_buf[slot, sl, :], nt, preferred_element_type=jnp.float32)
            s = s + jnp.dot(qr, kr_buf[slot, :, sl], preferred_element_type=jnp.float32)
            pos = lax.broadcasted_iota(jnp.int32, (1, t_chunk), 1) + i * t_chunk
            s = jnp.where(pos < limit, s, MASKED)
            for j in range(lanes):
                s_ref[pl.ds((i * lanes + j) * heads, heads), :] = s[:, j * 128:(j + 1) * 128]
            cm = jnp.max(s, axis=1, keepdims=True)
            top = cm if top is None else jnp.maximum(top, cm)
        top = jnp.maximum(top, FLOOR)
        acc, mass = None, None
        for i in range(n_chunks):
            sl = pl.ds(i * t_chunk, t_chunk)
            s = jnp.concatenate([s_ref[pl.ds((i * lanes + j) * heads, heads), :] for j in range(lanes)], axis=1)
            p = jnp.exp2((s - top) * k2)
            ls = jnp.sum(p, axis=1, keepdims=True)
            mass = ls if mass is None else mass + ls
            o = jnp.dot(p.astype(jnp.bfloat16), c_buf[slot, sl, :], preferred_element_type=jnp.float32)
            acc = o if acc is None else acc + o

        @pl.when(b >= 2)
        def _():
            send_a(b - 2).wait_send()

        @pl.when(b >= 3)
        def _():
            for d in (1, 2, 3):
                send_b(b - 3, d).wait_send()

        a_slot = lax.rem(b, 2)
        acc_buf[a_slot, :, :latent] = acc
        acc_buf[a_slot, :, latent:] = stats(top * scale, mass)

        @pl.when(b >= 1)
        def _():
            pair_merge(b - 1)

        return carry

    lax.fori_loop(0, n_req, step, 0)
    last = n_req - 1
    send_a(last).start()
    for d in (1, 2, 3):
        send_b(last - 1, d).start()
    send_a(last - 1).wait_send()
    for d in (1, 2, 3):
        send_b(last - 2, d).wait_send()
    pair_merge(last)
    for d in (1, 2, 3):
        send_b(last, d).start()

    def final(b, carry):
        for d in (1, 2, 3):
            send_b(b, d).wait_recv()
        q = q_ref[b, pl.ds(pl.multiple_of(my_head, hs), hs), :].astype(jnp.float32)
        qr = qr_ref[b, pl.ds(pl.multiple_of(my_head, hs), hs), :].astype(jnp.float32)
        cn = cn_ref[pl.ds(b, 1), :]
        kn = kn_ref[pl.ds(b, 1), :]
        s_new = (jnp.sum(q * cn, axis=1, keepdims=True) + jnp.sum(qr * kn, axis=1, keepdims=True)) * scale
        parts = [own_b[b]] + [recv_b[b, d] for d in range(3)]
        tops = [p[:, latent:latent + 1] for p in parts] + [s_new]
        top = functools.reduce(jnp.maximum, tops)
        w_new = jnp.exp(s_new - top)
        mass = w_new
        acc = w_new.astype(jnp.bfloat16).astype(jnp.float32) * cn
        for p, t in zip(parts, tops):
            f = jnp.exp(t - top)
            acc = acc + p[:, :latent] * f
            mass = mass + p[:, latent + 64:latent + 65] * f
        o_lat = (acc / mass).astype(jnp.bfloat16).astype(jnp.float32)
        for j in range(latent // 128):
            olat_ref[j, pl.ds(pl.multiple_of(b * hs, hs), hs), :] = o_lat[:, j * 128:(j + 1) * 128]
        return carry

    lax.fori_loop(0, n_req, final, 0)
    send_a(last).wait_send()
    for b in (last - 1, last):
        for d in (1, 2, 3):
            send_b(b, d).wait_send()

    for h in range(hs):
        lhs = jnp.concatenate([olat_ref[j, pl.ds(h, n_req, stride=hs), :] for j in range(latent // 128)], axis=1)
        o = jnp.dot(lhs.astype(jnp.bfloat16), uv_ref[h], preferred_element_type=jnp.float32)
        o_ref[:, h * v_dim:(h + 1) * v_dim] = o.astype(jnp.bfloat16)

    def project(i, carry):
        wo_copy(i).wait()
        cols = pl.ds(pl.multiple_of(i * wo_cols, wo_cols), wo_cols)
        po_ref[:, cols] = jnp.dot(o_ref[...], wo_buf[:, cols], preferred_element_type=jnp.float32)
        return carry

    lax.fori_loop(0, n_wo, project, 0)

    to_pair = exchange(po_ref.at[:, pl.ds(pl.multiple_of((1 - core) * half_cols, half_cols), half_cols)], half_ref, h_sem.at[0], h_sem.at[1], partner)
    to_pair.start()
    to_pair.wait()
    my_half = pl.ds(pl.multiple_of(core * half_cols, half_cols), half_cols)
    half_ref[...] = half_ref[...] + po_ref[:, my_half]

    def to_quart(d):
        return exchange(half_ref.at[:, pl.ds(pl.multiple_of(peer_chip(d) * qcols, qcols), qcols)], quart_ref.at[d - 1], q_sem.at[0, d - 1],
                        q_sem.at[1, d - 1], peer(d))

    for d in (1, 2, 3):
        to_quart(d).start()
    for d in (1, 2, 3):
        to_quart(d).wait()
    mine = pl.ds(pl.multiple_of(chip * qcols, qcols), qcols)
    my_cols = pl.ds(pl.multiple_of(core * half_cols + chip * qcols, qcols), qcols)
    total = half_ref[:, mine] + quart_ref[0] + quart_ref[1] + quart_ref[2]
    fin_ref[...] = (x_ref[:, my_cols].astype(jnp.float32) + total).astype(jnp.bfloat16).astype(jnp.float32)

    def to_all(d):
        return exchange(fin_ref, xo_ref.at[:, my_cols], f_sem.at[0, d - 1], f_sem.at[1, d - 1], peer(d))

    def from_all(d):
        cols = pl.ds(pl.multiple_of(core * half_cols + lax.rem(chip + 4 - d, 4) * qcols, qcols), qcols)
        return exchange(fin_ref, xo_ref.at[:, cols], f_sem.at[0, d - 1], f_sem.at[1, d - 1], peer(d)), cols

    for d in (1, 2, 3):
        to_all(d).start()
    g0 = exchange(fin_ref, xo_ref.at[:, my_cols], g_sem.at[0, 0], g_sem.at[1, 0], partner)
    g0.start()
    fwd = [g0]
    for d in (1, 2, 3):
        got, cols = from_all(d)
        got.wait_recv()
        f = exchange(xo_ref.at[:, cols], xo_ref.at[:, cols], g_sem.at[0, d], g_sem.at[1, d], partner)
        f.start()
        fwd.append(f)
    for d in (1, 2, 3):
        to_all(d).wait_send()
    for f in fwd:
        f.wait()
    for j in range(8):
        sl = pl.ds(j * qcols, qcols)
        out_ref[:, sl] = xo_ref[:, sl].astype(jnp.bfloat16)
    out_ref[:, my_cols] = fin_ref[...].astype(jnp.bfloat16)


def attend_out(x, q_lat, q_rope, c_new, kr_new, cache_c, cache_kr_t, w_uv, w_o, ctx_len, scale):
    n_req, heads, latent = q_lat.shape
    t_dev = cache_c.shape[1]
    rope = q_rope.shape[2]
    v_dim = w_uv.shape[2]
    d_model = x.shape[1]
    n_slots, n_split, wo_cols = 3, 4, 512
    hs = heads // 8
    wide = latent + 128
    f32, bf16 = jnp.float32, jnp.bfloat16
    dims = (n_req, heads, latent, t_dev, 512, n_slots, n_split, scale, v_dim, d_model, wo_cols)
    vmem = pl.BlockSpec(memory_space=pltpu.VMEM)
    hbm = pl.BlockSpec(memory_space=pl.ANY)
    dma = pltpu.SemaphoreType.DMA
    return pl.pallas_call(
        functools.partial(attend_out_body, dims),
        out_shape=jax.ShapeDtypeStruct(x.shape, bf16),
        in_specs=[pl.BlockSpec(memory_space=pltpu.SMEM)] + [vmem] * 5 + [hbm] * 4,
        out_specs=vmem,
        scratch_shapes=[
            pltpu.VMEM((n_slots, t_dev, latent), bf16),
            pltpu.VMEM((n_slots, rope, t_dev), bf16),
            pltpu.VMEM((t_dev * heads // 128, 128), f32),
            pltpu.VMEM((hs * v_dim, d_model), bf16),
            pltpu.VMEM((latent, hs, v_dim), bf16),
            pltpu.VMEM((hs, latent, v_dim), bf16),
            pltpu.VMEM((2, heads, wide), f32),
            pltpu.VMEM((n_req, heads // 2, wide), f32),
            pltpu.VMEM((2, heads // 2, wide), f32),
            pltpu.VMEM((n_req, 3, hs, wide), f32),
            pltpu.VMEM((n_req, hs, wide), f32),
            pltpu.VMEM((latent // 128, n_req * hs, 128), f32),
            pltpu.VMEM((n_req, hs * v_dim), bf16),
            pltpu.VMEM((n_req, d_model), f32),
            pltpu.VMEM((n_req, d_model // 2), f32),
            pltpu.VMEM((3, n_req, d_model // 8), f32),
            pltpu.VMEM((n_req, d_model // 8), f32),
            pltpu.VMEM((n_req, d_model), f32),
            dma((n_slots, n_split + 1)), dma, dma((d_model // wo_cols,)),
            dma((n_req,)), dma((n_req,)), dma((n_req, 3)), dma((n_req, 3)),
            dma((2,)), dma((2, 3)), dma((2, 3)), dma((2, 4)),
        ],
        compiler_params=pltpu.CompilerParams(
            vmem_limit_bytes=67043328, collective_id=0, has_side_effects=True),
        name='attend_out',
    )(ctx_len, q_lat, q_rope, c_new.astype(f32), kr_new.astype(f32), x, cache_c, cache_kr_t, w_uv, w_o)


def solution(mesh):
    def decode_step(x, w_dq, g_q, w_uq, w_dkv, g_kv, w_uk, w_uv, w_o, cache_c, cache_kr, ctx_len):
        scale = (w_uk.shape[2] + cache_kr.shape[2]) ** -0.5
        q_lat, q_rope, c_new, kr_new = project(x, w_dq, g_q, w_uq, w_dkv, g_kv, w_uk, ctx_len)
        x_out = attend_out(x, q_lat, q_rope, c_new, kr_new, cache_c, jnp.swapaxes(cache_kr, 1, 2), w_uv, w_o, ctx_len, scale)
        return x_out, c_new, kr_new

    spec_rows = P('dp', None)
    spec_cache = P('dp', 'cp', None)
    in_specs = (spec_rows, P(), P(), P(), P(), P(), P(), P(), P(), spec_cache, spec_cache, P('dp'))
    out_specs = (spec_rows, spec_rows, spec_rows)
    return jax.shard_map(decode_step, mesh=mesh, in_specs=in_specs, out_specs=out_specs, check_vma=False)
```

```python
import functools

import jax
import jax.numpy as jnp
from jax import lax
from jax.experimental import pallas as pl
from jax.experimental.pallas import tpu as pltpu
from jax.sharding import PartitionSpec as P

NORM_EPS = 1e-6
ROPE_THETA = 10000.0
MASKED = -1e30
FLOOR = -1e29
LOG2E = 1.4426950408889634


def exchange(src, dst, send_sem, recv_sem, peer):
    return pltpu.make_async_remote_copy(
        src_ref=src, dst_ref=dst, send_sem=send_sem, recv_sem=recv_sem,
        device_id={'cp': peer}, device_id_type=pl.DeviceIdType.MESH)


def merge(parts, latent):
    tops = [p[:, latent:latent + 1] for p in parts]
    top = functools.reduce(jnp.maximum, tops)
    acc, mass = None, None
    for p, t in zip(parts, tops):
        f = jnp.exp(t - top)
        a, w = p[:, :latent] * f, p[:, latent + 64:latent + 65] * f
        acc = a if acc is None else acc + a
        mass = w if mass is None else mass + w
    return acc, top, mass


def stats(top, mass):
    lane = lax.broadcasted_iota(jnp.int32, (top.shape[0], 128), 1)
    return jnp.where(lane < 64, top, mass)


def decode_body(
        dims, ctx_ref, x_ref, gq_ref, gkv_ref, tab_ref, dq_hbm, uq_hbm, dkv_hbm, uk_hbm, c_hbm, kr_hbm, uv_hbm, wo_hbm, out_ref,
        wo_buf, uk_buf, s_ref, turn_ref, cq_ref, kv_ref, norm_ref, q_ref, cn_ref, kn_ref,
        c_buf, kr_buf, acc_buf, recv_a, comb, recv_b, own_b, olat_ref, o_ref,
        po_ref, pair_ref, sum_ref, quart_ref, fin_ref, xo_ref,
        dq_sem, dkv_sem, uq_sem, uk_sem, cs_sem, cr_sem, ks_sem, kr_sem, qs_sem, qv_sem,
        c_sem, uv_sem, wo_sem, sa_sem, ra_sem, sb_sem, rb_sem, h_sem, p_sem, f_sem, g_sem):
    (n_req, heads, latent, nope, rope, v_dim, low, d_model, t_dev, t_chunk, n_dq, n_kv, n_uq, n_uk, grp, n_slots, n_split, scale) = dims
    f32, bf16 = jnp.float32, jnp.bfloat16
    nt = (((1,), (1,)), ((), ()))
    me = lax.axis_index('cp')
    core = lax.rem(me, 2)
    chip = me // 2
    partner = chip * 2 + (1 - core)
    hp = heads // 2
    hs = heads // 8
    my_head = core * hp + chip * hs
    n_lat = latent // 128
    lcols = low // 4
    kcols = latent // 4
    n_grp = hp // grp
    wide = grp * (nope + rope)
    drows = d_model // n_dq
    kdepth = d_model // n_kv
    krows = kcols + rope
    half_cols = d_model // 2
    qcols = d_model // 8
    n_wo = 8

    def peer_chip(d):
        return lax.rem(chip + d, 4)

    def from_chip(d):
        return lax.rem(chip + 4 - d, 4)

    def peer(d):
        return peer_chip(d) * 2 + core

    def dq_piece(i):
        return wo_buf.at[pl.ds(low, drows), pl.ds(i * lcols, lcols)]

    def dq_copy(i):
        return pltpu.make_async_copy(dq_hbm.at[pl.ds(i * drows, drows), pl.ds(pl.multiple_of(chip * lcols, lcols), lcols)], dq_piece(i), dq_sem.at[i])

    def kv_piece(i, row, rows):
        return wo_buf.at[pl.ds(i * krows + row, rows), pl.ds(n_uq * wide, kdepth)]

    def dkv_copies(i):
        cols = pl.ds(i * kdepth, kdepth)
        return [pltpu.make_async_copy(dkv_hbm.at[pl.ds(pl.multiple_of(chip * kcols, kcols), kcols), cols], kv_piece(i, 0, kcols), dkv_sem.at[0, i]),
                pltpu.make_async_copy(dkv_hbm.at[pl.ds(latent, rope), cols], kv_piece(i, kcols, rope), dkv_sem.at[1, i])]

    def uq_slot(g):
        return pl.ds(pl.multiple_of(lax.rem(g, n_uq) * wide, wide), wide)

    def grp_copies(g):
        head = core * hp + g * grp
        cols = pl.ds(pl.multiple_of(head * (nope + rope), wide), wide)
        half = low // 2
        slot = lax.rem(g, n_uq)
        return [pltpu.make_async_copy(uq_hbm.at[pl.ds(i * half, half), cols], wo_buf.at[pl.ds(i * half, half), uq_slot(g)], uq_sem.at[slot, i])
                for i in (0, 1)] + [
            pltpu.make_async_copy(uk_hbm.at[:, pl.ds(pl.multiple_of(head, grp), grp), :], uk_buf.at[lax.rem(g, n_uk)], uk_sem.at[lax.rem(g, n_uk)])]

    def c_copies(b):
        slot = lax.rem(b, n_slots)
        rows = t_dev // n_split
        out = []
        for i in range(n_split):
            sl = pl.ds(i * rows, rows)
            out.append(pltpu.make_async_copy(c_hbm.at[b, sl], c_buf.at[slot, sl], c_sem.at[slot, i]))
        out.append(pltpu.make_async_copy(kr_hbm.at[b], kr_buf.at[slot], c_sem.at[slot, n_split]))
        return out

    def uv_copy(i):
        return pltpu.make_async_copy(uv_hbm.at[:, pl.ds(pl.multiple_of(my_head + i * grp, grp), grp), :], uk_buf.at[i], uv_sem.at[i])

    def wo_block(i):
        half = jnp.where(i < 4, 1 - core, core)
        return half * half_cols + lax.rem(chip + 1 + i, 4) * qcols

    def wo_slot(i):
        return pl.ds(pl.multiple_of(i * qcols, qcols), qcols)

    def wo_copy(i):
        rows = pl.ds(pl.multiple_of(my_head * v_dim, hs * v_dim), hs * v_dim)
        return pltpu.make_async_copy(wo_hbm.at[rows, pl.ds(pl.multiple_of(wo_block(i), qcols), qcols)], wo_buf.at[:, wo_slot(i)], wo_sem.at[i])

    for i in range(n_dq):
        dq_copy(i).start()
    for i in range(n_kv):
        for cp in dkv_copies(i):
            cp.start()
    for g in range(n_uk - 1):
        for cp in grp_copies(g):
            cp.start()

    barrier = pltpu.get_barrier_semaphore()
    pl.semaphore_signal(barrier, inc=1, device_id={'cp': partner}, device_id_type=pl.DeviceIdType.MESH)
    for d in (1, 2, 3):
        pl.semaphore_signal(barrier, inc=1, device_id={'cp': peer(d)}, device_id_type=pl.DeviceIdType.MESH)

    cq = None
    for i in range(n_dq):
        dq_copy(i).wait()
        part = jnp.dot(x_ref[:, i * drows:(i + 1) * drows], wo_buf[low:low + drows, i * lcols:(i + 1) * lcols], preferred_element_type=f32)
        cq = part if cq is None else cq + part
    cq_ref[chip] = cq.astype(bf16).astype(f32)
    pl.semaphore_wait(barrier, 4)

    def send_cq(d):
        return exchange(cq_ref.at[chip], cq_ref.at[chip], cs_sem.at[d - 1], cr_sem.at[d - 1], peer(d))

    def recv_cq(d):
        return exchange(cq_ref.at[from_chip(d)], cq_ref.at[from_chip(d)], cs_sem.at[d - 1], cr_sem.at[d - 1], peer(d))

    def send_kv(d):
        return exchange(kv_ref.at[chip], kv_ref.at[chip], ks_sem.at[d - 1], kr_sem.at[d - 1], peer(d))

    def recv_kv(d):
        return exchange(kv_ref.at[from_chip(d)], kv_ref.at[from_chip(d)], ks_sem.at[d - 1], kr_sem.at[d - 1], peer(d))

    for d in (1, 2, 3):
        send_cq(d).start()

    kv = None
    for i in range(n_kv):
        for cp in dkv_copies(i):
            cp.wait()
        part = lax.dot_general(x_ref[:, i * kdepth:(i + 1) * kdepth], wo_buf[i * krows:(i + 1) * krows, n_uq * wide:n_uq * wide + kdepth],
                               nt, preferred_element_type=f32)
        kv = part if kv is None else kv + part
    kv_ref[chip] = kv[:, :kcols]
    cos, sin = tab_ref[:, :rope // 2], tab_ref[:, rope // 2:]

    def rotate(v):
        lo, hi = v[:, :rope // 2], v[:, rope // 2:]
        return jnp.concatenate([lo * cos - hi * sin, hi * cos + lo * sin], axis=1)

    kn_ref[...] = rotate(kv[:, kcols:kcols + rope]).astype(bf16).astype(f32)

    for d in (1, 2, 3):
        recv_cq(d).wait_recv()
    for d in (1, 2, 3):
        send_kv(d).start()

    def rms(parts):
        total = None
        for p in parts:
            sq = jnp.sum(p * p, axis=1, keepdims=True)
            total = sq if total is None else total + sq
        return lax.rsqrt(total * (1.0 / (len(parts) * parts[0].shape[1])) + NORM_EPS)

    inv = rms([cq_ref[i] for i in range(4)])
    for i in range(4):
        norm_ref[:, i * lcols:(i + 1) * lcols] = (cq_ref[i] * inv * gq_ref[:, i * lcols:(i + 1) * lcols]).astype(bf16)

    def q_rows(c, g):
        return pl.ds(pl.multiple_of((c * hp + g * grp) * n_req, grp * n_req), grp * n_req)

    def send_q(g):
        return exchange(q_ref.at[:, q_rows(core, g)], q_ref.at[:, q_rows(core, g)], qs_sem.at[g], qv_sem.at[g], partner)

    def recv_q(g):
        return exchange(q_ref.at[:, q_rows(1 - core, g)], q_ref.at[:, q_rows(1 - core, g)], qs_sem.at[g], qv_sem.at[g], partner)

    def group(g, carry):
        @pl.when(g + n_uk - 1 < n_grp)
        def _():
            for cp in grp_copies(g + n_uk - 1):
                cp.start()

        @pl.when(g >= n_grp - (n_slots - 1))
        def _():
            for cp in c_copies(g - (n_grp - (n_slots - 1))):
                cp.start()

        for cp in grp_copies(g):
            cp.wait()

        @pl.when(g >= 1)
        def _():
            send_q(g - 1).start()

        q = jnp.dot(norm_ref[...], wo_buf[:low, uq_slot(g)], preferred_element_type=f32).astype(bf16).astype(f32)
        s_ref[...] = uk_buf[lax.rem(g, n_uk)].astype(f32).reshape(latent * grp, nope)
        for h in range(grp):
            at = h * (nope + rope)
            turn_ref[h % 2, :nope, :] = s_ref[pl.ds(h, latent, stride=grp), :].astype(bf16).T
            lat = jnp.dot(q[:, at:at + nope].astype(bf16), turn_ref[h % 2, :nope, :], preferred_element_type=f32)
            rows = pl.ds(pl.multiple_of((core * hp + g * grp + h) * n_req, n_req), n_req)
            for j in range(n_lat):
                q_ref[j, rows, :] = lat[:, j * 128:(j + 1) * 128]
            rot = rotate(q[:, at + nope:at + nope + rope])
            q_ref[n_lat, rows, :] = jnp.concatenate([rot, jnp.zeros((n_req, 128 - rope), f32)], axis=1)
        return carry

    lax.fori_loop(0, n_grp, group, 0)
    send_q(n_grp - 1).start()

    for d in (1, 2, 3):
        recv_kv(d).wait_recv()
    inv = rms([kv_ref[i] for i in range(4)])
    for i in range(4):
        cn_ref[:, i * kcols:(i + 1) * kcols] = (kv_ref[i] * inv * gkv_ref[:, i * kcols:(i + 1) * kcols]).astype(bf16).astype(f32)
    for d in (1, 2, 3):
        send_cq(d).wait_send()
        send_kv(d).wait_send()

    def settle(g, carry):
        recv_q(g).wait_recv()
        return carry

    lax.fori_loop(0, n_grp, settle, 0)

    def send_a(b):
        slot = lax.rem(b, 2)
        return exchange(acc_buf.at[slot, pl.ds(pl.multiple_of((1 - core) * hp, hp), hp)], recv_a.at[slot], sa_sem.at[b], ra_sem.at[b], partner)

    def send_b(b, d):
        slot = lax.rem(b, 2)
        return exchange(comb.at[slot, pl.ds(pl.multiple_of(peer_chip(d) * hs, hs), hs)], recv_b.at[b, d - 1], sb_sem.at[b, d - 1],
                        rb_sem.at[b, d - 1], peer(d))

    def pair_merge(b):
        slot = lax.rem(b, 2)
        send_a(b).wait_recv()
        mine = acc_buf[slot, pl.ds(pl.multiple_of(core * hp, hp), hp), :]
        acc, top, mass = merge([mine, recv_a[slot]], latent)
        comb[slot, :, :latent] = acc
        comb[slot, :, latent:] = stats(top, mass)
        own_b[b] = comb[slot, pl.ds(pl.multiple_of(chip * hs, hs), hs), :]

    base = me * t_dev
    n_chunks = t_dev // t_chunk
    lanes = t_chunk // 128
    k2 = scale * LOG2E

    def step(b, carry):
        slot = lax.rem(b, n_slots)

        @pl.when(b + n_slots - 1 < n_req)
        def _():
            for cp in c_copies(b + n_slots - 1):
                cp.start()

        @pl.when(b < n_wo)
        def _():
            wo_copy(b).start()

        @pl.when(b == n_wo)
        def _():
            for i in range(hs // grp):
                uv_copy(i).start()

        for cp in c_copies(b):
            cp.wait()

        @pl.when(b >= 1)
        def _():
            send_a(b - 1).start()

        @pl.when(b >= 2)
        def _():
            for d in (1, 2, 3):
                send_b(b - 2, d).start()

        limit = ctx_ref[b] - base
        q = jnp.concatenate([q_ref[j, pl.ds(b, heads, stride=n_req), :].astype(bf16) for j in range(n_lat)], axis=1)
        qr = q_ref[n_lat, pl.ds(b, heads, stride=n_req), :][:, :rope].astype(bf16)
        top = None
        for i in range(n_chunks):
            sl = pl.ds(i * t_chunk, t_chunk)
            turn_ref[i % 2] = c_buf[slot, sl, :].T
            s = jnp.dot(q, turn_ref[i % 2], preferred_element_type=f32)
            s = s + jnp.dot(qr, kr_buf[slot, :, sl], preferred_element_type=f32)
            pos = lax.broadcasted_iota(jnp.int32, (1, t_chunk), 1) + i * t_chunk
            s = jnp.where(pos < limit, s, MASKED)
            for j in range(lanes):
                s_ref[pl.ds((i * lanes + j) * heads, heads), :] = s[:, j * 128:(j + 1) * 128]
            cm = jnp.max(s, axis=1, keepdims=True)
            top = cm if top is None else jnp.maximum(top, cm)
        top = jnp.maximum(top, FLOOR)
        acc, mass = None, None
        for i in range(n_chunks):
            sl = pl.ds(i * t_chunk, t_chunk)
            s = jnp.concatenate([s_ref[pl.ds((i * lanes + j) * heads, heads), :] for j in range(lanes)], axis=1)
            p = jnp.exp2((s - top) * k2)
            ls = jnp.sum(p, axis=1, keepdims=True)
            mass = ls if mass is None else mass + ls
            o = jnp.dot(p.astype(bf16), c_buf[slot, sl, :], preferred_element_type=f32)
            acc = o if acc is None else acc + o

        @pl.when(b >= 2)
        def _():
            send_a(b - 2).wait_send()

        @pl.when(b >= 3)
        def _():
            for d in (1, 2, 3):
                send_b(b - 3, d).wait_send()

        a_slot = lax.rem(b, 2)
        acc_buf[a_slot, :, :latent] = acc
        acc_buf[a_slot, :, latent:] = stats(top * scale, mass)

        @pl.when(b >= 1)
        def _():
            pair_merge(b - 1)

        return carry

    lax.fori_loop(0, n_req, step, 0)

    def final(b, carry):
        for d in (1, 2, 3):
            send_b(b, d).wait_recv()
        rows = pl.ds(my_head * n_req + b, hs, stride=n_req)
        cn = cn_ref[pl.ds(b, 1), :]
        s_new = jnp.sum(q_ref[n_lat, rows, :][:, :rope].astype(bf16).astype(f32) * kn_ref[pl.ds(b, 1), :], axis=1, keepdims=True)
        for j in range(n_lat):
            s_new = s_new + jnp.sum(q_ref[j, rows, :].astype(bf16).astype(f32) * cn[:, j * 128:(j + 1) * 128], axis=1, keepdims=True)
        s_new = s_new * scale
        parts = [own_b[b]] + [recv_b[b, d] for d in range(3)]
        tops = [p[:, latent:latent + 1] for p in parts] + [s_new]
        top = functools.reduce(jnp.maximum, tops)
        w_new = jnp.exp(s_new - top)
        mass = w_new
        acc = w_new.astype(bf16).astype(f32) * cn
        for p, t in zip(parts, tops):
            f = jnp.exp(t - top)
            acc = acc + p[:, :latent] * f
            mass = mass + p[:, latent + 64:latent + 65] * f
        o_lat = (acc / mass).astype(bf16).astype(f32)
        for j in range(n_lat):
            olat_ref[j, pl.ds(pl.multiple_of(b * hs, hs), hs), :] = o_lat[:, j * 128:(j + 1) * 128]
        return carry

    last = n_req - 1
    send_a(last).start()
    for d in (1, 2, 3):
        send_b(last - 1, d).start()
    lax.fori_loop(0, last - 1, final, 0)
    send_a(last - 1).wait_send()
    for d in (1, 2, 3):
        send_b(last - 2, d).wait_send()
    pair_merge(last)
    for i in range(hs // grp):
        uv_copy(i).wait()
        s_ref[...] = uk_buf[i].astype(f32).reshape(latent * grp, v_dim)
        if i == 0:
            for d in (1, 2, 3):
                send_b(last, d).start()
        for h in range(grp):
            c_buf[0, h * latent:(h + 1) * latent, i * v_dim:(i + 1) * v_dim] = s_ref[pl.ds(h, latent, stride=grp), :].astype(bf16)
    lax.fori_loop(last - 1, n_req, final, 0)
    send_a(last).wait_send()
    for b in (last - 1, last):
        for d in (1, 2, 3):
            send_b(b, d).wait_send()

    for h in range(hs):
        lhs = jnp.concatenate([olat_ref[j, pl.ds(h, n_req, stride=hs), :] for j in range(n_lat)], axis=1)
        uv = c_buf[0, (h % grp) * latent:(h % grp + 1) * latent, (h // grp) * v_dim:(h // grp + 1) * v_dim]
        o = jnp.dot(lhs.astype(bf16), uv, preferred_element_type=f32)
        o_ref[:, h * v_dim:(h + 1) * v_dim] = o.astype(bf16)

    def block(i):
        wo_copy(i).wait()
        return jnp.dot(o_ref[...], wo_buf[:, wo_slot(i)], preferred_element_type=f32)

    def to_pair(i):
        return exchange(po_ref.at[i], pair_ref.at[i], h_sem.at[0, i], h_sem.at[1, i], partner)

    def to_owner(i):
        return exchange(sum_ref.at[i], quart_ref.at[i], p_sem.at[0, i], p_sem.at[1, i], peer(i + 1))

    def first(i, carry):
        po_ref[i] = block(i)

        @pl.when(i >= 1)
        def _():
            to_pair(i - 1).start()

        return carry

    lax.fori_loop(0, 4, first, 0)
    to_pair(3).start()

    def second(i, carry):
        part = block(i + 4)
        to_pair(i).wait_recv()
        sum_ref[i] = part + pair_ref[i]

        @pl.when((i >= 1) & (i < 4))
        def _():
            to_owner(i - 1).start()

        return carry

    lax.fori_loop(0, 4, second, 0)
    for i in range(3):
        to_owner(i).wait_recv()
    my_cols = pl.ds(pl.multiple_of(core * half_cols + chip * qcols, qcols), qcols)
    total = sum_ref[3] + quart_ref[0] + quart_ref[1] + quart_ref[2]
    fin_ref[...] = (x_ref[:, my_cols].astype(f32) + total).astype(bf16).astype(f32)

    def to_all(d):
        return exchange(fin_ref, xo_ref.at[:, my_cols], f_sem.at[0, d - 1], f_sem.at[1, d - 1], peer(d))

    def from_all(d):
        cols = pl.ds(pl.multiple_of(core * half_cols + from_chip(d) * qcols, qcols), qcols)
        return exchange(fin_ref, xo_ref.at[:, cols], f_sem.at[0, d - 1], f_sem.at[1, d - 1], peer(d)), cols

    for d in (1, 2, 3):
        to_all(d).start()
    g0 = exchange(fin_ref, xo_ref.at[:, my_cols], g_sem.at[0, 0], g_sem.at[1, 0], partner)
    g0.start()
    out_ref[:, d_model:d_model + latent] = cn_ref[...]
    out_ref[:, d_model + latent:] = jnp.concatenate([kn_ref[...], jnp.zeros((n_req, 128 - rope), f32)], axis=1)
    fwd = [g0]
    for d in (1, 2, 3):
        got, cols = from_all(d)
        got.wait_recv()
        f = exchange(xo_ref.at[:, cols], xo_ref.at[:, cols], g_sem.at[0, d], g_sem.at[1, d], partner)
        f.start()
        fwd.append(f)
    for d in (1, 2, 3):
        to_all(d).wait_send()
    for i in range(3):
        to_owner(i).wait_send()
    for i in range(4):
        to_pair(i).wait_send()

    def settle_sent(g, carry):
        send_q(g).wait_send()
        return carry

    lax.fori_loop(0, n_grp, settle_sent, 0)
    for f in fwd:
        f.wait()
    xo_ref[:, my_cols] = fin_ref[...]
    out_ref[:, :d_model] = xo_ref[...]


def decode(x, w_dq, g_q, w_uq, w_dkv, g_kv, w_uk, w_uv, w_o, cache_c, cache_kr, ctx_len):
    n_req, d_model = x.shape
    latent, heads, nope = w_uk.shape
    rope = w_dkv.shape[1] - latent
    low = w_dq.shape[1]
    v_dim = w_uv.shape[2]
    t_dev = cache_c.shape[1]
    scale = (nope + rope) ** -0.5
    n_dq, n_kv, n_uq, n_uk, grp, n_slots, n_split, t_chunk = 14, 7, 4, 3, 8, 3, 4, 512
    f32, bf16 = jnp.float32, jnp.bfloat16
    dims = (n_req, heads, latent, nope, rope, v_dim, low, d_model, t_dev, t_chunk, n_dq, n_kv, n_uq, n_uk, grp, n_slots, n_split, scale)
    lane = jnp.arange(rope)
    inv_freq = ROPE_THETA ** (-2.0 * (lane % (rope // 2)).astype(f32) / rope)
    angles = ctx_len.astype(f32)[:, None] * inv_freq
    table = jnp.where(lane < rope // 2, jnp.cos(angles), jnp.sin(angles))
    hs = heads // 8
    hp = heads // 2
    tail = latent + 128
    qcols = d_model // 8
    n_grp = hp // grp
    vmem = pl.BlockSpec(memory_space=pltpu.VMEM)
    hbm = pl.BlockSpec(memory_space=pl.ANY)
    dma = pltpu.SemaphoreType.DMA
    out = pl.pallas_call(
        functools.partial(decode_body, dims),
        out_shape=jax.ShapeDtypeStruct((n_req, d_model + latent + 128), f32),
        in_specs=[pl.BlockSpec(memory_space=pltpu.SMEM)] + [vmem] * 4 + [hbm] * 8,
        out_specs=vmem,
        scratch_shapes=[
            pltpu.VMEM((hs * v_dim, d_model), bf16),
            pltpu.VMEM((n_uk, latent, grp, nope), bf16),
            pltpu.VMEM((t_dev * heads // 128, 128), f32),
            pltpu.VMEM((2, latent, t_chunk), bf16),
            pltpu.VMEM((4, n_req, low // 4), f32),
            pltpu.VMEM((4, n_req, latent // 4), f32),
            pltpu.VMEM((n_req, low), bf16),
            pltpu.VMEM((latent // 128 + 1, heads * n_req, 128), f32),
            pltpu.VMEM((n_req, latent), f32),
            pltpu.VMEM((n_req, rope), f32),
            pltpu.VMEM((n_slots, t_dev, latent), bf16),
            pltpu.VMEM((n_slots, rope, t_dev), bf16),
            pltpu.VMEM((2, heads, tail), f32),
            pltpu.VMEM((2, hp, tail), f32),
            pltpu.VMEM((2, hp, tail), f32),
            pltpu.VMEM((n_req, 3, hs, tail), f32),
            pltpu.VMEM((n_req, hs, tail), f32),
            pltpu.VMEM((latent // 128, n_req * hs, 128), f32),
            pltpu.VMEM((n_req, hs * v_dim), bf16),
            pltpu.VMEM((4, n_req, qcols), f32),
            pltpu.VMEM((4, n_req, qcols), f32),
            pltpu.VMEM((4, n_req, qcols), f32),
            pltpu.VMEM((3, n_req, qcols), f32),
            pltpu.VMEM((n_req, qcols), f32),
            pltpu.VMEM((n_req, d_model), f32),
            dma((n_dq,)), dma((2, n_kv)), dma((n_uq, 2)), dma((n_uk,)),
            dma((3,)), dma((3,)), dma((3,)), dma((3,)), dma((n_grp,)), dma((n_grp,)),
            dma((n_slots, n_split + 1)), dma((hs // grp,)), dma((8,)),
            dma((n_req,)), dma((n_req,)), dma((n_req, 3)), dma((n_req, 3)),
            dma((2, 4)), dma((2, 3)), dma((2, 3)), dma((2, 4)),
        ],
        compiler_params=pltpu.CompilerParams(
            vmem_limit_bytes=67043328, collective_id=0, has_side_effects=True),
        name='decode',
    )(ctx_len, x, g_q.reshape(1, low), g_kv.reshape(1, latent), table, w_dq, w_uq, jnp.swapaxes(w_dkv, 0, 1), w_uk,
      cache_c, jnp.swapaxes(cache_kr, 1, 2), w_uv, w_o)
    return out[:, :d_model].astype(bf16), out[:, d_model:d_model + latent].astype(bf16), out[:, d_model + latent:d_model + latent + rope].astype(bf16)


def solution(mesh):
    def decode_step(*args):
        return decode(*args)

    spec_rows = P('dp', None)
    spec_cache = P('dp', 'cp', None)
    in_specs = (spec_rows, P(), P(), P(), P(), P(), P(), P(), P(), spec_cache, spec_cache, P('dp'))
    out_specs = (spec_rows, spec_rows, spec_rows)
    return jax.shard_map(decode_step, mesh=mesh, in_specs=in_specs, out_specs=out_specs, check_vma=False)
```

```python
import functools

import jax
import jax.numpy as jnp
from jax import lax
from jax.experimental import pallas as pl
from jax.experimental.pallas import tpu as pltpu
from jax.sharding import PartitionSpec as P

NORM_EPS = 1e-6
ROPE_THETA = 10000.0
MASKED = -1e30
FLOOR = -1e29
LOG2E = 1.4426950408889634


def exchange(src, dst, send_sem, recv_sem, peer):
    return pltpu.make_async_remote_copy(
        src_ref=src, dst_ref=dst, send_sem=send_sem, recv_sem=recv_sem,
        device_id={'cp': peer}, device_id_type=pl.DeviceIdType.MESH)


def merge(parts, latent):
    tops = [p[:, latent:latent + 1] for p in parts]
    top = functools.reduce(jnp.maximum, tops)
    acc, mass = None, None
    for p, t in zip(parts, tops):
        f = jnp.exp(t - top)
        a, w = p[:, :latent] * f, p[:, latent + 64:latent + 65] * f
        acc = a if acc is None else acc + a
        mass = w if mass is None else mass + w
    return acc, top, mass


def stats(top, mass):
    lane = lax.broadcasted_iota(jnp.int32, (top.shape[0], 128), 1)
    return jnp.where(lane < 64, top, mass)


def decode_body(
        dims, c_buf, kr_buf, ctx_ref, x_ref, gq_ref, gkv_ref, tab_ref, dq_hbm, uq_hbm, dkv_hbm, uk_hbm, c_hbm, kr_hbm, uv_hbm, wo_hbm, out_ref, cno_ref, kno_ref,
        wo_buf, uk_buf, s_ref, turn_ref, cq_ref, kv_ref, norm_ref, q_ref, cn_ref, kn_ref,
        acc_buf, recv_a, comb, recv_b, own_b, olat_ref, o_ref,
        po_ref, pair_ref, sum_ref, quart_ref, fin_ref, xo_ref,
        dq_sem, dkv_sem, uq_sem, uk_sem, cs_sem, cr_sem, ks_sem, kr_sem, qs_sem, qv_sem,
        c_sem, uv_sem, wo_sem, sa_sem, ra_sem, sb_sem, rb_sem, h_sem, p_sem, f_sem, g_sem):
    (n_req, heads, latent, nope, rope, v_dim, low, d_model, t_dev, t_chunk, n_dq, n_kv, n_uq, n_uk, grp, n_slots, n_split, scale) = dims
    f32, bf16 = jnp.float32, jnp.bfloat16
    nt = (((1,), (1,)), ((), ()))
    me = lax.axis_index('cp')
    core = lax.rem(me, 2)
    chip = me // 2
    partner = chip * 2 + (1 - core)
    hp = heads // 2
    hs = heads // 8
    my_head = core * hp + chip * hs
    n_lat = latent // 128
    lcols = low // 4
    kcols = latent // 4
    n_grp = hp // grp
    wide = grp * (nope + rope)
    drows = d_model // n_dq
    kdepth = d_model // n_kv
    krows = kcols + rope
    half_cols = d_model // 2
    qcols = d_model // 8
    n_wo = 8

    def peer_chip(d):
        return lax.rem(chip + d, 4)

    def from_chip(d):
        return lax.rem(chip + 4 - d, 4)

    def peer(d):
        return peer_chip(d) * 2 + core

    def dq_piece(i):
        return wo_buf.at[pl.ds(low, drows), pl.ds(i * lcols, lcols)]

    def dq_copy(i):
        return pltpu.make_async_copy(dq_hbm.at[pl.ds(i * drows, drows), pl.ds(pl.multiple_of(chip * lcols, lcols), lcols)], dq_piece(i), dq_sem.at[i])

    def kv_piece(i, row, rows):
        return wo_buf.at[pl.ds(i * krows + row, rows), pl.ds(n_uq * wide, kdepth)]

    def dkv_copies(i):
        cols = pl.ds(i * kdepth, kdepth)
        return [pltpu.make_async_copy(dkv_hbm.at[pl.ds(pl.multiple_of(chip * kcols, kcols), kcols), cols], kv_piece(i, 0, kcols), dkv_sem.at[0, i]),
                pltpu.make_async_copy(dkv_hbm.at[pl.ds(latent, rope), cols], kv_piece(i, kcols, rope), dkv_sem.at[1, i])]

    def uq_slot(g):
        return pl.ds(pl.multiple_of(lax.rem(g, n_uq) * wide, wide), wide)

    def grp_copies(g):
        head = core * hp + g * grp
        cols = pl.ds(pl.multiple_of(head * (nope + rope), wide), wide)
        half = low // 2
        slot = lax.rem(g, n_uq)
        return [pltpu.make_async_copy(uq_hbm.at[pl.ds(i * half, half), cols], wo_buf.at[pl.ds(i * half, half), uq_slot(g)], uq_sem.at[slot, i])
                for i in (0, 1)] + [
            pltpu.make_async_copy(uk_hbm.at[:, pl.ds(pl.multiple_of(head, grp), grp), :], uk_buf.at[lax.rem(g, n_uk)], uk_sem.at[lax.rem(g, n_uk)])]

    def c_copies(b):
        slot = lax.rem(b, n_slots)
        rows = t_dev // n_split
        out = []
        for i in range(n_split):
            sl = pl.ds(i * rows, rows)
            out.append(pltpu.make_async_copy(c_hbm.at[b, sl], c_buf.at[slot, sl], c_sem.at[slot, i]))
        out.append(pltpu.make_async_copy(kr_hbm.at[b], kr_buf.at[slot], c_sem.at[slot, n_split]))
        return out

    def uv_copy(i):
        return pltpu.make_async_copy(uv_hbm.at[:, pl.ds(pl.multiple_of(my_head + i * grp, grp), grp), :], uk_buf.at[i], uv_sem.at[i])

    def wo_block(i):
        half = jnp.where(i < 4, 1 - core, core)
        return half * half_cols + lax.rem(chip + 1 + i, 4) * qcols

    def wo_slot(i):
        return pl.ds(pl.multiple_of(i * qcols, qcols), qcols)

    def wo_copy(i):
        rows = pl.ds(pl.multiple_of(my_head * v_dim, hs * v_dim), hs * v_dim)
        return pltpu.make_async_copy(wo_hbm.at[rows, pl.ds(pl.multiple_of(wo_block(i), qcols), qcols)], wo_buf.at[:, wo_slot(i)], wo_sem.at[i])

    for i in range(n_dq):
        dq_copy(i).start()
    for i in range(n_kv):
        for cp in dkv_copies(i):
            cp.start()
    for g in range(n_uk - 1):
        for cp in grp_copies(g):
            cp.start()

    barrier = pltpu.get_barrier_semaphore()
    pl.semaphore_signal(barrier, inc=1, device_id={'cp': partner}, device_id_type=pl.DeviceIdType.MESH)
    for d in (1, 2, 3):
        pl.semaphore_signal(barrier, inc=1, device_id={'cp': peer(d)}, device_id_type=pl.DeviceIdType.MESH)

    cq = None
    for i in range(n_dq):
        dq_copy(i).wait()
        part = jnp.dot(x_ref[:, i * drows:(i + 1) * drows], wo_buf[low:low + drows, i * lcols:(i + 1) * lcols], preferred_element_type=f32)
        cq = part if cq is None else cq + part
    cq_ref[chip] = cq.astype(bf16).astype(f32)
    pl.semaphore_wait(barrier, 4)

    def send_cq(d):
        return exchange(cq_ref.at[chip], cq_ref.at[chip], cs_sem.at[d - 1], cr_sem.at[d - 1], peer(d))

    def recv_cq(d):
        return exchange(cq_ref.at[from_chip(d)], cq_ref.at[from_chip(d)], cs_sem.at[d - 1], cr_sem.at[d - 1], peer(d))

    def send_kv(d):
        return exchange(kv_ref.at[chip], kv_ref.at[chip], ks_sem.at[d - 1], kr_sem.at[d - 1], peer(d))

    def recv_kv(d):
        return exchange(kv_ref.at[from_chip(d)], kv_ref.at[from_chip(d)], ks_sem.at[d - 1], kr_sem.at[d - 1], peer(d))

    for d in (1, 2, 3):
        send_cq(d).start()

    kv = None
    for i in range(n_kv):
        for cp in dkv_copies(i):
            cp.wait()
        part = lax.dot_general(x_ref[:, i * kdepth:(i + 1) * kdepth], wo_buf[i * krows:(i + 1) * krows, n_uq * wide:n_uq * wide + kdepth],
                               nt, preferred_element_type=f32)
        kv = part if kv is None else kv + part
    kv_ref[chip] = kv[:, :kcols]
    cos, sin = tab_ref[:, :rope // 2], tab_ref[:, rope // 2:]

    def rotate(v):
        lo, hi = v[:, :rope // 2], v[:, rope // 2:]
        return jnp.concatenate([lo * cos - hi * sin, hi * cos + lo * sin], axis=1)

    kn_ref[...] = rotate(kv[:, kcols:kcols + rope]).astype(bf16).astype(f32)

    for d in (1, 2, 3):
        recv_cq(d).wait_recv()
    for d in (1, 2, 3):
        send_kv(d).start()

    def rms(parts):
        total = None
        for p in parts:
            sq = jnp.sum(p * p, axis=1, keepdims=True)
            total = sq if total is None else total + sq
        return lax.rsqrt(total * (1.0 / (len(parts) * parts[0].shape[1])) + NORM_EPS)

    inv = rms([cq_ref[i] for i in range(4)])
    for i in range(4):
        norm_ref[:, i * lcols:(i + 1) * lcols] = (cq_ref[i] * inv * gq_ref[i * lcols:(i + 1) * lcols].reshape(1, lcols)).astype(bf16)

    def q_rows(c, g):
        return pl.ds(pl.multiple_of((c * hp + g * grp) * n_req, grp * n_req), grp * n_req)

    def send_q(g):
        return exchange(q_ref.at[:, q_rows(core, g)], q_ref.at[:, q_rows(core, g)], qs_sem.at[g], qv_sem.at[g], partner)

    def recv_q(g):
        return exchange(q_ref.at[:, q_rows(1 - core, g)], q_ref.at[:, q_rows(1 - core, g)], qs_sem.at[g], qv_sem.at[g], partner)

    def group(g, carry):
        @pl.when(g + n_uk - 1 < n_grp)
        def _():
            for cp in grp_copies(g + n_uk - 1):
                cp.start()

        @pl.when(g >= n_grp - (n_slots - 1))
        def _():
            for cp in c_copies(g - (n_grp - (n_slots - 1))):
                cp.start()

        for cp in grp_copies(g):
            cp.wait()

        @pl.when(g >= 1)
        def _():
            send_q(g - 1).start()

        q = jnp.dot(norm_ref[...], wo_buf[:low, uq_slot(g)], preferred_element_type=f32).astype(bf16).astype(f32)
        s_ref[...] = uk_buf[lax.rem(g, n_uk)].astype(f32).reshape(latent * grp, nope)
        for h in range(grp):
            at = h * (nope + rope)
            turn_ref[h % 2, :nope, :] = s_ref[pl.ds(h, latent, stride=grp), :].astype(bf16).T
            lat = jnp.dot(q[:, at:at + nope].astype(bf16), turn_ref[h % 2, :nope, :], preferred_element_type=f32)
            rows = pl.ds(pl.multiple_of((core * hp + g * grp + h) * n_req, n_req), n_req)
            for j in range(n_lat):
                q_ref[j, rows, :] = lat[:, j * 128:(j + 1) * 128]
            rot = rotate(q[:, at + nope:at + nope + rope])
            q_ref[n_lat, rows, :] = jnp.concatenate([rot, jnp.zeros((n_req, 128 - rope), f32)], axis=1)
        return carry

    lax.fori_loop(0, n_grp, group, 0)
    send_q(n_grp - 1).start()

    for d in (1, 2, 3):
        recv_kv(d).wait_recv()
    inv = rms([kv_ref[i] for i in range(4)])
    for i in range(4):
        cn_ref[:, i * kcols:(i + 1) * kcols] = (kv_ref[i] * inv * gkv_ref[i * kcols:(i + 1) * kcols].reshape(1, kcols)).astype(bf16).astype(f32)
    for d in (1, 2, 3):
        send_cq(d).wait_send()
        send_kv(d).wait_send()

    def settle(g, carry):
        recv_q(g).wait_recv()
        return carry

    lax.fori_loop(0, n_grp, settle, 0)

    def send_a(b):
        slot = lax.rem(b, 2)
        return exchange(acc_buf.at[slot, pl.ds(pl.multiple_of((1 - core) * hp, hp), hp)], recv_a.at[slot], sa_sem.at[b], ra_sem.at[b], partner)

    def send_b(b, d):
        slot = lax.rem(b, 2)
        return exchange(comb.at[slot, pl.ds(pl.multiple_of(peer_chip(d) * hs, hs), hs)], recv_b.at[b, d - 1], sb_sem.at[b, d - 1],
                        rb_sem.at[b, d - 1], peer(d))

    def pair_merge(b):
        slot = lax.rem(b, 2)
        send_a(b).wait_recv()
        mine = acc_buf[slot, pl.ds(pl.multiple_of(core * hp, hp), hp), :]
        acc, top, mass = merge([mine, recv_a[slot]], latent)
        comb[slot, :, :latent] = acc
        comb[slot, :, latent:] = stats(top, mass)
        own_b[b] = comb[slot, pl.ds(pl.multiple_of(chip * hs, hs), hs), :]

    base = me * t_dev
    n_chunks = t_dev // t_chunk
    lanes = t_chunk // 128
    k2 = scale * LOG2E

    def step(b, carry):
        slot = lax.rem(b, n_slots)

        @pl.when(b + n_slots - 1 < n_req)
        def _():
            for cp in c_copies(b + n_slots - 1):
                cp.start()

        for first_wo, at in ((0, 3), (3, 2), (6, 1)):
            @pl.when(b == n_req - at)
            def _():
                for i in range(first_wo, min(first_wo + 3, n_wo)):
                    wo_copy(i).start()

        @pl.when(b == n_req - 4)
        def _():
            for i in range(hs // grp):
                uv_copy(i).start()

        for cp in c_copies(b):
            cp.wait()

        @pl.when(b >= 1)
        def _():
            send_a(b - 1).start()

        @pl.when(b >= 2)
        def _():
            for d in (1, 2, 3):
                send_b(b - 2, d).start()

        limit = ctx_ref[b] - base
        q = jnp.concatenate([q_ref[j, pl.ds(b, heads, stride=n_req), :].astype(bf16) for j in range(n_lat)], axis=1)
        qr = q_ref[n_lat, pl.ds(b, heads, stride=n_req), :][:, :rope].astype(bf16)
        top = None
        for i in range(n_chunks):
            sl = pl.ds(i * t_chunk, t_chunk)
            turn_ref[i % 2] = c_buf[slot, sl, :].T
            s = jnp.dot(q, turn_ref[i % 2], preferred_element_type=f32)
            s = s + jnp.dot(qr, kr_buf[slot, :, sl], preferred_element_type=f32)
            pos = lax.broadcasted_iota(jnp.int32, (1, t_chunk), 1) + i * t_chunk
            s = jnp.where(pos < limit, s, MASKED)
            for j in range(lanes):
                s_ref[pl.ds((i * lanes + j) * heads, heads), :] = s[:, j * 128:(j + 1) * 128]
            cm = jnp.max(s, axis=1, keepdims=True)
            top = cm if top is None else jnp.maximum(top, cm)
        top = jnp.maximum(top, FLOOR)
        acc, mass = None, None
        for i in range(n_chunks):
            sl = pl.ds(i * t_chunk, t_chunk)
            s = jnp.concatenate([s_ref[pl.ds((i * lanes + j) * heads, heads), :] for j in range(lanes)], axis=1)
            p = jnp.exp2((s - top) * k2)
            ls = jnp.sum(p, axis=1, keepdims=True)
            mass = ls if mass is None else mass + ls
            o = jnp.dot(p.astype(bf16), c_buf[slot, sl, :], preferred_element_type=f32)
            acc = o if acc is None else acc + o

        @pl.when(b >= 2)
        def _():
            send_a(b - 2).wait_send()

        @pl.when(b >= 3)
        def _():
            for d in (1, 2, 3):
                send_b(b - 3, d).wait_send()

        a_slot = lax.rem(b, 2)
        acc_buf[a_slot, :, :latent] = acc
        acc_buf[a_slot, :, latent:] = stats(top * scale, mass)

        @pl.when(b >= 1)
        def _():
            pair_merge(b - 1)

        return carry

    lax.fori_loop(0, n_req, step, 0)

    def final(b, carry):
        for d in (1, 2, 3):
            send_b(b, d).wait_recv()
        rows = pl.ds(my_head * n_req + b, hs, stride=n_req)
        cn = cn_ref[pl.ds(b, 1), :]
        s_new = jnp.sum(q_ref[n_lat, rows, :][:, :rope].astype(bf16).astype(f32) * kn_ref[pl.ds(b, 1), :], axis=1, keepdims=True)
        for j in range(n_lat):
            s_new = s_new + jnp.sum(q_ref[j, rows, :].astype(bf16).astype(f32) * cn[:, j * 128:(j + 1) * 128], axis=1, keepdims=True)
        s_new = s_new * scale
        parts = [own_b[b]] + [recv_b[b, d] for d in range(3)]
        tops = [p[:, latent:latent + 1] for p in parts] + [s_new]
        top = functools.reduce(jnp.maximum, tops)
        w_new = jnp.exp(s_new - top)
        mass = w_new
        acc = w_new.astype(bf16).astype(f32) * cn
        for p, t in zip(parts, tops):
            f = jnp.exp(t - top)
            acc = acc + p[:, :latent] * f
            mass = mass + p[:, latent + 64:latent + 65] * f
        o_lat = (acc / mass).astype(bf16).astype(f32)
        for j in range(n_lat):
            olat_ref[j, pl.ds(pl.multiple_of(b * hs, hs), hs), :] = o_lat[:, j * 128:(j + 1) * 128]
        return carry

    last = n_req - 1
    send_a(last).start()
    for d in (1, 2, 3):
        send_b(last - 1, d).start()
    lax.fori_loop(0, last - 1, final, 0)
    send_a(last - 1).wait_send()
    for d in (1, 2, 3):
        send_b(last - 2, d).wait_send()
    pair_merge(last)
    for i in range(hs // grp):
        uv_copy(i).wait()
        s_ref[...] = uk_buf[i].astype(f32).reshape(latent * grp, v_dim)
        if i == 0:
            for d in (1, 2, 3):
                send_b(last, d).start()
        for h in range(grp):
            c_buf[0, h * latent:(h + 1) * latent, i * v_dim:(i + 1) * v_dim] = s_ref[pl.ds(h, latent, stride=grp), :].astype(bf16)
    lax.fori_loop(last - 1, n_req, final, 0)
    send_a(last).wait_send()
    for b in (last - 1, last):
        for d in (1, 2, 3):
            send_b(b, d).wait_send()

    for h in range(hs):
        lhs = jnp.concatenate([olat_ref[j, pl.ds(h, n_req, stride=hs), :] for j in range(n_lat)], axis=1)
        uv = c_buf[0, (h % grp) * latent:(h % grp + 1) * latent, (h // grp) * v_dim:(h // grp + 1) * v_dim]
        o = jnp.dot(lhs.astype(bf16), uv, preferred_element_type=f32)
        o_ref[:, h * v_dim:(h + 1) * v_dim] = o.astype(bf16)

    def block(i):
        wo_copy(i).wait()
        return jnp.dot(o_ref[...], wo_buf[:, wo_slot(i)], preferred_element_type=f32)

    def to_pair(i):
        return exchange(po_ref.at[i], pair_ref.at[i], h_sem.at[0, i], h_sem.at[1, i], partner)

    def to_owner(i):
        return exchange(sum_ref.at[i], quart_ref.at[i], p_sem.at[0, i], p_sem.at[1, i], peer(i + 1))

    def first(i, carry):
        po_ref[i] = block(i)

        @pl.when(i >= 1)
        def _():
            to_pair(i - 1).start()

        return carry

    lax.fori_loop(0, 4, first, 0)
    to_pair(3).start()

    def second(i, carry):
        part = block(i + 4)
        to_pair(i).wait_recv()
        sum_ref[i] = part + pair_ref[i]

        @pl.when((i >= 1) & (i < 4))
        def _():
            to_owner(i - 1).start()

        return carry

    lax.fori_loop(0, 4, second, 0)
    for i in range(3):
        to_owner(i).wait_recv()
    my_cols = pl.ds(pl.multiple_of(core * half_cols + chip * qcols, qcols), qcols)
    total = sum_ref[3] + quart_ref[0] + quart_ref[1] + quart_ref[2]
    fin_ref[...] = (x_ref[:, my_cols].astype(f32) + total).astype(bf16).astype(f32)

    def to_all(d):
        return exchange(fin_ref, xo_ref.at[:, my_cols], f_sem.at[0, d - 1], f_sem.at[1, d - 1], peer(d))

    def from_all(d):
        cols = pl.ds(pl.multiple_of(core * half_cols + from_chip(d) * qcols, qcols), qcols)
        return exchange(fin_ref, xo_ref.at[:, cols], f_sem.at[0, d - 1], f_sem.at[1, d - 1], peer(d)), cols

    for d in (1, 2, 3):
        to_all(d).start()
    g0 = exchange(fin_ref, xo_ref.at[:, my_cols], g_sem.at[0, 0], g_sem.at[1, 0], partner)
    g0.start()
    cno_ref[...] = cn_ref[...]
    kno_ref[...] = kn_ref[...]
    fwd = [g0]
    for d in (1, 2, 3):
        got, cols = from_all(d)
        got.wait_recv()
        f = exchange(xo_ref.at[:, cols], xo_ref.at[:, cols], g_sem.at[0, d], g_sem.at[1, d], partner)
        f.start()
        fwd.append(f)
    for d in (1, 2, 3):
        to_all(d).wait_send()
    for i in range(3):
        to_owner(i).wait_send()
    for i in range(4):
        to_pair(i).wait_send()

    def settle_sent(g, carry):
        send_q(g).wait_send()
        return carry

    lax.fori_loop(0, n_grp, settle_sent, 0)
    for f in fwd:
        f.wait()
    xo_ref[:, my_cols] = fin_ref[...]
    out_ref[...] = xo_ref[...]


def scoped_body(dims, *refs):
    latent, rope, t_dev, n_slots = dims[2], dims[4], dims[8], dims[15]
    pl.run_scoped(
        lambda c_buf, kr_buf: decode_body(dims, c_buf, kr_buf, *refs),
        pltpu.VMEM((n_slots, t_dev, latent), jnp.bfloat16), pltpu.VMEM((n_slots, rope, t_dev), jnp.bfloat16))


def decode(x, w_dq, g_q, w_uq, w_dkv, g_kv, w_uk, w_uv, w_o, cache_c, cache_kr, ctx_len):
    n_req, d_model = x.shape
    latent, heads, nope = w_uk.shape
    rope = w_dkv.shape[1] - latent
    low = w_dq.shape[1]
    v_dim = w_uv.shape[2]
    t_dev = cache_c.shape[1]
    scale = (nope + rope) ** -0.5
    n_dq, n_kv, n_uq, n_uk, grp, n_slots, n_split, t_chunk = 14, 7, 4, 3, 8, 3, 4, 512
    f32, bf16 = jnp.float32, jnp.bfloat16
    dims = (n_req, heads, latent, nope, rope, v_dim, low, d_model, t_dev, t_chunk, n_dq, n_kv, n_uq, n_uk, grp, n_slots, n_split, scale)
    lane = jnp.arange(rope)
    inv_freq = ROPE_THETA ** (-2.0 * (lane % (rope // 2)).astype(f32) / rope)
    angles = ctx_len.astype(f32)[:, None] * inv_freq
    table = jnp.where(lane < rope // 2, jnp.cos(angles), jnp.sin(angles))
    hs = heads // 8
    hp = heads // 2
    tail = latent + 128
    qcols = d_model // 8
    n_grp = hp // grp
    vmem = pl.BlockSpec(memory_space=pltpu.VMEM)
    hbm = pl.BlockSpec(memory_space=pl.ANY)
    dma = pltpu.SemaphoreType.DMA
    out = pl.pallas_call(
        functools.partial(scoped_body, dims),
        out_shape=[jax.ShapeDtypeStruct((n_req, n), f32) for n in (d_model, latent, rope)],
        in_specs=[pl.BlockSpec(memory_space=pltpu.SMEM)] + [vmem] * 4 + [hbm] * 8,
        out_specs=[vmem] * 3,
        scratch_shapes=[
            pltpu.VMEM((hs * v_dim, d_model), bf16),
            pltpu.VMEM((n_uk, latent, grp, nope), bf16),
            pltpu.VMEM((t_dev * heads // 128, 128), f32),
            pltpu.VMEM((2, latent, t_chunk), bf16),
            pltpu.VMEM((4, n_req, low // 4), f32),
            pltpu.VMEM((4, n_req, latent // 4), f32),
            pltpu.VMEM((n_req, low), bf16),
            pltpu.VMEM((latent // 128 + 1, heads * n_req, 128), f32),
            pltpu.VMEM((n_req, latent), f32),
            pltpu.VMEM((n_req, rope), f32),
            pltpu.VMEM((2, heads, tail), f32),
            pltpu.VMEM((2, hp, tail), f32),
            pltpu.VMEM((2, hp, tail), f32),
            pltpu.VMEM((n_req, 3, hs, tail), f32),
            pltpu.VMEM((n_req, hs, tail), f32),
            pltpu.VMEM((latent // 128, n_req * hs, 128), f32),
            pltpu.VMEM((n_req, hs * v_dim), bf16),
            pltpu.VMEM((4, n_req, qcols), f32),
            pltpu.VMEM((4, n_req, qcols), f32),
            pltpu.VMEM((4, n_req, qcols), f32),
            pltpu.VMEM((3, n_req, qcols), f32),
            pltpu.VMEM((n_req, qcols), f32),
            pltpu.VMEM((n_req, d_model), f32),
            dma((n_dq,)), dma((2, n_kv)), dma((n_uq, 2)), dma((n_uk,)),
            dma((3,)), dma((3,)), dma((3,)), dma((3,)), dma((n_grp,)), dma((n_grp,)),
            dma((n_slots, n_split + 1)), dma((hs // grp,)), dma((8,)),
            dma((n_req,)), dma((n_req,)), dma((n_req, 3)), dma((n_req, 3)),
            dma((2, 4)), dma((2, 3)), dma((2, 3)), dma((2, 4)),
        ],
        compiler_params=pltpu.CompilerParams(
            vmem_limit_bytes=67043328, collective_id=0, has_side_effects=True),
        name='decode',
    )(ctx_len, x, g_q, g_kv, table, w_dq, w_uq, jnp.swapaxes(w_dkv, 0, 1), w_uk,
      cache_c, jnp.swapaxes(cache_kr, 1, 2), w_uv, w_o)
    return tuple(o.astype(bf16) for o in out)


def solution(mesh):
    def decode_step(*args):
        return decode(*args)

    spec_rows = P('dp', None)
    spec_cache = P('dp', 'cp', None)
    in_specs = (spec_rows, P(), P(), P(), P(), P(), P(), P(), P(), spec_cache, spec_cache, P('dp'))
    out_specs = (spec_rows, spec_rows, spec_rows)
    return jax.shard_map(decode_step, mesh=mesh, in_specs=in_specs, out_specs=out_specs, check_vma=False)
```

```python
import functools

import jax
import jax.numpy as jnp
from jax import lax
from jax.experimental import pallas as pl
from jax.experimental.pallas import tpu as pltpu
from jax.sharding import PartitionSpec as P

NORM_EPS = 1e-6
ROPE_THETA = 10000.0
MASKED = -1e30
FLOOR = -1e29
LOG2E = 1.4426950408889634


def exchange(src, dst, send_sem, recv_sem, peer):
    return pltpu.make_async_remote_copy(
        src_ref=src, dst_ref=dst, send_sem=send_sem, recv_sem=recv_sem,
        device_id={'cp': peer}, device_id_type=pl.DeviceIdType.MESH)


def merge(parts, latent):
    tops = [p[:, latent:latent + 1] for p in parts]
    top = functools.reduce(jnp.maximum, tops)
    acc, mass = None, None
    for p, t in zip(parts, tops):
        f = jnp.exp(t - top)
        a, w = p[:, :latent] * f, p[:, latent + 64:latent + 65] * f
        acc = a if acc is None else acc + a
        mass = w if mass is None else mass + w
    return acc, top, mass


def stats(top, mass):
    lane = lax.broadcasted_iota(jnp.int32, (top.shape[0], 128), 1)
    return jnp.where(lane < 64, top, mass)


def decode_body(
        dims, c_buf, kr_buf, p_ref, turn_ref, ctx_ref, x_ref, gq_ref, gkv_ref, tab_ref, dq_hbm, uq_hbm, dkv_hbm, uk_hbm, c_hbm, kr_hbm, uv_hbm, wo_hbm, out_ref,
        wo_buf, uk_buf, s_ref, top_ref, cq_ref, kv_ref, norm_ref, q_ref, cn_ref, kn_ref,
        acc_buf, recv_a, comb, recv_b, own_b, olat_ref, o_ref,
        po_ref, pair_ref, sum_ref, quart_ref, fin_ref, xo_ref,
        dq_sem, dkv_sem, uq_sem, uk_sem, cs_sem, cr_sem, ks_sem, kr_sem, qs_sem, qv_sem,
        c_sem, uv_sem, wo_sem, sa_sem, ra_sem, sb_sem, rb_sem, h_sem, p_sem, f_sem, g_sem):
    (n_req, heads, latent, nope, rope, v_dim, low, d_model, t_dev, t_chunk, n_dq, n_kv, n_uq, n_uk, grp, n_slots, n_split, scale) = dims
    f32, bf16 = jnp.float32, jnp.bfloat16
    nt = (((1,), (1,)), ((), ()))
    me = lax.axis_index('cp')
    core = lax.rem(me, 2)
    chip = me // 2
    partner = chip * 2 + (1 - core)
    hp = heads // 2
    hs = heads // 8
    my_head = core * hp + chip * hs
    n_lat = latent // 128
    lcols = low // 4
    kcols = latent // 4
    n_grp = hp // grp
    wide = grp * (nope + rope)
    drows = d_model // n_dq
    kdepth = d_model // n_kv
    krows = kcols + rope
    half_cols = d_model // 2
    qcols = d_model // 8
    n_wo = 8

    def peer_chip(d):
        return lax.rem(chip + d, 4)

    def from_chip(d):
        return lax.rem(chip + 4 - d, 4)

    def peer(d):
        return peer_chip(d) * 2 + core

    def dq_piece(i):
        return wo_buf.at[pl.ds(low, drows), pl.ds(i * lcols, lcols)]

    def dq_copy(i):
        return pltpu.make_async_copy(dq_hbm.at[pl.ds(i * drows, drows), pl.ds(pl.multiple_of(chip * lcols, lcols), lcols)], dq_piece(i), dq_sem.at[i])

    def kv_piece(i, row, rows):
        return wo_buf.at[pl.ds(i * krows + row, rows), pl.ds(n_uq * wide, kdepth)]

    def dkv_copies(i):
        cols = pl.ds(i * kdepth, kdepth)
        return [pltpu.make_async_copy(dkv_hbm.at[pl.ds(pl.multiple_of(chip * kcols, kcols), kcols), cols], kv_piece(i, 0, kcols), dkv_sem.at[0, i]),
                pltpu.make_async_copy(dkv_hbm.at[pl.ds(latent, rope), cols], kv_piece(i, kcols, rope), dkv_sem.at[1, i])]

    def uq_slot(g):
        return pl.ds(pl.multiple_of(lax.rem(g, n_uq) * wide, wide), wide)

    def uq_copies(g):
        cols = pl.ds(pl.multiple_of((core * hp + g * grp) * (nope + rope), wide), wide)
        half = low // 2
        slot = lax.rem(g, n_uq)
        return [pltpu.make_async_copy(uq_hbm.at[pl.ds(i * half, half), cols], wo_buf.at[pl.ds(i * half, half), uq_slot(g)], uq_sem.at[slot, i])
                for i in (0, 1)]

    def uk_copy(g):
        slot = lax.rem(g, n_uk)
        return pltpu.make_async_copy(uk_hbm.at[:, pl.ds(pl.multiple_of(core * hp + g * grp, grp), grp), :], uk_buf.at[slot], uk_sem.at[slot])

    def c_copies(b, half):
        slot = lax.rem(b, n_slots)
        rows = t_dev // n_split
        out = []
        for i in range(half * n_split // 2, (half + 1) * n_split // 2):
            sl = pl.ds(i * rows, rows)
            out.append(pltpu.make_async_copy(c_hbm.at[b, sl], c_buf.at[slot, sl], c_sem.at[slot, i]))
        if half == 0:
            out.append(pltpu.make_async_copy(kr_hbm.at[b], kr_buf.at[slot], c_sem.at[slot, n_split]))
        return out

    def uv_copy(i):
        return pltpu.make_async_copy(uv_hbm.at[:, pl.ds(pl.multiple_of(my_head + i * grp, grp), grp), :], uk_buf.at[i], uv_sem.at[i])

    def wo_block(i):
        half = jnp.where(i < 4, 1 - core, core)
        return half * half_cols + lax.rem(chip + 1 + i, 4) * qcols

    def wo_slot(i):
        return pl.ds(pl.multiple_of(i * qcols, qcols), qcols)

    def wo_copy(i):
        rows = pl.ds(pl.multiple_of(my_head * v_dim, hs * v_dim), hs * v_dim)
        return pltpu.make_async_copy(wo_hbm.at[rows, pl.ds(pl.multiple_of(wo_block(i), qcols), qcols)], wo_buf.at[:, wo_slot(i)], wo_sem.at[i])

    for i in range(n_dq):
        dq_copy(i).start()
    for i in range(n_kv):
        for cp in dkv_copies(i):
            cp.start()
    uk_copy(0).start()
    for g in range(n_uq - 1):
        for cp in uq_copies(g):
            cp.start()

    barrier = pltpu.get_barrier_semaphore()
    pl.semaphore_signal(barrier, inc=1, device_id={'cp': partner}, device_id_type=pl.DeviceIdType.MESH)
    for d in (1, 2, 3):
        pl.semaphore_signal(barrier, inc=1, device_id={'cp': peer(d)}, device_id_type=pl.DeviceIdType.MESH)

    cq = None
    for i in range(n_dq):
        dq_copy(i).wait()
        part = jnp.dot(x_ref[:, i * drows:(i + 1) * drows], wo_buf[low:low + drows, i * lcols:(i + 1) * lcols], preferred_element_type=f32)
        cq = part if cq is None else cq + part
    cq_ref[chip] = cq.astype(bf16).astype(f32)
    pl.semaphore_wait(barrier, 4)

    def send_cq(d):
        return exchange(cq_ref.at[chip], cq_ref.at[chip], cs_sem.at[d - 1], cr_sem.at[d - 1], peer(d))

    def recv_cq(d):
        return exchange(cq_ref.at[from_chip(d)], cq_ref.at[from_chip(d)], cs_sem.at[d - 1], cr_sem.at[d - 1], peer(d))

    def send_kv(d):
        return exchange(kv_ref.at[chip], kv_ref.at[chip], ks_sem.at[d - 1], kr_sem.at[d - 1], peer(d))

    def recv_kv(d):
        return exchange(kv_ref.at[from_chip(d)], kv_ref.at[from_chip(d)], ks_sem.at[d - 1], kr_sem.at[d - 1], peer(d))

    for d in (1, 2, 3):
        send_cq(d).start()

    kv = None
    for i in range(n_kv):
        for cp in dkv_copies(i):
            cp.wait()
        part = lax.dot_general(x_ref[:, i * kdepth:(i + 1) * kdepth], wo_buf[i * krows:(i + 1) * krows, n_uq * wide:n_uq * wide + kdepth],
                               nt, preferred_element_type=f32)
        kv = part if kv is None else kv + part
    kv_ref[chip] = kv[:, :kcols]
    cos, sin = tab_ref[:, :rope // 2], tab_ref[:, rope // 2:]

    def rotate(v):
        lo, hi = v[:, :rope // 2], v[:, rope // 2:]
        return jnp.concatenate([lo * cos - hi * sin, hi * cos + lo * sin], axis=1)

    kn_ref[...] = rotate(kv[:, kcols:kcols + rope]).astype(bf16).astype(f32)

    for d in (1, 2, 3):
        recv_cq(d).wait_recv()
    for d in (1, 2, 3):
        send_kv(d).start()

    def rms(parts):
        total = None
        for p in parts:
            sq = jnp.sum(p * p, axis=1, keepdims=True)
            total = sq if total is None else total + sq
        return lax.rsqrt(total * (1.0 / (len(parts) * parts[0].shape[1])) + NORM_EPS)

    inv = rms([cq_ref[i] for i in range(4)])
    for i in range(4):
        norm_ref[:, i * lcols:(i + 1) * lcols] = (cq_ref[i] * inv * gq_ref[i * lcols:(i + 1) * lcols].reshape(1, lcols)).astype(bf16)

    def q_rows(c, g):
        return pl.ds(pl.multiple_of((c * hp + g * grp) * n_req, grp * n_req), grp * n_req)

    def send_q(g):
        return exchange(q_ref.at[:, q_rows(core, g)], q_ref.at[:, q_rows(core, g)], qs_sem.at[g], qv_sem.at[g], partner)

    def recv_q(g):
        return exchange(q_ref.at[:, q_rows(1 - core, g)], q_ref.at[:, q_rows(1 - core, g)], qs_sem.at[g], qv_sem.at[g], partner)

    def group(g, carry):
        @pl.when(g + 1 < n_grp)
        def _():
            uk_copy(g + 1).start()

        @pl.when(g + n_uq - 1 < n_grp)
        def _():
            for cp in uq_copies(g + n_uq - 1):
                cp.start()

        @pl.when(g >= n_grp - n_slots)
        def _():
            for cp in c_copies(g - (n_grp - n_slots), 0) + c_copies(g - (n_grp - n_slots), 1):
                cp.start()

        for cp in uq_copies(g):
            cp.wait()
        uk_copy(g).wait()

        @pl.when(g >= 1)
        def _():
            send_q(g - 1).start()

        q = jnp.dot(norm_ref[...], wo_buf[:low, uq_slot(g)], preferred_element_type=f32).astype(bf16).astype(f32)
        s_ref[...] = uk_buf[lax.rem(g, n_uk)].astype(f32).reshape(latent * grp, nope)
        for h in range(grp):
            at = h * (nope + rope)
            turn_ref[h % 2, :nope, :latent] = s_ref[pl.ds(h, latent, stride=grp), :].astype(bf16).T
            lat = jnp.dot(q[:, at:at + nope].astype(bf16), turn_ref[h % 2, :nope, :latent], preferred_element_type=f32)
            rows = pl.ds(pl.multiple_of((core * hp + g * grp + h) * n_req, n_req), n_req)
            for j in range(n_lat):
                q_ref[j, rows, :] = lat[:, j * 128:(j + 1) * 128]
            rot = rotate(q[:, at + nope:at + nope + rope])
            q_ref[n_lat, rows, :] = jnp.concatenate([rot, jnp.zeros((n_req, 128 - rope), f32)], axis=1)
        return carry

    lax.fori_loop(0, n_grp, group, 0)
    send_q(n_grp - 1).start()

    for d in (1, 2, 3):
        recv_kv(d).wait_recv()
    inv = rms([kv_ref[i] for i in range(4)])
    for i in range(4):
        cn_ref[:, i * kcols:(i + 1) * kcols] = (kv_ref[i] * inv * gkv_ref[i * kcols:(i + 1) * kcols].reshape(1, kcols)).astype(bf16).astype(f32)
    for d in (1, 2, 3):
        send_cq(d).wait_send()
        send_kv(d).wait_send()

    def settle(g, carry):
        recv_q(g).wait_recv()
        return carry

    lax.fori_loop(0, n_grp, settle, 0)

    def send_a(b):
        slot = lax.rem(b, 2)
        return exchange(acc_buf.at[slot, pl.ds(pl.multiple_of((1 - core) * hp, hp), hp)], recv_a.at[slot], sa_sem.at[b], ra_sem.at[b], partner)

    def send_b(b, d):
        slot = lax.rem(b, 2)
        return exchange(comb.at[slot, pl.ds(pl.multiple_of(peer_chip(d) * hs, hs), hs)], recv_b.at[b, d - 1], sb_sem.at[b, d - 1],
                        rb_sem.at[b, d - 1], peer(d))

    def pair_merge(b):
        slot = lax.rem(b, 2)
        send_a(b).wait_recv()
        mine = acc_buf[slot, pl.ds(pl.multiple_of(core * hp, hp), hp), :]
        acc, top, mass = merge([mine, recv_a[slot]], latent)
        comb[slot, :, :latent] = acc
        comb[slot, :, latent:] = stats(top, mass)
        own_b[b] = comb[slot, pl.ds(pl.multiple_of(chip * hs, hs), hs), :]

    base = me * t_dev
    n_chunks = t_dev // t_chunk
    lanes = t_chunk // 128
    k2 = scale * LOG2E

    def query(b):
        q = jnp.concatenate([q_ref[j, pl.ds(b, heads, stride=n_req), :].astype(bf16) for j in range(n_lat)], axis=1)
        return q, q_ref[n_lat, pl.ds(b, heads, stride=n_req), :][:, :rope].astype(bf16), ctx_ref[b] - base

    def scores(b, query_b, i):
        q, qr, limit = query_b
        slot = lax.rem(b, n_slots)
        sl = pl.ds(i * t_chunk, t_chunk)
        turn_ref[i % 2, :, :t_chunk] = c_buf[slot, sl, :].T
        s = jnp.dot(q, turn_ref[i % 2, :, :t_chunk], preferred_element_type=f32)
        s = s + jnp.dot(qr, kr_buf[slot, :, sl], preferred_element_type=f32)
        pos = lax.broadcasted_iota(jnp.int32, (1, t_chunk), 1) + i * t_chunk
        s = jnp.where(pos < limit, s, MASKED)
        top = None
        for j in range(lanes):
            part = s[:, j * 128:(j + 1) * 128]
            s_ref[pl.ds((i * lanes + j) * heads, heads), :] = part
            top = part if top is None else jnp.maximum(top, part)
        return top

    def weigh(top, i):
        mass = None
        for j in range(lanes):
            p = jnp.exp2((s_ref[pl.ds((i * lanes + j) * heads, heads), :] - top) * k2)
            mass = p if mass is None else mass + p
            p_ref[:, (i * lanes + j) * 128:(i * lanes + j + 1) * 128] = p.astype(bf16)
        return mass

    def values(b, i):
        sl = pl.ds(i * t_chunk, t_chunk)
        return jnp.dot(p_ref[:, sl], c_buf[lax.rem(b, n_slots), sl, :], preferred_element_type=f32)

    def add(a, v):
        return v if a is None else a + v

    def top_of(a):
        return jnp.maximum(jnp.max(a, axis=1, keepdims=True), FLOOR)

    def release(r):
        @pl.when(r >= 1)
        def _():
            send_a(r - 1).start()

        @pl.when(r >= 2)
        def _():
            for d in (1, 2, 3):
                send_b(r - 2, d).start()

    def settle_partial(r, acc, top, mass):
        @pl.when(r >= 2)
        def _():
            send_a(r - 2).wait_send()

        @pl.when(r >= 3)
        def _():
            for d in (1, 2, 3):
                send_b(r - 3, d).wait_send()

        a_slot = lax.rem(r, 2)
        acc_buf[a_slot, :, :latent] = acc
        acc_buf[a_slot, :, latent:] = stats(top * scale, jnp.sum(mass, axis=1, keepdims=True))

        @pl.when(r >= 1)
        def _():
            pair_merge(r - 1)

    for half in (0, 1):
        for cp in c_copies(0, half):
            cp.wait()
    top = None
    query_0 = query(0)
    for i in range(n_chunks):
        t = scores(0, query_0, i)
        top = t if top is None else jnp.maximum(top, t)
    top_ref[...] = top_of(top) + jnp.zeros((heads, 128), f32)

    def step(b, carry):
        r = b - 1
        release(r)
        for first_wo, at in ((0, 3), (3, 2), (6, 1)):
            @pl.when(b == n_req - at)
            def _():
                for i in range(first_wo, min(first_wo + 3, n_wo)):
                    wo_copy(i).start()

        @pl.when(b == n_req - 4)
        def _():
            for i in range(hs // grp):
                uv_copy(i).start()

        old = top_ref[...]
        query_b = query(b)
        top, mass, acc = None, None, None
        for half in (0, 1):
            for cp in c_copies(b, half):
                cp.wait()
            for i in range(half * n_chunks // 2, (half + 1) * n_chunks // 2):
                mass = add(mass, weigh(old, i))
                t = scores(b, query_b, i)
                top = t if top is None else jnp.maximum(top, t)
                acc = add(acc, values(r, i))

            @pl.when(b + 2 < n_req)
            def _():
                for cp in c_copies(b + 2, half):
                    cp.start()

        top_ref[...] = top_of(top) + jnp.zeros((heads, 128), f32)
        settle_partial(r, acc, old[:, :1], mass)
        return carry

    lax.fori_loop(1, n_req, step, 0)
    release(n_req - 1)
    old = top_ref[...]
    mass, acc = None, None
    for i in range(n_chunks):
        mass = add(mass, weigh(old, i))
        acc = add(acc, values(n_req - 1, i))
    settle_partial(n_req - 1, acc, old[:, :1], mass)

    def final(b, carry):
        for d in (1, 2, 3):
            send_b(b, d).wait_recv()
        rows = pl.ds(my_head * n_req + b, hs, stride=n_req)
        cn = cn_ref[pl.ds(b, 1), :]
        s_new = jnp.sum(q_ref[n_lat, rows, :][:, :rope].astype(bf16).astype(f32) * kn_ref[pl.ds(b, 1), :], axis=1, keepdims=True)
        for j in range(n_lat):
            s_new = s_new + jnp.sum(q_ref[j, rows, :].astype(bf16).astype(f32) * cn[:, j * 128:(j + 1) * 128], axis=1, keepdims=True)
        s_new = s_new * scale
        parts = [own_b[b]] + [recv_b[b, d] for d in range(3)]
        tops = [p[:, latent:latent + 1] for p in parts] + [s_new]
        top = functools.reduce(jnp.maximum, tops)
        w_new = jnp.exp(s_new - top)
        mass = w_new
        acc = w_new.astype(bf16).astype(f32) * cn
        for p, t in zip(parts, tops):
            f = jnp.exp(t - top)
            acc = acc + p[:, :latent] * f
            mass = mass + p[:, latent + 64:latent + 65] * f
        o_lat = (acc / mass).astype(bf16).astype(f32)
        for j in range(n_lat):
            olat_ref[j, pl.ds(pl.multiple_of(b * hs, hs), hs), :] = o_lat[:, j * 128:(j + 1) * 128]
        return carry

    last = n_req - 1
    send_a(last).start()
    for d in (1, 2, 3):
        send_b(last - 1, d).start()
    lax.fori_loop(0, last - 1, final, 0)
    send_a(last - 1).wait_send()
    for d in (1, 2, 3):
        send_b(last - 2, d).wait_send()
    pair_merge(last)
    for i in range(hs // grp):
        uv_copy(i).wait()
        s_ref[...] = uk_buf[i].astype(f32).reshape(latent * grp, v_dim)
        if i == 0:
            for d in (1, 2, 3):
                send_b(last, d).start()
        for h in range(grp):
            c_buf[0, h * latent:(h + 1) * latent, i * v_dim:(i + 1) * v_dim] = s_ref[pl.ds(h, latent, stride=grp), :].astype(bf16)
    lax.fori_loop(last - 1, n_req, final, 0)
    send_a(last).wait_send()
    for b in (last - 1, last):
        for d in (1, 2, 3):
            send_b(b, d).wait_send()

    for h in range(hs):
        lhs = jnp.concatenate([olat_ref[j, pl.ds(h, n_req, stride=hs), :] for j in range(n_lat)], axis=1)
        uv = c_buf[0, (h % grp) * latent:(h % grp + 1) * latent, (h // grp) * v_dim:(h // grp + 1) * v_dim]
        o = jnp.dot(lhs.astype(bf16), uv, preferred_element_type=f32)
        o_ref[:, h * v_dim:(h + 1) * v_dim] = o.astype(bf16)

    def block(i):
        wo_copy(i).wait()
        return jnp.dot(o_ref[...], wo_buf[:, wo_slot(i)], preferred_element_type=f32)

    def to_pair(i):
        return exchange(po_ref.at[i], pair_ref.at[i], h_sem.at[0, i], h_sem.at[1, i], partner)

    def to_owner(i):
        return exchange(sum_ref.at[i], quart_ref.at[i], p_sem.at[0, i], p_sem.at[1, i], peer(i + 1))

    def first(i, carry):
        po_ref[i] = block(i)

        @pl.when(i >= 1)
        def _():
            to_pair(i - 1).start()

        return carry

    lax.fori_loop(0, 4, first, 0)
    to_pair(3).start()

    def second(i, carry):
        part = block(i + 4)
        to_pair(i).wait_recv()
        sum_ref[i] = part + pair_ref[i]

        @pl.when((i >= 1) & (i < 4))
        def _():
            to_owner(i - 1).start()

        return carry

    lax.fori_loop(0, 4, second, 0)
    for i in range(3):
        to_owner(i).wait_recv()
    my_cols = pl.ds(pl.multiple_of(core * half_cols + chip * qcols, qcols), qcols)
    total = sum_ref[3] + quart_ref[0] + quart_ref[1] + quart_ref[2]
    fin_ref[...] = (x_ref[:, my_cols].astype(f32) + total).astype(bf16).astype(f32)

    def to_all(d):
        return exchange(fin_ref, xo_ref.at[:, my_cols], f_sem.at[0, d - 1], f_sem.at[1, d - 1], peer(d))

    def from_all(d):
        cols = pl.ds(pl.multiple_of(core * half_cols + from_chip(d) * qcols, qcols), qcols)
        return exchange(fin_ref, xo_ref.at[:, cols], f_sem.at[0, d - 1], f_sem.at[1, d - 1], peer(d)), cols

    for d in (1, 2, 3):
        to_all(d).start()
    g0 = exchange(fin_ref, xo_ref.at[:, my_cols], g_sem.at[0, 0], g_sem.at[1, 0], partner)
    g0.start()
    out_ref[:, d_model:d_model + latent] = cn_ref[...]
    out_ref[:, d_model + latent:] = jnp.concatenate([kn_ref[...], jnp.zeros((n_req, 128 - rope), f32)], axis=1)
    fwd = [g0]
    for d in (1, 2, 3):
        got, cols = from_all(d)
        got.wait_recv()
        f = exchange(xo_ref.at[:, cols], xo_ref.at[:, cols], g_sem.at[0, d], g_sem.at[1, d], partner)
        f.start()
        fwd.append(f)
    for d in (1, 2, 3):
        to_all(d).wait_send()
    for i in range(3):
        to_owner(i).wait_send()
    for i in range(4):
        to_pair(i).wait_send()

    def settle_sent(g, carry):
        send_q(g).wait_send()
        return carry

    lax.fori_loop(0, n_grp, settle_sent, 0)
    for f in fwd:
        f.wait()
    xo_ref[:, my_cols] = fin_ref[...]
    out_ref[:, :d_model] = xo_ref[...]


def scoped_body(dims, *refs):
    heads, latent, rope, t_dev, t_chunk, n_slots = dims[1], dims[2], dims[4], dims[8], dims[9], dims[15]
    pl.run_scoped(
        lambda *scoped: decode_body(dims, *scoped, *refs),
        pltpu.VMEM((n_slots, t_dev, latent), jnp.bfloat16), pltpu.VMEM((n_slots, rope, t_dev), jnp.bfloat16),
        pltpu.VMEM((heads, t_dev), jnp.bfloat16), pltpu.VMEM((2, latent, max(t_chunk, latent)), jnp.bfloat16))


def decode(x, w_dq, g_q, w_uq, w_dkv, g_kv, w_uk, w_uv, w_o, cache_c, cache_kr, ctx_len):
    n_req, d_model = x.shape
    latent, heads, nope = w_uk.shape
    rope = w_dkv.shape[1] - latent
    low = w_dq.shape[1]
    v_dim = w_uv.shape[2]
    t_dev = cache_c.shape[1]
    scale = (nope + rope) ** -0.5
    n_dq, n_kv, n_uq, n_uk, grp, n_slots, n_split, t_chunk = 14, 7, 4, 2, 8, 3, 4, 512
    f32, bf16 = jnp.float32, jnp.bfloat16
    dims = (n_req, heads, latent, nope, rope, v_dim, low, d_model, t_dev, t_chunk, n_dq, n_kv, n_uq, n_uk, grp, n_slots, n_split, scale)
    lane = jnp.arange(rope)
    inv_freq = ROPE_THETA ** (-2.0 * (lane % (rope // 2)).astype(f32) / rope)
    angles = ctx_len.astype(f32)[:, None] * inv_freq
    table = jnp.where(lane < rope // 2, jnp.cos(angles), jnp.sin(angles))
    turn = max(t_chunk, latent)
    hs = heads // 8
    hp = heads // 2
    tail = latent + 128
    qcols = d_model // 8
    n_grp = hp // grp
    vmem = pl.BlockSpec(memory_space=pltpu.VMEM)
    hbm = pl.BlockSpec(memory_space=pl.ANY)
    dma = pltpu.SemaphoreType.DMA
    out = pl.pallas_call(
        functools.partial(scoped_body, dims),
        out_shape=jax.ShapeDtypeStruct((n_req, d_model + latent + 128), f32),
        in_specs=[pl.BlockSpec(memory_space=pltpu.SMEM)] + [vmem] * 4 + [hbm] * 8,
        out_specs=vmem,
        scratch_shapes=[
            pltpu.VMEM((hs * v_dim, d_model), bf16),
            pltpu.VMEM((n_uk, latent, grp, nope), bf16),
            pltpu.VMEM((t_dev * heads // 128, 128), f32),
            pltpu.VMEM((heads, 128), f32),
            pltpu.VMEM((4, n_req, low // 4), f32),
            pltpu.VMEM((4, n_req, latent // 4), f32),
            pltpu.VMEM((n_req, low), bf16),
            pltpu.VMEM((latent // 128 + 1, heads * n_req, 128), f32),
            pltpu.VMEM((n_req, latent), f32),
            pltpu.VMEM((n_req, rope), f32),
            pltpu.VMEM((2, heads, tail), f32),
            pltpu.VMEM((2, hp, tail), f32),
            pltpu.VMEM((2, hp, tail), f32),
            pltpu.VMEM((n_req, 3, hs, tail), f32),
            pltpu.VMEM((n_req, hs, tail), f32),
            pltpu.VMEM((latent // 128, n_req * hs, 128), f32),
            pltpu.VMEM((n_req, hs * v_dim), bf16),
            pltpu.VMEM((4, n_req, qcols), f32),
            pltpu.VMEM((4, n_req, qcols), f32),
            pltpu.VMEM((4, n_req, qcols), f32),
            pltpu.VMEM((3, n_req, qcols), f32),
            pltpu.VMEM((n_req, qcols), f32),
            pltpu.VMEM((n_req, d_model), f32),
            dma((n_dq,)), dma((2, n_kv)), dma((n_uq, 2)), dma((n_uk,)),
            dma((3,)), dma((3,)), dma((3,)), dma((3,)), dma((n_grp,)), dma((n_grp,)),
            dma((n_slots, n_split + 1)), dma((hs // grp,)), dma((8,)),
            dma((n_req,)), dma((n_req,)), dma((n_req, 3)), dma((n_req, 3)),
            dma((2, 4)), dma((2, 3)), dma((2, 3)), dma((2, 4)),
        ],
        compiler_params=pltpu.CompilerParams(
            vmem_limit_bytes=67043328, collective_id=0, has_side_effects=True),
        name='decode',
    )(ctx_len, x, g_q, g_kv, table, w_dq, w_uq, jnp.swapaxes(w_dkv, 0, 1), w_uk,
      cache_c, jnp.swapaxes(cache_kr, 1, 2), w_uv, w_o)
    return out[:, :d_model].astype(bf16), out[:, d_model:d_model + latent].astype(bf16), out[:, d_model + latent:d_model + latent + rope].astype(bf16)


def solution(mesh):
    def decode_step(*args):
        return decode(*args)

    spec_rows = P('dp', None)
    spec_cache = P('dp', 'cp', None)
    in_specs = (spec_rows, P(), P(), P(), P(), P(), P(), P(), P(), spec_cache, spec_cache, P('dp'))
    out_specs = (spec_rows, spec_rows, spec_rows)
    return jax.shard_map(decode_step, mesh=mesh, in_specs=in_specs, out_specs=out_specs, check_vma=False)
```

```python
import functools

import jax
import jax.numpy as jnp
from jax import lax
from jax.experimental import pallas as pl
from jax.experimental.pallas import tpu as pltpu
from jax.sharding import PartitionSpec as P

NORM_EPS = 1e-6
ROPE_THETA = 10000.0
MASKED = -1e30
FLOOR = -1e29
LOG2E = 1.4426950408889634


def exchange(src, dst, send_sem, recv_sem, peer):
    return pltpu.make_async_remote_copy(
        src_ref=src, dst_ref=dst, send_sem=send_sem, recv_sem=recv_sem,
        device_id={'cp': peer}, device_id_type=pl.DeviceIdType.MESH)


def merge(parts, latent):
    tops = [p[:, latent:latent + 1] for p in parts]
    top = functools.reduce(jnp.maximum, tops)
    acc, mass = None, None
    for p, t in zip(parts, tops):
        f = jnp.exp(t - top)
        a, w = p[:, :latent] * f, p[:, latent + 64:latent + 65] * f
        acc = a if acc is None else acc + a
        mass = w if mass is None else mass + w
    return acc, top, mass


def stats(top, mass):
    lane = lax.broadcasted_iota(jnp.int32, (top.shape[0], 128), 1)
    return jnp.where(lane < 64, top, mass)


def decode_body(
        dims, c_buf, kr_buf, p_ref, turn_ref, qs_ref, ctx_ref, x_ref, gq_ref, gkv_ref, tab_ref, dq_hbm, uq_hbm, dkv_hbm, uk_hbm, c_hbm, kr_hbm, uv_hbm, wo_hbm, out_ref,
        wo_buf, uk_buf, s_ref, top_ref, cq_ref, kv_ref, norm_ref, q_ref, cn_ref, kn_ref,
        acc_buf, recv_a, comb, recv_b, own_b, olat_ref, o_ref,
        po_ref, pair_ref, sum_ref, quart_ref, fin_ref, xo_ref,
        dq_sem, dkv_sem, uq_sem, uk_sem, cs_sem, cr_sem, ks_sem, kr_sem, qs_sem, qv_sem,
        c_sem, uv_sem, wo_sem, sa_sem, ra_sem, sb_sem, rb_sem, h_sem, p_sem, f_sem, g_sem):
    (n_req, heads, latent, nope, rope, v_dim, low, d_model, t_dev, t_chunk, n_dq, n_kv, n_uq, n_uk, grp, n_slots, n_split, scale) = dims
    f32, bf16 = jnp.float32, jnp.bfloat16
    nt = (((1,), (1,)), ((), ()))
    me = lax.axis_index('cp')
    core = lax.rem(me, 2)
    chip = me // 2
    partner = chip * 2 + (1 - core)
    hp = heads // 2
    hs = heads // 8
    my_head = core * hp + chip * hs
    n_lat = latent // 128
    lcols = low // 4
    kcols = latent // 4
    n_grp = hp // grp
    wide = grp * (nope + rope)
    drows = d_model // n_dq
    kdepth = d_model // n_kv
    krows = kcols + rope
    half_cols = d_model // 2
    qcols = d_model // 8
    n_wo = 8

    def peer_chip(d):
        return lax.rem(chip + d, 4)

    def from_chip(d):
        return lax.rem(chip + 4 - d, 4)

    def peer(d):
        return peer_chip(d) * 2 + core

    def dq_piece(i):
        return wo_buf.at[pl.ds(low, drows), pl.ds(i * lcols, lcols)]

    def dq_copy(i):
        return pltpu.make_async_copy(dq_hbm.at[pl.ds(i * drows, drows), pl.ds(pl.multiple_of(chip * lcols, lcols), lcols)], dq_piece(i), dq_sem.at[i])

    def kv_piece(i, row, rows):
        return wo_buf.at[pl.ds(i * krows + row, rows), pl.ds(n_uq * wide, kdepth)]

    def dkv_copies(i):
        cols = pl.ds(i * kdepth, kdepth)
        return [pltpu.make_async_copy(dkv_hbm.at[pl.ds(pl.multiple_of(chip * kcols, kcols), kcols), cols], kv_piece(i, 0, kcols), dkv_sem.at[0, i]),
                pltpu.make_async_copy(dkv_hbm.at[pl.ds(latent, rope), cols], kv_piece(i, kcols, rope), dkv_sem.at[1, i])]

    def uq_slot(g):
        return pl.ds(pl.multiple_of(lax.rem(g, n_uq) * wide, wide), wide)

    def uq_copies(g):
        cols = pl.ds(pl.multiple_of((core * hp + g * grp) * (nope + rope), wide), wide)
        half = low // 2
        slot = lax.rem(g, n_uq)
        return [pltpu.make_async_copy(uq_hbm.at[pl.ds(i * half, half), cols], wo_buf.at[pl.ds(i * half, half), uq_slot(g)], uq_sem.at[slot, i])
                for i in (0, 1)]

    def uk_copy(g):
        slot = lax.rem(g, n_uk)
        return pltpu.make_async_copy(uk_hbm.at[:, pl.ds(pl.multiple_of(core * hp + g * grp, grp), grp), :], uk_buf.at[slot], uk_sem.at[slot])

    def c_copies(b, half):
        slot = lax.rem(b, n_slots)
        rows = t_dev // n_split
        out = []
        for i in range(half * n_split // 2, (half + 1) * n_split // 2):
            sl = pl.ds(i * rows, rows)
            out.append(pltpu.make_async_copy(c_hbm.at[b, sl], c_buf.at[slot, sl], c_sem.at[slot, i]))
        if half == 0:
            out.append(pltpu.make_async_copy(kr_hbm.at[b], kr_buf.at[slot], c_sem.at[slot, n_split]))
        return out

    def uv_copy(i):
        return pltpu.make_async_copy(uv_hbm.at[:, pl.ds(pl.multiple_of(my_head + i * grp, grp), grp), :], uk_buf.at[i], uv_sem.at[i])

    def wo_block(i):
        half = jnp.where((i < 3) | (i == 6), 1 - core, core)
        d = jnp.where(i < 3, i + 1, jnp.where(i < 6, i - 2, 0))
        return half * half_cols + lax.rem(chip + d, 4) * qcols

    def wo_slot(i):
        return pl.ds(pl.multiple_of(i * qcols, qcols), qcols)

    def wo_copy(i):
        rows = pl.ds(pl.multiple_of(my_head * v_dim, hs * v_dim), hs * v_dim)
        return pltpu.make_async_copy(wo_hbm.at[rows, pl.ds(pl.multiple_of(wo_block(i), qcols), qcols)], wo_buf.at[:, wo_slot(i)], wo_sem.at[i])

    for i in range(n_dq):
        dq_copy(i).start()
    for i in range(n_kv):
        for cp in dkv_copies(i):
            cp.start()
    uk_copy(0).start()
    for g in range(n_uq - 1):
        for cp in uq_copies(g):
            cp.start()

    barrier = pltpu.get_barrier_semaphore()
    pl.semaphore_signal(barrier, inc=1, device_id={'cp': partner}, device_id_type=pl.DeviceIdType.MESH)
    for d in (1, 2, 3):
        pl.semaphore_signal(barrier, inc=1, device_id={'cp': peer(d)}, device_id_type=pl.DeviceIdType.MESH)

    cq = None
    for i in range(n_dq):
        dq_copy(i).wait()
        part = jnp.dot(x_ref[:, i * drows:(i + 1) * drows], wo_buf[low:low + drows, i * lcols:(i + 1) * lcols], preferred_element_type=f32)
        cq = part if cq is None else cq + part
    cq_ref[chip] = cq.astype(bf16).astype(f32)
    pl.semaphore_wait(barrier, 4)

    def send_cq(d):
        return exchange(cq_ref.at[chip], cq_ref.at[chip], cs_sem.at[d - 1], cr_sem.at[d - 1], peer(d))

    def recv_cq(d):
        return exchange(cq_ref.at[from_chip(d)], cq_ref.at[from_chip(d)], cs_sem.at[d - 1], cr_sem.at[d - 1], peer(d))

    def send_kv(d):
        return exchange(kv_ref.at[chip], kv_ref.at[chip], ks_sem.at[d - 1], kr_sem.at[d - 1], peer(d))

    def recv_kv(d):
        return exchange(kv_ref.at[from_chip(d)], kv_ref.at[from_chip(d)], ks_sem.at[d - 1], kr_sem.at[d - 1], peer(d))

    for d in (1, 2, 3):
        send_cq(d).start()

    kv = None
    for i in range(n_kv):
        for cp in dkv_copies(i):
            cp.wait()
        part = lax.dot_general(x_ref[:, i * kdepth:(i + 1) * kdepth], wo_buf[i * krows:(i + 1) * krows, n_uq * wide:n_uq * wide + kdepth],
                               nt, preferred_element_type=f32)
        kv = part if kv is None else kv + part
    kv_ref[chip] = kv[:, :kcols]
    cos, sin = tab_ref[:, :rope // 2], tab_ref[:, rope // 2:]

    def rotate(v):
        lo, hi = v[:, :rope // 2], v[:, rope // 2:]
        return jnp.concatenate([lo * cos - hi * sin, hi * cos + lo * sin], axis=1)

    kn_ref[...] = rotate(kv[:, kcols:kcols + rope]).astype(bf16).astype(f32)

    for d in (1, 2, 3):
        recv_cq(d).wait_recv()
    for d in (1, 2, 3):
        send_kv(d).start()

    def rms(parts):
        total = None
        for p in parts:
            sq = jnp.sum(p * p, axis=1, keepdims=True)
            total = sq if total is None else total + sq
        return lax.rsqrt(total * (1.0 / (len(parts) * parts[0].shape[1])) + NORM_EPS)

    inv = rms([cq_ref[i] for i in range(4)])
    for i in range(4):
        norm_ref[:, i * lcols:(i + 1) * lcols] = (cq_ref[i] * inv * gq_ref[i * lcols:(i + 1) * lcols].reshape(1, lcols)).astype(bf16)

    def q_rows(c, g):
        return pl.ds(pl.multiple_of((c * hp + g * grp) * n_req, grp * n_req), grp * n_req)

    def send_q(g):
        return exchange(q_ref.at[:, q_rows(core, g)], q_ref.at[:, q_rows(core, g)], qs_sem.at[g], qv_sem.at[g], partner)

    def recv_q(g):
        return exchange(q_ref.at[:, q_rows(1 - core, g)], q_ref.at[:, q_rows(1 - core, g)], qs_sem.at[g], qv_sem.at[g], partner)

    def group(g, carry):
        @pl.when(g + 1 < n_grp)
        def _():
            uk_copy(g + 1).start()

        @pl.when(g + n_uq - 1 < n_grp)
        def _():
            for cp in uq_copies(g + n_uq - 1):
                cp.start()

        @pl.when(g >= n_grp - n_slots)
        def _():
            for cp in c_copies(g - (n_grp - n_slots), 0) + c_copies(g - (n_grp - n_slots), 1):
                cp.start()

        for cp in uq_copies(g):
            cp.wait()
        uk_copy(g).wait()

        @pl.when(g >= 1)
        def _():
            send_q(g - 1).start()

        q = jnp.dot(norm_ref[...], wo_buf[:low, uq_slot(g)], preferred_element_type=f32).astype(bf16).astype(f32)
        s_ref[...] = uk_buf[lax.rem(g, n_uk)].astype(f32).reshape(latent * grp, nope)
        for h in range(grp):
            at = h * (nope + rope)
            p_ref[:nope, (h % 2) * latent:(h % 2 + 1) * latent] = s_ref[pl.ds(h, latent, stride=grp), :].astype(bf16).T
            lat = jnp.dot(q[:, at:at + nope].astype(bf16), p_ref[:nope, (h % 2) * latent:(h % 2 + 1) * latent], preferred_element_type=f32)
            rows = pl.ds(pl.multiple_of((core * hp + g * grp + h) * n_req, n_req), n_req)
            for j in range(n_lat):
                q_ref[j, rows, :] = lat[:, j * 128:(j + 1) * 128]
            rot = rotate(q[:, at + nope:at + nope + rope])
            q_ref[n_lat, rows, :] = jnp.concatenate([rot, jnp.zeros((n_req, 128 - rope), f32)], axis=1)
        return carry

    lax.fori_loop(0, n_grp, group, 0)
    send_q(n_grp - 1).start()

    for d in (1, 2, 3):
        recv_kv(d).wait_recv()
    inv = rms([kv_ref[i] for i in range(4)])
    for i in range(4):
        cn_ref[:, i * kcols:(i + 1) * kcols] = (kv_ref[i] * inv * gkv_ref[i * kcols:(i + 1) * kcols].reshape(1, kcols)).astype(bf16).astype(f32)
    for d in (1, 2, 3):
        send_cq(d).wait_send()
        send_kv(d).wait_send()

    def settle(g, carry):
        recv_q(g).wait_recv()
        return carry

    lax.fori_loop(0, n_grp, settle, 0)

    def send_a(b):
        slot = lax.rem(b, 2)
        return exchange(acc_buf.at[slot, pl.ds(pl.multiple_of((1 - core) * hp, hp), hp)], recv_a.at[slot], sa_sem.at[b], ra_sem.at[b], partner)

    def send_b(b, d):
        slot = lax.rem(b, 2)
        return exchange(comb.at[slot, pl.ds(pl.multiple_of(peer_chip(d) * hs, hs), hs)], recv_b.at[b, d - 1], sb_sem.at[b, d - 1],
                        rb_sem.at[b, d - 1], peer(d))

    def pair_merge(b):
        slot = lax.rem(b, 2)
        send_a(b).wait_recv()
        mine = acc_buf[slot, pl.ds(pl.multiple_of(core * hp, hp), hp), :]
        acc, top, mass = merge([mine, recv_a[slot]], latent)
        comb[slot, :, :latent] = acc
        comb[slot, :, latent:] = stats(top, mass)
        own_b[b] = comb[slot, pl.ds(pl.multiple_of(chip * hs, hs), hs), :]

    base = me * t_dev
    n_chunks = t_dev // t_chunk
    lanes = t_chunk // 128
    k2 = scale * LOG2E

    def query(b):
        q = jnp.concatenate([q_ref[j, pl.ds(b, heads, stride=n_req), :].astype(bf16) for j in range(n_lat)], axis=1)
        return q, q_ref[n_lat, pl.ds(b, heads, stride=n_req), :][:, :rope].astype(bf16), ctx_ref[b] - base

    def stage(b, row):
        q, qr, _ = query(row)
        qs_ref[lax.rem(b, 2), :, :latent] = q
        qs_ref[lax.rem(b, 2), :, latent:] = jnp.concatenate([qr, qr], axis=1)

    def staged(b):
        slot = lax.rem(b, 2)
        return qs_ref[slot, :, :latent], qs_ref[slot, :, latent:latent + rope], ctx_ref[b] - base

    def scores(b, query_b, i):
        q, qr, limit = query_b
        slot = lax.rem(b, n_slots)
        sl = pl.ds(i * t_chunk, t_chunk)
        turn_ref[i % 2, :, :t_chunk] = c_buf[slot, sl, :].T
        s = jnp.dot(q, turn_ref[i % 2, :, :t_chunk], preferred_element_type=f32)
        s = s + jnp.dot(qr, kr_buf[slot, :, sl], preferred_element_type=f32)
        pos = lax.broadcasted_iota(jnp.int32, (1, t_chunk), 1) + i * t_chunk
        s = jnp.where(pos < limit, s, MASKED)
        top = None
        for j in range(lanes):
            part = s[:, j * 128:(j + 1) * 128]
            s_ref[pl.ds((i * lanes + j) * heads, heads), :] = part
            top = part if top is None else jnp.maximum(top, part)
        return top

    def weigh(top, i):
        mass = None
        for j in range(lanes):
            p = jnp.exp2((s_ref[pl.ds((i * lanes + j) * heads, heads), :] - top) * k2)
            mass = p if mass is None else mass + p
            p_ref[:, (i * lanes + j) * 128:(i * lanes + j + 1) * 128] = p.astype(bf16)
        return mass

    def values(b, i):
        sl = pl.ds(i * t_chunk, t_chunk)
        return jnp.dot(p_ref[:, sl], c_buf[lax.rem(b, n_slots), sl, :], preferred_element_type=f32)

    def add(a, v):
        return v if a is None else a + v

    def top_of(a):
        return jnp.maximum(jnp.max(a, axis=1, keepdims=True), FLOOR)

    def release(r):
        @pl.when(r >= 1)
        def _():
            send_a(r - 1).start()

        @pl.when(r >= 2)
        def _():
            for d in (1, 2, 3):
                send_b(r - 2, d).start()

    def settle_partial(r, acc, top, mass):
        @pl.when(r >= 2)
        def _():
            send_a(r - 2).wait_send()

        @pl.when(r >= 3)
        def _():
            for d in (1, 2, 3):
                send_b(r - 3, d).wait_send()

        a_slot = lax.rem(r, 2)
        acc_buf[a_slot, :, :latent] = acc
        acc_buf[a_slot, :, latent:] = stats(top * scale, jnp.sum(mass, axis=1, keepdims=True))

        @pl.when(r >= 1)
        def _():
            pair_merge(r - 1)

    for half in (0, 1):
        for cp in c_copies(0, half):
            cp.wait()
    top = None
    query_0 = query(0)
    stage(1, 1)
    for i in range(n_chunks):
        t = scores(0, query_0, i)
        top = t if top is None else jnp.maximum(top, t)
    top_ref[...] = top_of(top) + jnp.zeros((heads, 128), f32)

    def step(b, carry):
        r = b - 1
        release(r)
        for first_wo, at in ((0, 3), (3, 2), (6, 1)):
            @pl.when(b == n_req - at)
            def _():
                for i in range(first_wo, min(first_wo + 3, n_wo)):
                    wo_copy(i).start()

        @pl.when(b == n_req - 4)
        def _():
            for i in range(hs // grp):
                uv_copy(i).start()

        old = top_ref[...]
        query_b = staged(b)
        top, mass, acc = None, None, None
        for half in (0, 1):
            for cp in c_copies(b, half):
                cp.wait()
            for i in range(half * n_chunks // 2, (half + 1) * n_chunks // 2):
                mass = add(mass, weigh(old, i))
                t = scores(b, query_b, i)
                top = t if top is None else jnp.maximum(top, t)
                acc = add(acc, values(r, i))

            if half == 0:
                stage(b + 1, lax.rem(b + 1, n_req))

            @pl.when(b + 2 < n_req)
            def _():
                for cp in c_copies(b + 2, half):
                    cp.start()

        top_ref[...] = top_of(top) + jnp.zeros((heads, 128), f32)
        settle_partial(r, acc, old[:, :1], mass)
        return carry

    lax.fori_loop(1, n_req, step, 0)
    release(n_req - 1)
    old = top_ref[...]
    mass, acc = None, None
    for i in range(n_chunks):
        mass = add(mass, weigh(old, i))
        acc = add(acc, values(n_req - 1, i))
    settle_partial(n_req - 1, acc, old[:, :1], mass)

    def final(b, carry):
        for d in (1, 2, 3):
            send_b(b, d).wait_recv()
        rows = pl.ds(my_head * n_req + b, hs, stride=n_req)
        cn = cn_ref[pl.ds(b, 1), :]
        s_new = jnp.sum(q_ref[n_lat, rows, :][:, :rope].astype(bf16).astype(f32) * kn_ref[pl.ds(b, 1), :], axis=1, keepdims=True)
        for j in range(n_lat):
            s_new = s_new + jnp.sum(q_ref[j, rows, :].astype(bf16).astype(f32) * cn[:, j * 128:(j + 1) * 128], axis=1, keepdims=True)
        s_new = s_new * scale
        parts = [own_b[b]] + [recv_b[b, d] for d in range(3)]
        tops = [p[:, latent:latent + 1] for p in parts] + [s_new]
        top = functools.reduce(jnp.maximum, tops)
        w_new = jnp.exp(s_new - top)
        mass = w_new
        acc = w_new.astype(bf16).astype(f32) * cn
        for p, t in zip(parts, tops):
            f = jnp.exp(t - top)
            acc = acc + p[:, :latent] * f
            mass = mass + p[:, latent + 64:latent + 65] * f
        o_lat = (acc / mass).astype(bf16).astype(f32)
        for j in range(n_lat):
            olat_ref[j, pl.ds(pl.multiple_of(b * hs, hs), hs), :] = o_lat[:, j * 128:(j + 1) * 128]
        return carry

    last = n_req - 1
    send_a(last).start()
    for d in (1, 2, 3):
        send_b(last - 1, d).start()
    lax.fori_loop(0, last - 1, final, 0)
    send_a(last - 1).wait_send()
    for d in (1, 2, 3):
        send_b(last - 2, d).wait_send()
    pair_merge(last)
    for i in range(hs // grp):
        uv_copy(i).wait()
        s_ref[...] = uk_buf[i].astype(f32).reshape(latent * grp, v_dim)
        if i == 0:
            for d in (1, 2, 3):
                send_b(last, d).start()
        for h in range(grp):
            c_buf[0, h * latent:(h + 1) * latent, i * v_dim:(i + 1) * v_dim] = s_ref[pl.ds(h, latent, stride=grp), :].astype(bf16)
    lax.fori_loop(last - 1, n_req, final, 0)
    send_a(last).wait_send()
    for b in (last - 1, last):
        for d in (1, 2, 3):
            send_b(b, d).wait_send()

    for h in range(hs):
        lhs = jnp.concatenate([olat_ref[j, pl.ds(h, n_req, stride=hs), :] for j in range(n_lat)], axis=1)
        uv = c_buf[0, (h % grp) * latent:(h % grp + 1) * latent, (h // grp) * v_dim:(h // grp + 1) * v_dim]
        o = jnp.dot(lhs.astype(bf16), uv, preferred_element_type=f32)
        o_ref[:, h * v_dim:(h + 1) * v_dim] = o.astype(bf16)

    def block(i):
        wo_copy(i).wait()
        return jnp.dot(o_ref[...], wo_buf[:, wo_slot(i)], preferred_element_type=f32)

    def to_pair(i):
        return exchange(po_ref.at[i], pair_ref.at[i], h_sem.at[0, i], h_sem.at[1, i], partner)

    def to_owner(i):
        return exchange(sum_ref.at[i], quart_ref.at[i], p_sem.at[0, i], p_sem.at[1, i], peer(i + 1))

    def first(i, carry):
        po_ref[i] = block(i)

        @pl.when(i >= 1)
        def _():
            to_pair(i - 1).start()

        return carry

    lax.fori_loop(0, 3, first, 0)
    to_pair(2).start()

    def second(i, carry):
        part = block(i + 3)
        to_pair(i).wait_recv()
        sum_ref[i] = part + pair_ref[i]

        @pl.when(i >= 1)
        def _():
            to_owner(i - 1).start()

        return carry

    lax.fori_loop(0, 3, second, 0)

    def third(i, carry):
        @pl.when(i == 0)
        def _():
            to_owner(2).start()

        @pl.when(i == 1)
        def _():
            to_pair(3).start()

        part = block(i + 6)

        @pl.when(i == 0)
        def _():
            po_ref[3] = part

        @pl.when(i == 1)
        def _():
            sum_ref[3] = part

        return carry

    lax.fori_loop(0, 2, third, 0)
    to_pair(3).wait_recv()
    sum_ref[3] = sum_ref[3] + pair_ref[3]
    for i in range(3):
        to_owner(i).wait_recv()
    my_cols = pl.ds(pl.multiple_of(core * half_cols + chip * qcols, qcols), qcols)
    total = sum_ref[3] + quart_ref[0] + quart_ref[1] + quart_ref[2]
    fin_ref[...] = (x_ref[:, my_cols].astype(f32) + total).astype(bf16).astype(f32)

    def to_all(d):
        return exchange(fin_ref, xo_ref.at[:, my_cols], f_sem.at[0, d - 1], f_sem.at[1, d - 1], peer(d))

    def from_all(d):
        cols = pl.ds(pl.multiple_of(core * half_cols + from_chip(d) * qcols, qcols), qcols)
        return exchange(fin_ref, xo_ref.at[:, cols], f_sem.at[0, d - 1], f_sem.at[1, d - 1], peer(d)), cols

    for d in (1, 2, 3):
        to_all(d).start()
    g0 = exchange(fin_ref, xo_ref.at[:, my_cols], g_sem.at[0, 0], g_sem.at[1, 0], partner)
    g0.start()
    out_ref[:, d_model:d_model + latent] = cn_ref[...]
    out_ref[:, d_model + latent:] = jnp.concatenate([kn_ref[...], jnp.zeros((n_req, 128 - rope), f32)], axis=1)
    fwd = [g0]
    for d in (1, 2, 3):
        got, cols = from_all(d)
        got.wait_recv()
        f = exchange(xo_ref.at[:, cols], xo_ref.at[:, cols], g_sem.at[0, d], g_sem.at[1, d], partner)
        f.start()
        fwd.append(f)
    for d in (1, 2, 3):
        to_all(d).wait_send()
    for i in range(3):
        to_owner(i).wait_send()
    for i in range(4):
        to_pair(i).wait_send()

    def settle_sent(g, carry):
        send_q(g).wait_send()
        return carry

    lax.fori_loop(0, n_grp, settle_sent, 0)
    for f in fwd:
        f.wait()
    xo_ref[:, my_cols] = fin_ref[...]
    out_ref[:, :d_model] = xo_ref[...]


def scoped_body(dims, *refs):
    heads, latent, rope, t_dev, t_chunk, n_slots = dims[1], dims[2], dims[4], dims[8], dims[9], dims[15]
    pl.run_scoped(
        lambda *scoped: decode_body(dims, *scoped, *refs),
        pltpu.VMEM((n_slots, t_dev, latent), jnp.bfloat16), pltpu.VMEM((n_slots, rope, t_dev), jnp.bfloat16),
        pltpu.VMEM((heads, t_dev), jnp.bfloat16), pltpu.VMEM((2, latent, t_chunk), jnp.bfloat16),
        pltpu.VMEM((2, heads, latent + 2 * rope), jnp.bfloat16))


def decode(x, w_dq, g_q, w_uq, w_dkv, g_kv, w_uk, w_uv, w_o, cache_c, cache_kr, ctx_len):
    n_req, d_model = x.shape
    latent, heads, nope = w_uk.shape
    rope = w_dkv.shape[1] - latent
    low = w_dq.shape[1]
    v_dim = w_uv.shape[2]
    t_dev = cache_c.shape[1]
    scale = (nope + rope) ** -0.5
    n_dq, n_kv, n_uq, n_uk, grp, n_slots, n_split, t_chunk = 14, 7, 4, 2, 8, 3, 4, 256
    f32, bf16 = jnp.float32, jnp.bfloat16
    dims = (n_req, heads, latent, nope, rope, v_dim, low, d_model, t_dev, t_chunk, n_dq, n_kv, n_uq, n_uk, grp, n_slots, n_split, scale)
    lane = jnp.arange(rope)
    inv_freq = ROPE_THETA ** (-2.0 * (lane % (rope // 2)).astype(f32) / rope)
    angles = ctx_len.astype(f32)[:, None] * inv_freq
    table = jnp.where(lane < rope // 2, jnp.cos(angles), jnp.sin(angles))
    turn = max(t_chunk, latent)
    hs = heads // 8
    hp = heads // 2
    tail = latent + 128
    qcols = d_model // 8
    n_grp = hp // grp
    vmem = pl.BlockSpec(memory_space=pltpu.VMEM)
    hbm = pl.BlockSpec(memory_space=pl.ANY)
    dma = pltpu.SemaphoreType.DMA
    out = pl.pallas_call(
        functools.partial(scoped_body, dims),
        out_shape=jax.ShapeDtypeStruct((n_req, d_model + latent + 128), f32),
        in_specs=[pl.BlockSpec(memory_space=pltpu.SMEM)] + [vmem] * 4 + [hbm] * 8,
        out_specs=vmem,
        scratch_shapes=[
            pltpu.VMEM((hs * v_dim, d_model), bf16),
            pltpu.VMEM((n_uk, latent, grp, nope), bf16),
            pltpu.VMEM((t_dev * heads // 128, 128), f32),
            pltpu.VMEM((heads, 128), f32),
            pltpu.VMEM((4, n_req, low // 4), f32),
            pltpu.VMEM((4, n_req, latent // 4), f32),
            pltpu.VMEM((n_req, low), bf16),
            pltpu.VMEM((latent // 128 + 1, heads * n_req, 128), f32),
            pltpu.VMEM((n_req, latent), f32),
            pltpu.VMEM((n_req, rope), f32),
            pltpu.VMEM((2, heads, tail), f32),
            pltpu.VMEM((2, hp, tail), f32),
            pltpu.VMEM((2, hp, tail), f32),
            pltpu.VMEM((n_req, 3, hs, tail), f32),
            pltpu.VMEM((n_req, hs, tail), f32),
            pltpu.VMEM((latent // 128, n_req * hs, 128), f32),
            pltpu.VMEM((n_req, hs * v_dim), bf16),
            pltpu.VMEM((4, n_req, qcols), f32),
            pltpu.VMEM((4, n_req, qcols), f32),
            pltpu.VMEM((4, n_req, qcols), f32),
            pltpu.VMEM((3, n_req, qcols), f32),
            pltpu.VMEM((n_req, qcols), f32),
            pltpu.VMEM((n_req, d_model), f32),
            dma((n_dq,)), dma((2, n_kv)), dma((n_uq, 2)), dma((n_uk,)),
            dma((3,)), dma((3,)), dma((3,)), dma((3,)), dma((n_grp,)), dma((n_grp,)),
            dma((n_slots, n_split + 1)), dma((hs // grp,)), dma((8,)),
            dma((n_req,)), dma((n_req,)), dma((n_req, 3)), dma((n_req, 3)),
            dma((2, 4)), dma((2, 3)), dma((2, 3)), dma((2, 4)),
        ],
        compiler_params=pltpu.CompilerParams(
            vmem_limit_bytes=67043328, collective_id=0, has_side_effects=True),
        name='decode',
    )(ctx_len, x, g_q, g_kv, table, w_dq, w_uq, jnp.swapaxes(w_dkv, 0, 1), w_uk,
      cache_c, jnp.swapaxes(cache_kr, 1, 2), w_uv, w_o)
    return out[:, :d_model].astype(bf16), out[:, d_model:d_model + latent].astype(bf16), out[:, d_model + latent:d_model + latent + rope].astype(bf16)


def solution(mesh):
    def decode_step(*args):
        return decode(*args)

    spec_rows = P('dp', None)
    spec_cache = P('dp', 'cp', None)
    in_specs = (spec_rows, P(), P(), P(), P(), P(), P(), P(), P(), spec_cache, spec_cache, P('dp'))
    out_specs = (spec_rows, spec_rows, spec_rows)
    return jax.shard_map(decode_step, mesh=mesh, in_specs=in_specs, out_specs=out_specs, check_vma=False)
```

```python
import functools

import jax
import jax.numpy as jnp
from jax import lax
from jax.experimental import pallas as pl
from jax.experimental.pallas import tpu as pltpu
from jax.sharding import PartitionSpec as P

NORM_EPS = 1e-6
ROPE_THETA = 10000.0
MASKED = -1e30
FLOOR = -1e29
LOG2E = 1.4426950408889634


def exchange(src, dst, send_sem, recv_sem, peer):
    return pltpu.make_async_remote_copy(
        src_ref=src, dst_ref=dst, send_sem=send_sem, recv_sem=recv_sem,
        device_id={'cp': peer}, device_id_type=pl.DeviceIdType.MESH)


def merge(parts, latent):
    tops = [p[:, latent:latent + 1] for p in parts]
    top = functools.reduce(jnp.maximum, tops)
    acc, mass = None, None
    for p, t in zip(parts, tops):
        f = jnp.exp(t - top)
        a, w = p[:, :latent] * f, p[:, latent + 64:latent + 65] * f
        acc = a if acc is None else acc + a
        mass = w if mass is None else mass + w
    return acc, top, mass


def stats(top, mass):
    lane = lax.broadcasted_iota(jnp.int32, (top.shape[0], 128), 1)
    return jnp.where(lane < 64, top, mass)


def decode_body(
        dims, c_buf, kr_buf, p_ref, turn_ref, qs_ref, ctx_ref, x_ref, gq_ref, gkv_ref, tab_ref, dq_hbm, uq_hbm, dkv_hbm, uk_hbm, c_hbm, kr_hbm, uv_hbm, wo_hbm, out_ref,
        wo_buf, uk_buf, s_ref, top_ref, cq_ref, kv_ref, norm_ref, q_ref, cn_ref, kn_ref,
        acc_buf, recv_a, comb, recv_b, own_b, olat_ref, o_ref,
        po_ref, pair_ref, sum_ref, quart_ref, fin_ref, xo_ref,
        dq_sem, dkv_sem, uq_sem, uk_sem, cs_sem, cr_sem, ks_sem, kr_sem, qs_sem, qv_sem,
        c_sem, uv_sem, wo_sem, sa_sem, ra_sem, sb_sem, rb_sem, h_sem, p_sem, f_sem, g_sem):
    (n_req, heads, latent, nope, rope, v_dim, low, d_model, t_dev, t_chunk, n_dq, n_kv, n_uq, n_uk, grp, n_slots, n_split, scale) = dims
    f32, bf16 = jnp.float32, jnp.bfloat16
    nt = (((1,), (1,)), ((), ()))
    me = lax.axis_index('cp')
    core = lax.rem(me, 2)
    chip = me // 2
    partner = chip * 2 + (1 - core)
    hp = heads // 2
    hs = heads // 8
    my_head = core * hp + chip * hs
    n_lat = latent // 128
    lcols = low // 4
    kcols = latent // 4
    n_grp = hp // grp
    wide = grp * (nope + rope)
    drows = d_model // n_dq
    kdepth = d_model // n_kv
    krows = kcols + rope
    half_cols = d_model // 2
    qcols = d_model // 8
    n_wo = 8

    def peer_chip(d):
        return lax.rem(chip + d, 4)

    def from_chip(d):
        return lax.rem(chip + 4 - d, 4)

    def peer(d):
        return peer_chip(d) * 2 + core

    def dq_piece(i):
        return wo_buf.at[pl.ds(low, drows), pl.ds(i * lcols, lcols)]

    def dq_copy(i):
        return pltpu.make_async_copy(dq_hbm.at[pl.ds(i * drows, drows), pl.ds(pl.multiple_of(chip * lcols, lcols), lcols)], dq_piece(i), dq_sem.at[i])

    def kv_piece(i, row, rows):
        return wo_buf.at[pl.ds(i * krows + row, rows), pl.ds(n_uq * wide, kdepth)]

    def dkv_copies(i):
        cols = pl.ds(i * kdepth, kdepth)
        return [pltpu.make_async_copy(dkv_hbm.at[pl.ds(pl.multiple_of(chip * kcols, kcols), kcols), cols], kv_piece(i, 0, kcols), dkv_sem.at[0, i]),
                pltpu.make_async_copy(dkv_hbm.at[pl.ds(latent, rope), cols], kv_piece(i, kcols, rope), dkv_sem.at[1, i])]

    def uq_slot(g):
        return pl.ds(pl.multiple_of(lax.rem(g, n_uq) * wide, wide), wide)

    def uq_copies(g):
        cols = pl.ds(pl.multiple_of((core * hp + g * grp) * (nope + rope), wide), wide)
        half = low // 2
        slot = lax.rem(g, n_uq)
        return [pltpu.make_async_copy(uq_hbm.at[pl.ds(i * half, half), cols], wo_buf.at[pl.ds(i * half, half), uq_slot(g)], uq_sem.at[slot, i])
                for i in (0, 1)]

    def uk_copy(g):
        slot = lax.rem(g, n_uk)
        return pltpu.make_async_copy(uk_hbm.at[:, pl.ds(pl.multiple_of(core * hp + g * grp, grp), grp), :], uk_buf.at[slot], uk_sem.at[slot])

    def c_copies(b, half):
        slot = lax.rem(b, n_slots)
        rows = t_dev // n_split
        out = []
        for i in range(half * n_split // 2, (half + 1) * n_split // 2):
            sl = pl.ds(i * rows, rows)
            out.append(pltpu.make_async_copy(c_hbm.at[b, sl], c_buf.at[slot, sl], c_sem.at[slot, i]))
        if half == 0:
            out.append(pltpu.make_async_copy(kr_hbm.at[b], kr_buf.at[slot], c_sem.at[slot, n_split]))
        return out

    def uv_copy(i):
        return pltpu.make_async_copy(uv_hbm.at[:, pl.ds(pl.multiple_of(my_head + i * grp, grp), grp), :], uk_buf.at[i], uv_sem.at[i])

    def wo_block(i):
        half = jnp.where((i < 3) | (i == 6), 1 - core, core)
        d = jnp.where(i < 3, i + 1, jnp.where(i < 6, i - 2, 0))
        return half * half_cols + lax.rem(chip + d, 4) * qcols

    def wo_slot(i):
        return pl.ds(pl.multiple_of(i * qcols, qcols), qcols)

    def wo_copy(i):
        rows = pl.ds(pl.multiple_of(my_head * v_dim, hs * v_dim), hs * v_dim)
        return pltpu.make_async_copy(wo_hbm.at[rows, pl.ds(pl.multiple_of(wo_block(i), qcols), qcols)], wo_buf.at[:, wo_slot(i)], wo_sem.at[i])

    for i in range(n_dq):
        dq_copy(i).start()
    for i in range(n_kv):
        for cp in dkv_copies(i):
            cp.start()
    uk_copy(0).start()
    for g in range(n_uq - 1):
        for cp in uq_copies(g):
            cp.start()

    barrier = pltpu.get_barrier_semaphore()
    pl.semaphore_signal(barrier, inc=1, device_id={'cp': partner}, device_id_type=pl.DeviceIdType.MESH)
    for d in (1, 2, 3):
        pl.semaphore_signal(barrier, inc=1, device_id={'cp': peer(d)}, device_id_type=pl.DeviceIdType.MESH)

    cq = None
    for i in range(n_dq):
        dq_copy(i).wait()
        part = jnp.dot(x_ref[:, i * drows:(i + 1) * drows], wo_buf[low:low + drows, i * lcols:(i + 1) * lcols], preferred_element_type=f32)
        cq = part if cq is None else cq + part
    cq_ref[chip] = cq.astype(bf16).astype(f32)
    pl.semaphore_wait(barrier, 4)

    def send_cq(d):
        return exchange(cq_ref.at[chip], cq_ref.at[chip], cs_sem.at[d - 1], cr_sem.at[d - 1], peer(d))

    def recv_cq(d):
        return exchange(cq_ref.at[from_chip(d)], cq_ref.at[from_chip(d)], cs_sem.at[d - 1], cr_sem.at[d - 1], peer(d))

    def send_kv(d):
        return exchange(kv_ref.at[chip], kv_ref.at[chip], ks_sem.at[d - 1], kr_sem.at[d - 1], peer(d))

    def recv_kv(d):
        return exchange(kv_ref.at[from_chip(d)], kv_ref.at[from_chip(d)], ks_sem.at[d - 1], kr_sem.at[d - 1], peer(d))

    for d in (1, 2, 3):
        send_cq(d).start()

    kv = None
    for i in range(n_kv):
        for cp in dkv_copies(i):
            cp.wait()
        part = lax.dot_general(x_ref[:, i * kdepth:(i + 1) * kdepth], wo_buf[i * krows:(i + 1) * krows, n_uq * wide:n_uq * wide + kdepth],
                               nt, preferred_element_type=f32)
        kv = part if kv is None else kv + part
    kv_ref[chip] = kv[:, :kcols]
    cos, sin = tab_ref[:, :rope // 2], tab_ref[:, rope // 2:]

    def rotate(v):
        lo, hi = v[:, :rope // 2], v[:, rope // 2:]
        return jnp.concatenate([lo * cos - hi * sin, hi * cos + lo * sin], axis=1)

    kn_ref[...] = rotate(kv[:, kcols:kcols + rope]).astype(bf16).astype(f32)

    for d in (1, 2, 3):
        recv_cq(d).wait_recv()
    for d in (1, 2, 3):
        send_kv(d).start()

    def rms(parts):
        total = None
        for p in parts:
            sq = jnp.sum(p * p, axis=1, keepdims=True)
            total = sq if total is None else total + sq
        return lax.rsqrt(total * (1.0 / (len(parts) * parts[0].shape[1])) + NORM_EPS)

    inv = rms([cq_ref[i] for i in range(4)])
    for i in range(4):
        norm_ref[:, i * lcols:(i + 1) * lcols] = (cq_ref[i] * inv * gq_ref[i * lcols:(i + 1) * lcols].reshape(1, lcols)).astype(bf16)

    def q_rows(c, g):
        return pl.ds(pl.multiple_of((c * hp + g * grp) * n_req, grp * n_req), grp * n_req)

    def send_q(g):
        return exchange(q_ref.at[:, q_rows(core, g)], q_ref.at[:, q_rows(core, g)], qs_sem.at[g], qv_sem.at[g], partner)

    def recv_q(g):
        return exchange(q_ref.at[:, q_rows(1 - core, g)], q_ref.at[:, q_rows(1 - core, g)], qs_sem.at[g], qv_sem.at[g], partner)

    def group(g, carry):
        @pl.when(g + 1 < n_grp)
        def _():
            uk_copy(g + 1).start()

        @pl.when(g + n_uq - 1 < n_grp)
        def _():
            for cp in uq_copies(g + n_uq - 1):
                cp.start()

        @pl.when(g >= n_grp - n_slots)
        def _():
            for cp in c_copies(g - (n_grp - n_slots), 0) + c_copies(g - (n_grp - n_slots), 1):
                cp.start()

        for cp in uq_copies(g):
            cp.wait()
        uk_copy(g).wait()

        @pl.when(g >= 1)
        def _():
            send_q(g - 1).start()

        q = jnp.dot(norm_ref[...], wo_buf[:low, uq_slot(g)], preferred_element_type=f32).astype(bf16).astype(f32)
        s_ref[...] = uk_buf[lax.rem(g, n_uk)].astype(f32).reshape(latent * grp, nope)
        for h in range(grp):
            at = h * (nope + rope)
            p_ref[:nope, (h % 2) * latent:(h % 2 + 1) * latent] = s_ref[pl.ds(h, latent, stride=grp), :].astype(bf16).T
            lat = jnp.dot(q[:, at:at + nope].astype(bf16), p_ref[:nope, (h % 2) * latent:(h % 2 + 1) * latent], preferred_element_type=f32)
            rows = pl.ds(pl.multiple_of((core * hp + g * grp + h) * n_req, n_req), n_req)
            for j in range(n_lat):
                q_ref[j, rows, :] = lat[:, j * 128:(j + 1) * 128]
            rot = rotate(q[:, at + nope:at + nope + rope])
            q_ref[n_lat, rows, :] = jnp.concatenate([rot, jnp.zeros((n_req, 128 - rope), f32)], axis=1)
        return carry

    lax.fori_loop(0, n_grp, group, 0)
    send_q(n_grp - 1).start()

    for d in (1, 2, 3):
        recv_kv(d).wait_recv()
    inv = rms([kv_ref[i] for i in range(4)])
    for i in range(4):
        cn_ref[:, i * kcols:(i + 1) * kcols] = (kv_ref[i] * inv * gkv_ref[i * kcols:(i + 1) * kcols].reshape(1, kcols)).astype(bf16).astype(f32)
    for d in (1, 2, 3):
        send_cq(d).wait_send()
        send_kv(d).wait_send()

    def settle(g, carry):
        recv_q(g).wait_recv()
        return carry

    lax.fori_loop(0, n_grp, settle, 0)

    def send_a(b):
        slot = lax.rem(b, 2)
        return exchange(acc_buf.at[slot, pl.ds(pl.multiple_of((1 - core) * hp, hp), hp)], recv_a.at[slot], sa_sem.at[b], ra_sem.at[b], partner)

    def send_b(b, d):
        slot = lax.rem(b, 2)
        return exchange(comb.at[slot, pl.ds(pl.multiple_of(peer_chip(d) * hs, hs), hs)], recv_b.at[b, d - 1], sb_sem.at[b, d - 1],
                        rb_sem.at[b, d - 1], peer(d))

    def pair_merge(b):
        slot = lax.rem(b, 2)
        send_a(b).wait_recv()
        mine = acc_buf[slot, pl.ds(pl.multiple_of(core * hp, hp), hp), :]
        acc, top, mass = merge([mine, recv_a[slot]], latent)
        comb[slot, :, :latent] = acc
        comb[slot, :, latent:] = stats(top, mass)
        own_b[b] = comb[slot, pl.ds(pl.multiple_of(chip * hs, hs), hs), :]

    base = me * t_dev
    n_chunks = t_dev // t_chunk
    lanes = t_chunk // 128
    k2 = scale * LOG2E

    def query(b):
        q = jnp.concatenate([q_ref[j, pl.ds(b, heads, stride=n_req), :].astype(bf16) for j in range(n_lat)], axis=1)
        return q, q_ref[n_lat, pl.ds(b, heads, stride=n_req), :][:, :rope].astype(bf16), ctx_ref[b] - base

    def stage(b, row):
        q, qr, _ = query(row)
        qs_ref[lax.rem(b, 2), :, :latent] = q
        qs_ref[lax.rem(b, 2), :, latent:] = jnp.concatenate([qr, qr], axis=1)

    def staged(b):
        slot = lax.rem(b, 2)
        return qs_ref[slot, :, :latent], qs_ref[slot, :, latent:latent + rope], ctx_ref[b] - base

    def scores(b, query_b, i):
        q, qr, limit = query_b
        slot = lax.rem(b, n_slots)
        sl = pl.ds(i * t_chunk, t_chunk)
        turn_ref[i % 2, :, :t_chunk] = c_buf[slot, sl, :].T
        s = jnp.dot(q, turn_ref[i % 2, :, :t_chunk], preferred_element_type=f32)
        s = s + jnp.dot(qr, kr_buf[slot, :, sl], preferred_element_type=f32)
        pos = lax.broadcasted_iota(jnp.int32, (1, t_chunk), 1) + i * t_chunk
        s = jnp.where(pos < limit, s, MASKED)
        top = None
        for j in range(lanes):
            part = s[:, j * 128:(j + 1) * 128]
            s_ref[pl.ds((i * lanes + j) * heads, heads), :] = part
            top = part if top is None else jnp.maximum(top, part)
        return top

    def weigh(top, i):
        mass = None
        for j in range(lanes):
            p = jnp.exp2((s_ref[pl.ds((i * lanes + j) * heads, heads), :] - top) * k2)
            mass = p if mass is None else mass + p
            p_ref[:, (i * lanes + j) * 128:(i * lanes + j + 1) * 128] = p.astype(bf16)
        return mass

    def values(b, i):
        sl = pl.ds(i * t_chunk, t_chunk)
        return jnp.dot(p_ref[:, sl], c_buf[lax.rem(b, n_slots), sl, :], preferred_element_type=f32)

    def add(a, v):
        return v if a is None else a + v

    def top_of(a):
        return jnp.maximum(jnp.max(a, axis=1, keepdims=True), FLOOR)

    def release(r):
        @pl.when(r >= 1)
        def _():
            send_a(r - 1).start()

        @pl.when(r >= 2)
        def _():
            for d in (1, 2, 3):
                send_b(r - 2, d).start()

    def settle_partial(r, acc, top, mass):
        @pl.when(r >= 2)
        def _():
            send_a(r - 2).wait_send()

        @pl.when(r >= 3)
        def _():
            for d in (1, 2, 3):
                send_b(r - 3, d).wait_send()

        a_slot = lax.rem(r, 2)
        acc_buf[a_slot, :, :latent] = acc
        acc_buf[a_slot, :, latent:] = stats(top * scale, jnp.sum(mass, axis=1, keepdims=True))

        @pl.when(r >= 1)
        def _():
            pair_merge(r - 1)

    for half in (0, 1):
        for cp in c_copies(0, half):
            cp.wait()
    top = None
    query_0 = query(0)
    stage(1, 1)
    for i in range(n_chunks):
        t = scores(0, query_0, i)
        top = t if top is None else jnp.maximum(top, t)
    top_ref[...] = top_of(top) + jnp.zeros((heads, 128), f32)

    def step(b, carry):
        r = b - 1
        release(r)
        for first_wo, at in ((0, 3), (3, 2), (6, 1)):
            @pl.when(b == n_req - at)
            def _():
                for i in range(first_wo, min(first_wo + 3, n_wo)):
                    wo_copy(i).start()

        @pl.when(b == n_req - 4)
        def _():
            for i in range(hs // grp):
                uv_copy(i).start()

        old = top_ref[...]
        query_b = staged(b)
        top, mass, acc = None, None, None
        for half in (0, 1):
            for cp in c_copies(b, half):
                cp.wait()
            for i in range(half * n_chunks // 2, (half + 1) * n_chunks // 2):
                mass = add(mass, weigh(old, i))
                t = scores(b, query_b, i)
                top = t if top is None else jnp.maximum(top, t)
                acc = add(acc, values(r, i))

            if half == 0:
                stage(b + 1, lax.rem(b + 1, n_req))

            @pl.when(b + 2 < n_req)
            def _():
                for cp in c_copies(b + 2, half):
                    cp.start()

        top_ref[...] = top_of(top) + jnp.zeros((heads, 128), f32)
        settle_partial(r, acc, old[:, :1], mass)
        return carry

    lax.fori_loop(1, n_req, step, 0)
    release(n_req - 1)
    old = top_ref[...]
    mass, acc = None, None
    for i in range(n_chunks):
        mass = add(mass, weigh(old, i))
        acc = add(acc, values(n_req - 1, i))
    settle_partial(n_req - 1, acc, old[:, :1], mass)

    def final(b, carry):
        for d in (1, 2, 3):
            send_b(b, d).wait_recv()
        rows = pl.ds(my_head * n_req + b, hs, stride=n_req)
        cn = cn_ref[pl.ds(b, 1), :]
        s_new = jnp.sum(q_ref[n_lat, rows, :][:, :rope].astype(bf16).astype(f32) * kn_ref[pl.ds(b, 1), :], axis=1, keepdims=True)
        for j in range(n_lat):
            s_new = s_new + jnp.sum(q_ref[j, rows, :].astype(bf16).astype(f32) * cn[:, j * 128:(j + 1) * 128], axis=1, keepdims=True)
        s_new = s_new * scale
        parts = [own_b[b]] + [recv_b[b, d] for d in range(3)]
        tops = [p[:, latent:latent + 1] for p in parts] + [s_new]
        top = functools.reduce(jnp.maximum, tops)
        w_new = jnp.exp(s_new - top)
        mass = w_new
        acc = w_new.astype(bf16).astype(f32) * cn
        for p, t in zip(parts, tops):
            f = jnp.exp(t - top)
            acc = acc + p[:, :latent] * f
            mass = mass + p[:, latent + 64:latent + 65] * f
        o_lat = (acc / mass).astype(bf16).astype(f32)
        for j in range(n_lat):
            olat_ref[j, pl.ds(pl.multiple_of(b * hs, hs), hs), :] = o_lat[:, j * 128:(j + 1) * 128]
        return carry

    last = n_req - 1
    send_a(last).start()
    for d in (1, 2, 3):
        send_b(last - 1, d).start()
    lax.fori_loop(0, last - 1, final, 0)
    send_a(last - 1).wait_send()
    for d in (1, 2, 3):
        send_b(last - 2, d).wait_send()
    pair_merge(last)
    for i in range(hs // grp):
        uv_copy(i).wait()
        s_ref[...] = uk_buf[i].astype(f32).reshape(latent * grp, v_dim)
        if i == 0:
            for d in (1, 2, 3):
                send_b(last, d).start()
        for h in range(grp):
            c_buf[0, h * latent:(h + 1) * latent, i * v_dim:(i + 1) * v_dim] = s_ref[pl.ds(h, latent, stride=grp), :].astype(bf16)
    lax.fori_loop(last - 1, n_req, final, 0)
    send_a(last).wait_send()
    for b in (last - 1, last):
        for d in (1, 2, 3):
            send_b(b, d).wait_send()

    for h in range(hs):
        lhs = jnp.concatenate([olat_ref[j, pl.ds(h, n_req, stride=hs), :] for j in range(n_lat)], axis=1)
        uv = c_buf[0, (h % grp) * latent:(h % grp + 1) * latent, (h // grp) * v_dim:(h // grp + 1) * v_dim]
        o = jnp.dot(lhs.astype(bf16), uv, preferred_element_type=f32)
        o_ref[:, h * v_dim:(h + 1) * v_dim] = o.astype(bf16)

    def block(i):
        wo_copy(i).wait()
        return jnp.dot(o_ref[...], wo_buf[:, wo_slot(i)], preferred_element_type=f32)

    def to_pair(i):
        return exchange(po_ref.at[i], pair_ref.at[i], h_sem.at[0, i], h_sem.at[1, i], partner)

    def to_owner(i):
        return exchange(sum_ref.at[i], quart_ref.at[i], p_sem.at[0, i], p_sem.at[1, i], peer(i + 1))

    def first(i, carry):
        po_ref[i] = block(i)

        @pl.when(i >= 1)
        def _():
            to_pair(i - 1).start()

        return carry

    lax.fori_loop(0, 3, first, 0)
    to_pair(2).start()

    def second(i, carry):
        part = block(i + 3)
        to_pair(i).wait_recv()
        sum_ref[i] = part + pair_ref[i]

        @pl.when(i >= 1)
        def _():
            to_owner(i - 1).start()

        return carry

    lax.fori_loop(0, 3, second, 0)

    def third(i, carry):
        @pl.when(i == 0)
        def _():
            to_owner(2).start()

        @pl.when(i == 1)
        def _():
            to_pair(3).start()

        part = block(i + 6)

        @pl.when(i == 0)
        def _():
            po_ref[3] = part

        @pl.when(i == 1)
        def _():
            sum_ref[3] = part

        return carry

    lax.fori_loop(0, 2, third, 0)
    to_pair(3).wait_recv()
    sum_ref[3] = sum_ref[3] + pair_ref[3]
    for i in range(3):
        to_owner(i).wait_recv()
    my_cols = pl.ds(pl.multiple_of(core * half_cols + chip * qcols, qcols), qcols)
    total = sum_ref[3] + quart_ref[0] + quart_ref[1] + quart_ref[2]
    fin_ref[...] = (x_ref[:, my_cols].astype(f32) + total).astype(bf16).astype(f32)

    def to_all(d):
        return exchange(fin_ref, xo_ref.at[:, my_cols], f_sem.at[0, d - 1], f_sem.at[1, d - 1], peer(d))

    def from_all(d):
        cols = pl.ds(pl.multiple_of(core * half_cols + from_chip(d) * qcols, qcols), qcols)
        return exchange(fin_ref, xo_ref.at[:, cols], f_sem.at[0, d - 1], f_sem.at[1, d - 1], peer(d)), cols

    for d in (1, 2, 3):
        to_all(d).start()
    g0 = exchange(fin_ref, xo_ref.at[:, my_cols], g_sem.at[0, 0], g_sem.at[1, 0], partner)
    g0.start()
    out_ref[:, d_model:d_model + latent] = cn_ref[...]
    out_ref[:, d_model + latent:] = jnp.concatenate([kn_ref[...], jnp.zeros((n_req, 128 - rope), f32)], axis=1)
    fwd = [g0]
    for d in (1, 2, 3):
        got, cols = from_all(d)
        got.wait_recv()
        f = exchange(xo_ref.at[:, cols], xo_ref.at[:, cols], g_sem.at[0, d], g_sem.at[1, d], partner)
        f.start()
        fwd.append(f)
    for d in (1, 2, 3):
        to_all(d).wait_send()
    for i in range(3):
        to_owner(i).wait_send()
    for i in range(4):
        to_pair(i).wait_send()

    def settle_sent(g, carry):
        send_q(g).wait_send()
        return carry

    lax.fori_loop(0, n_grp, settle_sent, 0)
    for f in fwd:
        f.wait()
    xo_ref[:, my_cols] = fin_ref[...]
    out_ref[:, :d_model] = xo_ref[...]


def scoped_body(dims, *refs):
    heads, latent, rope, t_dev, t_chunk, n_slots = dims[1], dims[2], dims[4], dims[8], dims[9], dims[15]
    pl.run_scoped(
        lambda *scoped: decode_body(dims, *scoped, *refs),
        pltpu.VMEM((n_slots, t_dev, latent), jnp.bfloat16), pltpu.VMEM((n_slots, rope, t_dev), jnp.bfloat16),
        pltpu.VMEM((heads, t_dev), jnp.bfloat16), pltpu.VMEM((2, latent, t_chunk), jnp.bfloat16),
        pltpu.VMEM((2, heads, latent + 2 * rope), jnp.bfloat16))


def decode(x, w_dq, g_q, w_uq, w_dkv, g_kv, w_uk, w_uv, w_o, cache_c, cache_kr, ctx_len):
    n_req, d_model = x.shape
    latent, heads, nope = w_uk.shape
    rope = w_dkv.shape[1] - latent
    low = w_dq.shape[1]
    v_dim = w_uv.shape[2]
    t_dev = cache_c.shape[1]
    scale = (nope + rope) ** -0.5
    n_dq, n_kv, n_uq, n_uk, grp, n_slots, n_split, t_chunk = 14, 7, 4, 2, 8, 3, 4, 512
    f32, bf16 = jnp.float32, jnp.bfloat16
    dims = (n_req, heads, latent, nope, rope, v_dim, low, d_model, t_dev, t_chunk, n_dq, n_kv, n_uq, n_uk, grp, n_slots, n_split, scale)
    lane = jnp.arange(rope)
    inv_freq = ROPE_THETA ** (-2.0 * (lane % (rope // 2)).astype(f32) / rope)
    angles = ctx_len.astype(f32)[:, None] * inv_freq
    table = jnp.where(lane < rope // 2, jnp.cos(angles), jnp.sin(angles))
    turn = max(t_chunk, latent)
    hs = heads // 8
    hp = heads // 2
    tail = latent + 128
    qcols = d_model // 8
    n_grp = hp // grp
    vmem = pl.BlockSpec(memory_space=pltpu.VMEM)
    hbm = pl.BlockSpec(memory_space=pl.ANY)
    dma = pltpu.SemaphoreType.DMA
    out = pl.pallas_call(
        functools.partial(scoped_body, dims),
        out_shape=jax.ShapeDtypeStruct((n_req, d_model + latent + 128), f32),
        in_specs=[pl.BlockSpec(memory_space=pltpu.SMEM)] + [vmem] * 4 + [hbm] * 8,
        out_specs=vmem,
        scratch_shapes=[
            pltpu.VMEM((hs * v_dim, d_model), bf16),
            pltpu.VMEM((n_uk, latent, grp, nope), bf16),
            pltpu.VMEM((t_dev * heads // 128, 128), f32),
            pltpu.VMEM((heads, 128), f32),
            pltpu.VMEM((4, n_req, low // 4), f32),
            pltpu.VMEM((4, n_req, latent // 4), f32),
            pltpu.VMEM((n_req, low), bf16),
            pltpu.VMEM((latent // 128 + 1, heads * n_req, 128), f32),
            pltpu.VMEM((n_req, latent), f32),
            pltpu.VMEM((n_req, rope), f32),
            pltpu.VMEM((2, heads, tail), f32),
            pltpu.VMEM((2, hp, tail), f32),
            pltpu.VMEM((2, hp, tail), f32),
            pltpu.VMEM((n_req, 3, hs, tail), f32),
            pltpu.VMEM((n_req, hs, tail), f32),
            pltpu.VMEM((latent // 128, n_req * hs, 128), f32),
            pltpu.VMEM((n_req, hs * v_dim), bf16),
            pltpu.VMEM((4, n_req, qcols), f32),
            pltpu.VMEM((4, n_req, qcols), f32),
            pltpu.VMEM((4, n_req, qcols), f32),
            pltpu.VMEM((3, n_req, qcols), f32),
            pltpu.VMEM((n_req, qcols), f32),
            pltpu.VMEM((n_req, d_model), f32),
            dma((n_dq,)), dma((2, n_kv)), dma((n_uq, 2)), dma((n_uk,)),
            dma((3,)), dma((3,)), dma((3,)), dma((3,)), dma((n_grp,)), dma((n_grp,)),
            dma((n_slots, n_split + 1)), dma((hs // grp,)), dma((8,)),
            dma((n_req,)), dma((n_req,)), dma((n_req, 3)), dma((n_req, 3)),
            dma((2, 4)), dma((2, 3)), dma((2, 3)), dma((2, 4)),
        ],
        compiler_params=pltpu.CompilerParams(
            vmem_limit_bytes=67043328, collective_id=0, has_side_effects=True),
        name='decode',
    )(ctx_len, x, g_q, g_kv, table, w_dq, w_uq, jnp.swapaxes(w_dkv, 0, 1), w_uk,
      cache_c, jnp.swapaxes(cache_kr, 1, 2), w_uv, w_o)
    return out[:, :d_model].astype(bf16), out[:, d_model:d_model + latent].astype(bf16), out[:, d_model + latent:d_model + latent + rope].astype(bf16)


def solution(mesh):
    def decode_step(*args):
        return decode(*args)

    spec_rows = P('dp', None)
    spec_cache = P('dp', 'cp', None)
    in_specs = (spec_rows, P(), P(), P(), P(), P(), P(), P(), P(), spec_cache, spec_cache, P('dp'))
    out_specs = (spec_rows, spec_rows, spec_rows)
    return jax.shard_map(decode_step, mesh=mesh, in_specs=in_specs, out_specs=out_specs, check_vma=False)
```
